256 devices in a mesh: section: 4 (over x), slab: 16 (over z, core), img: 4 (over y).
Axes of the slice: x: 4, y: 4, z: 8, core: 2. Of those that a mesh axis runs over, the one named last changes fastest.
Arguments:
- strips: bfloat16 [4, 4, 8, 128, 320], P('img', None, None, 'slab'), may hold values from -6 to 6
- kernels: bfloat16 [4, 2, 9, 320, 320], P('section'), may hold values from -0.109375 to 0.109375
- cotangent: bfloat16 [4, 4, 8, 128, 320], P('img', None, None, 'slab'), may hold values from -18 to 18
Outputs:
- grad_kernels: float32 [4, 2, 9, 320, 320], P('section', None, None, 'slab', 'img')
- grad_inputs: bfloat16 [4, 4, 4, 8, 128, 320], P('section', 'img', None, None, 'slab')
The draws below stay inside these ranges and needn't reach their ends.
All inputs are finite; a program needn't handle non-finite values.
Results may differ from the reference program's by a relative error of at most 0.023.
Values may be sent and summed in bfloat16 or wider, within the bound.
A program may use at most 128 MiB of HBM per device.

```python
import math
import jax
import jax.numpy as jnp
from jax import lax

C = 320
ROWS = 8
STRIPS = 4
SECTIONS = 4
IMAGES = 4
WIDTH = 128


def draw_cotangent(key, part):
    full_shape = (IMAGES, STRIPS, ROWS, WIDTH, C)
    column = jnp.arange(WIDTH).astype(jnp.float32) / max(WIDTH - 1, 1)
    image_pos = jnp.arange(IMAGES).astype(jnp.float32) / max(IMAGES - 1, 1)
    scales = 0.5 * jnp.power(3.0, column)[None, None, None, :, None] * jnp.power(3.0, image_pos)[:, None, None, None, None]
    own_key = jax.random.fold_in(jax.random.fold_in(key, 7), 0)
    values = jnp.clip(jax.random.normal(own_key, full_shape, jnp.float32), -4.0, 4.0)
    return (values * scales).astype(jnp.bfloat16)


def levels(rng, shape, cuts, low, high):
    factor_of = 1.0
    for axis_at, blocks in cuts:
        heights = jax.random.uniform(jax.random.fold_in(jax.random.fold_in(rng, 6), axis_at), (blocks,), jnp.float32, low / len(cuts), high / len(cuts))
        factor_of = factor_of * jnp.repeat(jnp.exp(heights), shape[axis_at] // blocks).reshape((-1,) + (1,) * (len(shape) - 1 - axis_at))
    return factor_of


def centred(rng, extent, deviation, most, shards=(), kind=jnp.bfloat16):
    factor_of = levels(rng, extent, shards, -0.22, 0.18) if shards else 1.0
    array = jax.random.normal(rng, extent, jnp.float32) * deviation * factor_of
    return jnp.minimum(jnp.maximum(array, -most), most).astype(kind)


def setup_inputs(seed: int = 0) -> dict:
    key_of = jax.random.split(jax.random.key(seed), 4)
    strips = centred(key_of[0], (IMAGES, STRIPS, ROWS, WIDTH, C), 1.0, 6.0, ((0, 4), (3, 16)))
    kernels = centred(key_of[1], (SECTIONS, 2, 9, C, C), (9 * C) ** -0.5, 0.109375, ((0, 4),))
    cotangent = draw_cotangent(jax.random.fold_in(key_of[3], 71), 0)
    return dict(strips=strips, kernels=kernels, cotangent=cotangent)


def unfold(padded, row_count, col_count):
    tap_list = [padded[:, down_at:down_at + row_count, right_at:right_at + col_count, :] for down_at in range(3) for right_at in range(3)]
    stacked = jnp.concatenate(tap_list, axis=3)
    return stacked.reshape(-1, stacked.shape[3])

def columns_of(wide_field):
    row_count = wide_field.shape[1]
    col_count = wide_field.shape[2] - 2
    padded = jnp.pad(wide_field, ((0, 0), (1, 1), (0, 0), (0, 0)))
    return unfold(padded, row_count, col_count)

def convolve(matrix, wide_field):
    count, row_count = (wide_field.shape[0], wide_field.shape[1])
    col_count = wide_field.shape[2] - 2
    flat_out = jnp.dot(columns_of(wide_field), matrix, preferred_element_type=jnp.float32)
    return flat_out.reshape(count, row_count, col_count, matrix.shape[1])

def contract(wide_field, grad_out):
    flat_grad = grad_out.reshape(-1, grad_out.shape[3])
    return lax.dot_general(columns_of(wide_field), flat_grad, (((0,), (0,)), ((), ())), preferred_element_type=jnp.float32)

def silu_slope(hidden):
    sigmoid_at = jax.nn.sigmoid(hidden)
    return sigmoid_at * (1.0 + hidden * (1.0 - sigmoid_at))

def pad_cols(field_in):
    return jnp.pad(field_in, ((0, 0), (0, 0), (1, 1), (0, 0)))

def forward_matrix(kernel):
    return kernel.reshape(9 * kernel.shape[1], kernel.shape[2])

def backward_matrix(kernel):
    return jnp.transpose(kernel[::-1], (0, 2, 1)).reshape(9 * kernel.shape[1], kernel.shape[2])

def reference(strips, kernels, cotangent):
    channels = kernels.shape[3]
    batch_size = IMAGES * STRIPS
    scaling = 1.0 / math.sqrt(IMAGES * STRIPS * ROWS * WIDTH)
    field_in = strips.reshape(batch_size, ROWS, WIDTH, channels)
    saved_list = []
    for section_no in range(SECTIONS):
        wide_field = pad_cols(field_in)
        hidden = convolve(forward_matrix(kernels[section_no, 0]), wide_field)
        active = jax.nn.silu(hidden).astype(jnp.bfloat16)
        wide_active = pad_cols(active)
        result_out = field_in.astype(jnp.float32) + convolve(forward_matrix(kernels[section_no, 1]), wide_active)
        saved_list.append((wide_field, hidden, wide_active))
        field_in = result_out.astype(jnp.bfloat16)
    grad_out = cotangent.reshape(batch_size, ROWS, WIDTH, channels)
    kernel_list = [None for section_no in range(SECTIONS)]
    grad_list = [None for section_no in range(SECTIONS)]
    for section_no in reversed(range(SECTIONS)):
        wide_field, hidden, wide_active = saved_list[section_no]
        upper_term = contract(wide_active, grad_out)
        grad_active = convolve(backward_matrix(kernels[section_no, 1]), pad_cols(grad_out))
        grad_hidden = (grad_active * silu_slope(hidden)).astype(jnp.bfloat16)
        lower_term = contract(wide_field, grad_hidden)
        grad_sum = grad_out.astype(jnp.float32) + convolve(backward_matrix(kernels[section_no, 0]), pad_cols(grad_hidden))
        grad_out = grad_sum.astype(jnp.bfloat16)
        kernel_list[section_no] = jnp.stack([lower_term, upper_term]).reshape(2, 9, channels, channels)
        grad_list[section_no] = grad_out.reshape(IMAGES, STRIPS, ROWS, WIDTH, channels)
    grad_kernels = jnp.stack(kernel_list, axis=0) * scaling
    grad_inputs = jnp.stack(grad_list, axis=0)
    return (grad_kernels, grad_inputs)
```

```python
import math

import jax
import jax.numpy as jnp
from jax import lax
from jax.experimental import pallas as pl
from jax.experimental.pallas import tpu as pltpu
from jax.sharding import PartitionSpec as P

MESH = pl.DeviceIdType.MESH
F32 = jnp.float32
BF16 = jnp.bfloat16

C = 320
SECTIONS = 4
IMAGES = 4
CROPS = 4
CHIPS = 8
SLABS = 16
ROWS = 8
COLS = 8
POS = ROWS * COLS
WIDE = POS + 16
DEEP = POS + 32
OUT_SHARE = C // IMAGES
IN_SHARE = C // SLABS
HALF = 256
PEERS = 8


def iota(shape, dim):
    return lax.broadcasted_iota(jnp.int32, shape, dim)


def onehot(cond):
    return jnp.where(cond, 1.0, 0.0).astype(BF16)


def sigmoid(v):
    return 1.0 / (1.0 + jnp.exp(-v))


def row_shifts(x):
    count = x.shape[0]
    row = iota(x.shape, 0) % ROWS
    above = jnp.where(row == 0, 0.0, pltpu.roll(x, 1, 0))
    below = jnp.where(row == ROWS - 1, 0.0, pltpu.roll(x, count - 1, 0))
    return above, x, below


def conv(x, weights, part, count):
    shifted = row_shifts(x)
    total = None
    for a in range(3):
        for b in range(3):
            lhs = shifted[a][8 * b : 8 * b + count].astype(BF16)
            term = jnp.dot(lhs, weights[part, 3 * a + b], preferred_element_type=F32)
            total = term if total is None else total + term
    return total


def conv_t(x, weights, part, count):
    shifted = row_shifts(x)
    total = None
    for a in range(3):
        for b in range(3):
            lhs = shifted[a][8 * b : 8 * b + count].astype(BF16)
            term = lax.dot_general(
                lhs,
                weights[part, 8 - (3 * a + b)],
                (((1,), (1,)), ((), ())),
                preferred_element_type=F32,
            )
            total = term if total is None else total + term
    return total


def kernel(
    scaling,
    strips,
    kernels,
    cotangent,
    gk_out,
    gi_out,
    w,
    sv,
    cv,
    fin,
    gin,
    fout,
    gout,
    hid,
    fs,
    fg,
    gs,
    gg,
    cc,
    acc,
    pkl,
    pk,
    rz,
    pc,
    sel,
    c6,
    local_sem,
    fr,
    fsend,
    br,
    bsend,
    edge_send,
    fg_recv,
    fg_send,
    gg_recv,
    gg_send,
    z_recv,
    z_send,
):
    s = lax.axis_index("section")
    slab = lax.axis_index("slab")
    img = lax.axis_index("img")
    z = slab // 2
    core = slab % 2
    has_left = slab > 0
    has_right = slab < SLABS - 1

    loads = [
        pltpu.make_async_copy(strips, sv, local_sem.at[0]),
        pltpu.make_async_copy(cotangent, cv, local_sem.at[1]),
        pltpu.make_async_copy(kernels, w, local_sem.at[2]),
    ]
    for load in loads:
        load.start()

    @pl.when(slab == 0)
    def _():
        for buf in (fin, gin):
            buf[:, 0:16, :] = jnp.zeros((CROPS, 16, C), BF16)

    @pl.when(slab == SLABS - 1)
    def _():
        for buf in (fin, gin):
            buf[:, DEEP - 16 : DEEP, :] = jnp.zeros((CROPS, 16, C), BF16)

    barrier = pltpu.get_barrier_semaphore()

    def greet(where):
        pl.semaphore_signal(barrier, inc=1, device_id=where, device_id_type=MESH)

    def peer_of(m):
        return (s, 2 * z + (core + m % 2) % 2, (img + m // 2) % IMAGES)

    def chip_of(d):
        return (s, 2 * ((z + d) % CHIPS) + core, img)

    greeted = jnp.int32(0)
    for ds in (-1, 0, 1):
        for dj in (-1, 0, 1):
            if ds == 0 and dj == 0:
                continue
            ok = (s + ds >= 0) & (s + ds < SECTIONS) & (slab + dj >= 0) & (slab + dj < SLABS)

            @pl.when(ok)
            def _():
                greet((s + ds, slab + dj, img))

            greeted = greeted + jnp.where(ok, 1, 0)
    for m in range(1, PEERS):
        greet(peer_of(m))
    for d in range(1, CHIPS):
        greet(chip_of(d))
    pl.semaphore_wait(barrier, greeted + (PEERS - 1) + (CHIPS - 1))

    i, j = iota((POS, POS), 0), iota((POS, POS), 1)
    swap = onehot((i // 8 == j % 8) & (i % 8 == j // 8))
    i, j = iota((C, 2 * HALF), 0), iota((C, 2 * HALF), 1)
    lane = j % 32
    pc[...] = onehot((lane < IN_SHARE) & (i == IN_SHARE * (2 * ((j % HALF) // 32) + j // HALF) + lane))
    lane = j % 128
    sel[...] = onehot((lane < OUT_SHARE) & (i == OUT_SHARE * (j // 128) + lane))
    i, j = iota((768, 512), 0), iota((768, 512), 1)
    lane = i % 32
    c6[...] = onehot(
        (lane < IN_SHARE)
        & ((i % 128) // 32 == j // 128)
        & (j % 128 == IN_SHARE * (i // 128) + lane)
    )

    def permuted(x, matrix):
        return jnp.dot(x, matrix, preferred_element_type=F32).astype(BF16)

    def spread(src, dst, send, recv, k, ds, center):
        if center:
            pltpu.make_async_remote_copy(
                src_ref=src.at[k, pl.ds(16, POS)] if src is dst else src.at[k],
                dst_ref=dst.at[k, pl.ds(16, POS)],
                send_sem=send.at[k, 1],
                recv_sem=recv.at[k, 1],
                device_id=(s + ds, slab, img),
                device_id_type=MESH,
            ).start()
        base = 16 if src is dst else 0

        @pl.when(has_right)
        def _():
            pltpu.make_async_remote_copy(
                src_ref=src.at[k, pl.ds(base + POS - 16, 16)],
                dst_ref=dst.at[k, pl.ds(0, 16)],
                send_sem=send.at[k, 2],
                recv_sem=recv.at[k, 0],
                device_id=(s + ds, slab + 1, img),
                device_id_type=MESH,
            ).start()

        @pl.when(has_left)
        def _():
            pltpu.make_async_remote_copy(
                src_ref=src.at[k, pl.ds(base, 16)],
                dst_ref=dst.at[k, pl.ds(DEEP - 16, 16)],
                send_sem=send.at[k, 0],
                recv_sem=recv.at[k, 2],
                device_id=(s + ds, slab - 1, img),
                device_id_type=MESH,
            ).start()

    def waited(ref, sem):
        pltpu.make_async_copy(ref, ref, sem).wait()

    def arrive(dst, recv, k, center):
        @pl.when(center)
        def _():
            waited(dst.at[k, pl.ds(16, POS)], recv.at[k, 1])

        @pl.when(has_left)
        def _():
            waited(dst.at[k, pl.ds(0, 16)], recv.at[k, 0])

        @pl.when(has_right)
        def _():
            waited(dst.at[k, pl.ds(DEEP - 16, 16)], recv.at[k, 2])

    def sent(src, send, k, center):
        base = 16 if center is None else 0
        if center is not None:
            waited(src.at[k], send.at[k, 1])

        @pl.when(has_right)
        def _():
            waited(src.at[k, pl.ds(base + POS - 16, 16)], send.at[k, 2])

        @pl.when(has_left)
        def _():
            waited(src.at[k, pl.ds(base, 16)], send.at[k, 0])

    loads[0].wait()
    loads[1].wait()

    @pl.when(s == 0)
    def _():
        def step(k, carry):
            fin[k, 16 : 16 + POS, :] = permuted(swap, sv[k])
            spread(fin, fin, edge_send, fr, k, 0, False)
            return carry

        lax.fori_loop(0, CROPS, step, 0)

    @pl.when(s == SECTIONS - 1)
    def _():
        def step(k, carry):
            gin[k, 16 : 16 + POS, :] = permuted(swap, cv[k])
            spread(gin, gin, edge_send, br, k, 0, False)
            return carry

        lax.fori_loop(0, CROPS, step, 0)

    loads[2].wait()

    row = iota((WIDE, C), 0)
    inside = jnp.logical_not(
        ((row < 8) & (slab == 0)) | ((row >= WIDE - 8) & (slab == SLABS - 1))
    )

    def share_field(a, k, wide):
        both = permuted(wide, pc[...])
        fs[a, k, 0] = both[:, :HALF]
        fs[a, k, 1] = both[:, HALF:]
        fg[a, k, PEERS - 1] = fs[a, k, core]
        for m in range(1, PEERS):
            pltpu.make_async_remote_copy(
                src_ref=fs.at[a, k, (core + m % 2) % 2],
                dst_ref=fg.at[a, k, m - 1],
                send_sem=fg_send.at[a, k],
                recv_sem=fg_recv.at[a, k],
                device_id=peer_of(m),
                device_id_type=MESH,
            ).start()

    def share_grad(a, k, grad):
        chunks = permuted(grad, sel[...])
        for n in range(IMAGES):
            gs[a, k, n] = chunks[:, 128 * n : 128 * (n + 1)]
        gg[a, k, PEERS - 1] = gs[a, k, img]
        for m in range(1, PEERS):
            pltpu.make_async_remote_copy(
                src_ref=gs.at[a, k, (img + m // 2) % IMAGES],
                dst_ref=gg.at[a, k, m - 1],
                send_sem=gg_send.at[a, k],
                recv_sem=gg_recv.at[a, k],
                device_id=peer_of(m),
                device_id_type=MESH,
            ).start()

    def forward(k, carry):
        arrive(fin, fr, k, s > 0)
        x = fin[k].astype(F32)
        hidden = conv(x, w, 0, WIDE)
        hid[k] = hidden
        active = jnp.where(inside, hidden * sigmoid(hidden), 0.0).astype(BF16)

        @pl.when(s < SECTIONS - 1)
        def _():
            result = x[16 : 16 + POS] + conv(active.astype(F32), w, 1, POS)
            fout[k] = result.astype(BF16)
            spread(fout, fin, fsend, fr, k, 1, True)

        share_field(0, k, x[8 : 8 + WIDE].astype(BF16))
        share_field(1, k, active)
        return carry

    lax.fori_loop(0, CROPS, forward, 0)

    def backward(k, carry):
        arrive(gin, br, k, s < SECTIONS - 1)
        g = gin[k].astype(F32)
        grad_active = conv_t(g, w, 1, WIDE)
        hidden = hid[k]
        q = sigmoid(hidden)
        slope = q * (1.0 + hidden * (1.0 - q))
        grad_hidden = jnp.where(inside, grad_active * slope, 0.0).astype(BF16)
        wide = grad_hidden.astype(F32)
        center = g[16 : 16 + POS]
        grad_in = (center + conv_t(wide, w, 0, POS)).astype(BF16)
        gout[k] = grad_in

        @pl.when(s > 0)
        def _():
            spread(gout, gin, bsend, br, k, -1, True)

        gi_out[k] = permuted(swap, grad_in)
        share_grad(1, k, center.astype(BF16))
        share_grad(0, k, wide[8 : 8 + POS].astype(BF16))
        return carry

    lax.fori_loop(0, CROPS, backward, 0)

    acc[...] = jnp.zeros_like(acc)

    def contract(n, carry):
        a, k = n // CROPS, n % CROPS
        waited(fg.at[a, k, pl.ds(0, PEERS - 1)], fg_recv.at[a, k])
        waited(gg.at[a, k, pl.ds(0, PEERS - 1)], gg_recv.at[a, k])

        def unfold(m, carry):
            shifted = row_shifts(fg[a, k, m].astype(F32))
            for d in range(3):
                for b in range(3):
                    cc[3 * d + b, pl.ds(pl.multiple_of(m * POS, POS), POS), :] = shifted[d][
                        8 * b : 8 * b + POS
                    ].astype(BF16)
            return carry

        lax.fori_loop(0, PEERS, unfold, 0)
        grads = gg[a, k].reshape(PEERS * POS, 128).T

        def tap(t, carry):
            acc[a, t] += jnp.dot(grads, cc[t], preferred_element_type=F32)
            return carry

        lax.fori_loop(0, 9, tap, 0)
        return carry

    lax.fori_loop(0, 2 * CROPS, contract, 0)

    for t in range(3):
        for p in range(6):
            a, tap = divmod(6 * t + p, 9)
            block = acc[a, tap, 0:OUT_SHARE, :].astype(BF16)
            for half in range(2):
                pkl[2 * t + half, :, 128 * p : 128 * (p + 1)] = block[:, 128 * half : 128 * (half + 1)]
    for n in range(6):
        t, half = divmod(n, 2)
        packed = permuted(pkl[n], c6[...])
        for q in range(4):
            pk[4 * half + q, t] = packed[:, 128 * q : 128 * (q + 1)]
    for d in range(1, CHIPS):
        pltpu.make_async_remote_copy(
            src_ref=pk.at[(z + d) % CHIPS],
            dst_ref=rz.at[d - 1],
            send_sem=z_send,
            recv_sem=z_recv,
            device_id=chip_of(d),
            device_id_type=MESH,
        ).start()
    waited(rz, z_recv)
    for t in range(3):
        total = pk[z, t].astype(F32)
        for d in range(CHIPS - 1):
            total = total + rz[d, t].astype(F32)
        gk_out[t] = (total * scaling).T

    waited(rz, z_send)

    def drain(k, carry):
        @pl.when(s == 0)
        def _():
            sent(fin, edge_send, k, None)

        @pl.when(s == SECTIONS - 1)
        def _():
            sent(gin, edge_send, k, None)

        @pl.when(s < SECTIONS - 1)
        def _():
            sent(fout, fsend, k, True)

        @pl.when(s > 0)
        def _():
            sent(gout, bsend, k, True)

        for a in range(2):
            waited(fg.at[a, k, pl.ds(0, PEERS - 1)], fg_send.at[a, k])
            waited(gg.at[a, k, pl.ds(0, PEERS - 1)], gg_send.at[a, k])
        return carry

    lax.fori_loop(0, CROPS, drain, 0)


def shards(strips, kernels, cotangent):
    scaling = 1.0 / math.sqrt(IMAGES * CROPS * ROWS * COLS * SLABS)
    dma = pltpu.SemaphoreType.DMA
    vmem = pl.BlockSpec(memory_space=pltpu.VMEM)
    hbm = pl.BlockSpec(memory_space=pl.ANY)
    gk, gi = pl.pallas_call(
        lambda *refs: kernel(scaling, *refs),
        out_shape=(
            jax.ShapeDtypeStruct((3, 128, OUT_SHARE), F32),
            jax.ShapeDtypeStruct((CROPS, POS, C), BF16),
        ),
        in_specs=[hbm, hbm, hbm],
        out_specs=(vmem, vmem),
        scratch_shapes=[
            pltpu.VMEM((2, 9, C, C), BF16),
            pltpu.VMEM((CROPS, POS, C), BF16),
            pltpu.VMEM((CROPS, POS, C), BF16),
            pltpu.VMEM((CROPS, DEEP, C), BF16),
            pltpu.VMEM((CROPS, DEEP, C), BF16),
            pltpu.VMEM((CROPS, POS, C), BF16),
            pltpu.VMEM((CROPS, POS, C), BF16),
            pltpu.VMEM((CROPS, WIDE, C), F32),
            pltpu.VMEM((2, CROPS, 2, WIDE, HALF), BF16),
            pltpu.VMEM((2, CROPS, PEERS, WIDE, HALF), BF16),
            pltpu.VMEM((2, CROPS, IMAGES, POS, 128), BF16),
            pltpu.VMEM((2, CROPS, PEERS, POS, 128), BF16),
            pltpu.VMEM((9, PEERS * POS, HALF), BF16),
            pltpu.VMEM((2, 9, 128, HALF), F32),
            pltpu.VMEM((6, OUT_SHARE, 768), BF16),
            pltpu.VMEM((CHIPS, 3, OUT_SHARE, 128), BF16),
            pltpu.VMEM((CHIPS - 1, 3, OUT_SHARE, 128), BF16),
            pltpu.VMEM((C, 2 * HALF), BF16),
            pltpu.VMEM((C, 512), BF16),
            pltpu.VMEM((768, 512), BF16),
            dma((3,)),
            dma((CROPS, 3)),
            dma((CROPS, 3)),
            dma((CROPS, 3)),
            dma((CROPS, 3)),
            dma((CROPS, 3)),
            dma((2, CROPS)),
            dma((2, CROPS)),
            dma((2, CROPS)),
            dma((2, CROPS)),
            dma,
            dma,
        ],
        compiler_params=pltpu.CompilerParams(
            collective_id=0, has_side_effects=True, vmem_limit_bytes=60 * 1024 * 1024
        ),
        name="residual_step",
    )(
        strips.reshape(CROPS, POS, C),
        kernels.reshape(2, 9, C, C),
        cotangent.reshape(CROPS, POS, C),
    )
    grad_kernels = gk[:, : 6 * IN_SHARE].reshape(1, 2, 9, IN_SHARE, OUT_SHARE)
    return grad_kernels, gi.reshape(1, 1, CROPS, ROWS, COLS, C)


def solution(mesh):
    return jax.shard_map(
        shards,
        mesh=mesh,
        in_specs=(
            P("img", None, None, "slab", None),
            P("section", None, None, None, None),
            P("img", None, None, "slab", None),
        ),
        out_specs=(
            P("section", None, None, "slab", "img"),
            P("section", "img", None, None, "slab", None),
        ),
        check_vma=False,
    )
```

```python
import math

import jax
import jax.numpy as jnp
from jax import lax
from jax.experimental import pallas as pl
from jax.experimental.pallas import tpu as pltpu
from jax.sharding import PartitionSpec as P

MESH = pl.DeviceIdType.MESH
F32 = jnp.float32
BF16 = jnp.bfloat16

C = 320
SECTIONS = 4
IMAGES = 4
CROPS = 4
CHIPS = 8
SLABS = 16
ROWS = 8
COLS = 8
POS = ROWS * COLS
WIDE = POS + 16
DEEP = POS + 32
OUT_SHARE = C // IMAGES
IN_SHARE = C // SLABS
HALF = 256
PEERS = 8


def iota(shape, dim):
    return lax.broadcasted_iota(jnp.int32, shape, dim)


def onehot(cond):
    return jnp.where(cond, 1.0, 0.0).astype(BF16)


def sigmoid(v):
    return 1.0 / (1.0 + jnp.exp(-v))


def row_shifts(x):
    count = x.shape[0]
    row = iota(x.shape, 0) % ROWS
    above = jnp.where(row == 0, 0.0, pltpu.roll(x, 1, 0))
    below = jnp.where(row == ROWS - 1, 0.0, pltpu.roll(x, count - 1, 0))
    return above, x, below


def conv(x, weights, part, count):
    shifted = row_shifts(x)
    total = None
    for a in range(3):
        for b in range(3):
            lhs = shifted[a][8 * b : 8 * b + count].astype(BF16)
            term = jnp.dot(lhs, weights[part, 3 * a + b], preferred_element_type=F32)
            total = term if total is None else total + term
    return total


def kernel(
    scaling,
    strips,
    kernels,
    cotangent,
    gk_out,
    gi_out,
    w,
    wt,
    sv,
    cv,
    gi,
    fin,
    gin,
    fout,
    gout,
    hid,
    fs,
    fg,
    gs,
    gg,
    cc,
    acc,
    pkl,
    pk,
    rz,
    pc,
    sel,
    c6,
    local_sem,
    weight_sem,
    gi_sem,
    fr,
    fsend,
    br,
    bsend,
    edge_send,
    fg_recv,
    fg_send,
    gg_recv,
    gg_send,
    z_recv,
    z_send,
):
    s = lax.axis_index("section")
    slab = lax.axis_index("slab")
    img = lax.axis_index("img")
    z = slab // 2
    core = slab % 2
    has_left = slab > 0
    has_right = slab < SLABS - 1

    loads = [
        pltpu.make_async_copy(strips, sv, local_sem.at[0]),
        pltpu.make_async_copy(cotangent, cv, local_sem.at[1]),
    ]
    for part in range(2):
        for tap in range(9):
            loads.append(
                pltpu.make_async_copy(
                    kernels.at[part, tap], w.at[part, tap], weight_sem.at[part, tap]
                )
            )
    for load in loads:
        load.start()

    @pl.when(slab == 0)
    def _():
        for buf in (fin, gin):
            buf[:, 0:16, :] = jnp.zeros((CROPS, 16, C), BF16)

    @pl.when(slab == SLABS - 1)
    def _():
        for buf in (fin, gin):
            buf[:, DEEP - 16 : DEEP, :] = jnp.zeros((CROPS, 16, C), BF16)

    barrier = pltpu.get_barrier_semaphore()

    def greet(where):
        pl.semaphore_signal(barrier, inc=1, device_id=where, device_id_type=MESH)

    def peer_of(m):
        return (s, 2 * z + (core + m % 2) % 2, (img + m // 2) % IMAGES)

    def chip_of(d):
        return (s, 2 * ((z + d) % CHIPS) + core, img)

    greeted = jnp.int32(0)
    for ds in (-1, 0, 1):
        for dj in (-1, 0, 1):
            if ds == 0 and dj == 0:
                continue
            ok = (s + ds >= 0) & (s + ds < SECTIONS) & (slab + dj >= 0) & (slab + dj < SLABS)

            @pl.when(ok)
            def _():
                greet((s + ds, slab + dj, img))

            greeted = greeted + jnp.where(ok, 1, 0)
    for m in range(1, PEERS):
        greet(peer_of(m))
    for d in range(1, CHIPS):
        greet(chip_of(d))
    i, j = iota((POS, POS), 0), iota((POS, POS), 1)
    swap = onehot((i // 8 == j % 8) & (i % 8 == j // 8))
    i, j = iota((C, 2 * HALF), 0), iota((C, 2 * HALF), 1)
    lane = j % 32
    pc[...] = onehot((lane < IN_SHARE) & (i == IN_SHARE * (2 * ((j % HALF) // 32) + j // HALF) + lane))
    lane = j % 128
    sel[...] = onehot((lane < OUT_SHARE) & (i == OUT_SHARE * (j // 128) + lane))
    i, j = iota((768, 512), 0), iota((768, 512), 1)
    lane = i % 32
    c6[...] = onehot(
        (lane < IN_SHARE)
        & ((i % 128) // 32 == j // 128)
        & (j % 128 == IN_SHARE * (i // 128) + lane)
    )

    acc[...] = jnp.zeros_like(acc)
    pl.semaphore_wait(barrier, greeted + (PEERS - 1) + (CHIPS - 1))

    def permuted(x, matrix):
        return jnp.dot(x, matrix, preferred_element_type=F32).astype(BF16)

    def spread(src, dst, send, recv, k, ds, center):
        base = 16 if src is dst else 0

        @pl.when(has_right)
        def _():
            pltpu.make_async_remote_copy(
                src_ref=src.at[k, pl.ds(base + POS - 16, 16)],
                dst_ref=dst.at[k, pl.ds(0, 16)],
                send_sem=send.at[k, 2],
                recv_sem=recv.at[k, 0],
                device_id=(s + ds, slab + 1, img),
                device_id_type=MESH,
            ).start()

        @pl.when(has_left)
        def _():
            pltpu.make_async_remote_copy(
                src_ref=src.at[k, pl.ds(base, 16)],
                dst_ref=dst.at[k, pl.ds(DEEP - 16, 16)],
                send_sem=send.at[k, 0],
                recv_sem=recv.at[k, 2],
                device_id=(s + ds, slab - 1, img),
                device_id_type=MESH,
            ).start()

        if center:
            pltpu.make_async_remote_copy(
                src_ref=src.at[k],
                dst_ref=dst.at[k, pl.ds(16, POS)],
                send_sem=send.at[k, 1],
                recv_sem=recv.at[k, 1],
                device_id=(s + ds, slab, img),
                device_id_type=MESH,
            ).start()

    def waited(ref, sem):
        pltpu.make_async_copy(ref, ref, sem).wait()

    def arrive(dst, recv, k, center):
        @pl.when(center)
        def _():
            waited(dst.at[k, pl.ds(16, POS)], recv.at[k, 1])

        @pl.when(has_left)
        def _():
            waited(dst.at[k, pl.ds(0, 16)], recv.at[k, 0])

        @pl.when(has_right)
        def _():
            waited(dst.at[k, pl.ds(DEEP - 16, 16)], recv.at[k, 2])

    def sent(src, send, k, center):
        base = 16 if center is None else 0
        if center is not None:
            waited(src.at[k], send.at[k, 1])

        @pl.when(has_right)
        def _():
            waited(src.at[k, pl.ds(base + POS - 16, 16)], send.at[k, 2])

        @pl.when(has_left)
        def _():
            waited(src.at[k, pl.ds(base, 16)], send.at[k, 0])

    loads[0].wait()
    loads[1].wait()

    @pl.when(s == 0)
    def _():
        def step(k, carry):
            fin[k, 16 : 16 + POS, :] = permuted(swap, sv[k])
            spread(fin, fin, edge_send, fr, k, 0, False)
            return carry

        lax.fori_loop(0, CROPS, step, 0)

    @pl.when(s == SECTIONS - 1)
    def _():
        def step(k, carry):
            gin[k, 16 : 16 + POS, :] = permuted(swap, cv[k])
            spread(gin, gin, edge_send, br, k, 0, False)
            return carry

        lax.fori_loop(0, CROPS, step, 0)

    for load in loads[2:]:
        load.wait()

    def transpose_weights():
        def step(n, carry):
            part, tap = n // 9, n % 9
            wt[part, 8 - tap] = w[part, tap].T
            return carry

        lax.fori_loop(0, 18, step, 0)

    pl.when(s > 0)(transpose_weights)

    row = iota((WIDE, C), 0)
    inside = jnp.logical_not(
        ((row < 8) & (slab == 0)) | ((row >= WIDE - 8) & (slab == SLABS - 1))
    )

    def share_field(a, k, wide):
        both = permuted(wide, pc[...])
        fs[a, k, 0] = both[:, :HALF]
        fs[a, k, 1] = both[:, HALF:]
        fg[a, k, PEERS - 1] = fs[a, k, core]
        for m in range(1, PEERS):
            pltpu.make_async_remote_copy(
                src_ref=fs.at[a, k, (core + m % 2) % 2],
                dst_ref=fg.at[a, k, m - 1],
                send_sem=fg_send.at[a, k],
                recv_sem=fg_recv.at[a, k],
                device_id=peer_of(m),
                device_id_type=MESH,
            ).start()

    def share_grad(a, k, grad):
        chunks = permuted(grad, sel[...])
        for n in range(IMAGES):
            gs[a, k, n] = chunks[:, 128 * n : 128 * (n + 1)]
        gg[a, k, PEERS - 1] = gs[a, k, img]
        for m in range(1, PEERS):
            pltpu.make_async_remote_copy(
                src_ref=gs.at[a, k, (img + m // 2) % IMAGES],
                dst_ref=gg.at[a, k, m - 1],
                send_sem=gg_send.at[a, k],
                recv_sem=gg_recv.at[a, k],
                device_id=peer_of(m),
                device_id_type=MESH,
            ).start()

    def forward(k, carry):
        arrive(fin, fr, k, s > 0)
        x = fin[k].astype(F32)
        hidden = conv(x, w, 0, WIDE)
        hid[k] = hidden
        active = jnp.where(inside, hidden * sigmoid(hidden), 0.0).astype(BF16)

        @pl.when(s < SECTIONS - 1)
        def _():
            result = x[16 : 16 + POS] + conv(active.astype(F32), w, 1, POS)
            fout[k] = result.astype(BF16)
            spread(fout, fin, fsend, fr, k, 1, True)

        share_field(0, k, x[8 : 8 + WIDE].astype(BF16))
        share_field(1, k, active)
        return carry

    lax.fori_loop(0, CROPS, forward, 0)
    pl.when(s == 0)(transpose_weights)

    def backward(k):
        arrive(gin, br, k, s < SECTIONS - 1)
        g = gin[k].astype(F32)
        grad_active = conv(g, wt, 1, WIDE)
        hidden = hid[k]
        q = sigmoid(hidden)
        slope = q * (1.0 + hidden * (1.0 - q))
        grad_hidden = jnp.where(inside, grad_active * slope, 0.0).astype(BF16)
        wide = grad_hidden.astype(F32)
        center = g[16 : 16 + POS]
        grad_in = (center + conv(wide, wt, 0, POS)).astype(BF16)
        gout[k] = grad_in

        @pl.when(s > 0)
        def _():
            spread(gout, gin, bsend, br, k, -1, True)

        gi[k] = permuted(swap, grad_in)
        pltpu.make_async_copy(gi.at[k], gi_out.at[k], gi_sem.at[k]).start()
        share_grad(1, k, center.astype(BF16))
        share_grad(0, k, wide[8 : 8 + POS].astype(BF16))

    def unfold(k):
        for a in range(2):
            waited(fg.at[a, k, pl.ds(0, PEERS - 1)], fg_recv.at[a, k])

            def source(m, carry):
                shifted = row_shifts(fg[a, k, m].astype(F32))
                for d in range(3):
                    for b in range(3):
                        cc[a, k, 3 * d + b, pl.ds(pl.multiple_of(m * POS, POS), POS), :] = shifted[d][
                            8 * b : 8 * b + POS
                        ].astype(BF16)
                return carry

            lax.fori_loop(0, PEERS, source, 0)

    def contract(k):
        for a in range(2):
            waited(gg.at[a, k, pl.ds(0, PEERS - 1)], gg_recv.at[a, k])
            grads = gg[a, k].reshape(PEERS * POS, 128).T

            def tap(t, carry):
                acc[a, t] += jnp.dot(grads, cc[a, k, t], preferred_element_type=F32)
                return carry

            lax.fori_loop(0, 9, tap, 0)

    last = CROPS - 1
    early = s < 2

    def middle(i, carry):
        unfolding = jnp.where(early, i < last, i >= CROPS)

        @pl.when(unfolding)
        def _():
            unfold(jnp.where(early, i, i - CROPS))

        @pl.when(jnp.logical_not(unfolding))
        def _():
            backward(jnp.where(early, i - last, i))

        return carry

    lax.fori_loop(0, CROPS + last, middle, 0)

    def finish(k, carry):
        @pl.when(k == last)
        def _():
            unfold(k)

        contract(k)
        return carry

    lax.fori_loop(0, CROPS, finish, 0)

    for t in range(3):
        for p in range(6):
            a, tap = divmod(6 * t + p, 9)
            block = acc[a, tap, 0:OUT_SHARE, :].astype(BF16)
            for half in range(2):
                pkl[2 * t + half, :, 128 * p : 128 * (p + 1)] = block[:, 128 * half : 128 * (half + 1)]
    for pair in range(2):
        packed = permuted(
            pkl[...].reshape(6 * OUT_SHARE, 768), c6[:, 256 * pair : 256 * (pair + 1)]
        ).reshape(6, OUT_SHARE, 256)
        for t in range(3):
            for half in range(2):
                for q in range(2):
                    pk[4 * half + 2 * pair + q, t] = packed[2 * t + half, :, 128 * q : 128 * (q + 1)]
    for d in range(1, CHIPS):
        pltpu.make_async_remote_copy(
            src_ref=pk.at[(z + d) % CHIPS],
            dst_ref=rz.at[d - 1],
            send_sem=z_send,
            recv_sem=z_recv,
            device_id=chip_of(d),
            device_id_type=MESH,
        ).start()
    waited(rz, z_recv)
    for t in range(3):
        total = pk[z, t].astype(F32)
        for d in range(CHIPS - 1):
            total = total + rz[d, t].astype(F32)
        flipped = (total * scaling).T
        for p in range(6):
            a, tap = divmod(6 * t + p, 9)
            gk_out[a, tap] = flipped[IN_SHARE * p : IN_SHARE * (p + 1)]

    waited(rz, z_send)

    def drain(k, carry):
        pltpu.make_async_copy(gi.at[k], gi_out.at[k], gi_sem.at[k]).wait()

        @pl.when(s == 0)
        def _():
            sent(fin, edge_send, k, None)

        @pl.when(s == SECTIONS - 1)
        def _():
            sent(gin, edge_send, k, None)

        @pl.when(s < SECTIONS - 1)
        def _():
            sent(fout, fsend, k, True)

        @pl.when(s > 0)
        def _():
            sent(gout, bsend, k, True)

        for a in range(2):
            waited(fg.at[a, k, pl.ds(0, PEERS - 1)], fg_send.at[a, k])
            waited(gg.at[a, k, pl.ds(0, PEERS - 1)], gg_send.at[a, k])
        return carry

    lax.fori_loop(0, CROPS, drain, 0)


def shards(strips, kernels, cotangent):
    scaling = 1.0 / math.sqrt(IMAGES * CROPS * ROWS * COLS * SLABS)
    dma = pltpu.SemaphoreType.DMA
    vmem = pl.BlockSpec(memory_space=pltpu.VMEM)
    hbm = pl.BlockSpec(memory_space=pl.ANY)
    gk, gi = pl.pallas_call(
        lambda *refs: kernel(scaling, *refs),
        out_shape=(
            jax.ShapeDtypeStruct((2, 9, IN_SHARE, OUT_SHARE), F32),
            jax.ShapeDtypeStruct((CROPS, POS, C), BF16),
        ),
        in_specs=[hbm, hbm, hbm],
        out_specs=(vmem, hbm),
        scratch_shapes=[
            pltpu.VMEM((2, 9, C, C), BF16),
            pltpu.VMEM((2, 9, C, C), BF16),
            pltpu.VMEM((CROPS, POS, C), BF16),
            pltpu.VMEM((CROPS, POS, C), BF16),
            pltpu.VMEM((CROPS, POS, C), BF16),
            pltpu.VMEM((CROPS, DEEP, C), BF16),
            pltpu.VMEM((CROPS, DEEP, C), BF16),
            pltpu.VMEM((CROPS, POS, C), BF16),
            pltpu.VMEM((CROPS, POS, C), BF16),
            pltpu.VMEM((CROPS, WIDE, C), F32),
            pltpu.VMEM((2, CROPS, 2, WIDE, HALF), BF16),
            pltpu.VMEM((2, CROPS, PEERS, WIDE, HALF), BF16),
            pltpu.VMEM((2, CROPS, IMAGES, POS, 128), BF16),
            pltpu.VMEM((2, CROPS, PEERS, POS, 128), BF16),
            pltpu.VMEM((2, CROPS, 9, PEERS * POS, HALF), BF16),
            pltpu.VMEM((2, 9, 128, HALF), F32),
            pltpu.VMEM((6, OUT_SHARE, 768), BF16),
            pltpu.VMEM((CHIPS, 3, OUT_SHARE, 128), BF16),
            pltpu.VMEM((CHIPS - 1, 3, OUT_SHARE, 128), BF16),
            pltpu.VMEM((C, 2 * HALF), BF16),
            pltpu.VMEM((C, 512), BF16),
            pltpu.VMEM((768, 512), BF16),
            dma((2,)),
            dma((2, 9)),
            dma((CROPS,)),
            dma((CROPS, 3)),
            dma((CROPS, 3)),
            dma((CROPS, 3)),
            dma((CROPS, 3)),
            dma((CROPS, 3)),
            dma((2, CROPS)),
            dma((2, CROPS)),
            dma((2, CROPS)),
            dma((2, CROPS)),
            dma,
            dma,
        ],
        compiler_params=pltpu.CompilerParams(
            collective_id=0, has_side_effects=True, vmem_limit_bytes=60 * 1024 * 1024
        ),
        name="residual_step",
    )(
        strips.reshape(CROPS, POS, C),
        kernels.reshape(2, 9, C, C),
        cotangent.reshape(CROPS, POS, C),
    )
    return gk[None], gi.reshape(1, 1, CROPS, ROWS, COLS, C)


def solution(mesh):
    return jax.shard_map(
        shards,
        mesh=mesh,
        in_specs=(
            P("img", None, None, "slab", None),
            P("section", None, None, None, None),
            P("img", None, None, "slab", None),
        ),
        out_specs=(
            P("section", None, None, "slab", "img"),
            P("section", "img", None, None, "slab", None),
        ),
        check_vma=False,
    )
```

```python
import math

import jax
import jax.numpy as jnp
from jax import lax
from jax.experimental import pallas as pl
from jax.experimental.pallas import tpu as pltpu
from jax.sharding import PartitionSpec as P

MESH = pl.DeviceIdType.MESH
F32 = jnp.float32
BF16 = jnp.bfloat16

C = 320
SECTIONS = 4
IMAGES = 4
CROPS = 4
CHIPS = 8
SLABS = 16
ROWS = 8
COLS = 8
POS = ROWS * COLS
WIDE = POS + 16
DEEP = POS + 32
OUT_SHARE = C // IMAGES
IN_SHARE = C // SLABS
HALF = 256
PEERS = 8


def iota(shape, dim):
    return lax.broadcasted_iota(jnp.int32, shape, dim)


def onehot(cond):
    return jnp.where(cond, 1.0, 0.0).astype(BF16)


def sigmoid(v):
    return 1.0 / (1.0 + jnp.exp(-v))


def row_shifts(x):
    count = x.shape[0]
    row = iota(x.shape, 0) % ROWS
    above = jnp.where(row == 0, 0.0, pltpu.roll(x, 1, 0))
    below = jnp.where(row == ROWS - 1, 0.0, pltpu.roll(x, count - 1, 0))
    return above, x, below


def conv(x, weights, part, count):
    shifted = row_shifts(x)
    total = None
    for a in range(3):
        for b in range(3):
            lhs = shifted[a][8 * b : 8 * b + count].astype(BF16)
            term = jnp.dot(lhs, weights[part, 3 * a + b], preferred_element_type=F32)
            total = term if total is None else total + term
    return total


def kernel(
    scaling,
    strips,
    kernels,
    cotangent,
    gk_out,
    gi_out,
    w,
    wt,
    sv,
    cv,
    gi,
    fin,
    gin,
    fout,
    gout,
    hid,
    raw,
    fs,
    fg,
    gs,
    gg,
    cc,
    acc,
    pkl,
    pk,
    rz,
    pc,
    sel,
    c6,
    local_sem,
    weight_sem,
    gi_sem,
    fr,
    fsend,
    br,
    bsend,
    edge_send,
    raw_recv,
    raw_send,
    fg_recv,
    fg_send,
    gg_recv,
    gg_send,
    gr_recv,
    gr_send,
    z_recv,
    z_send,
):
    s = lax.axis_index("section")
    slab = lax.axis_index("slab")
    img = lax.axis_index("img")
    z = slab // 2
    core = slab % 2
    has_left = slab > 0
    has_right = slab < SLABS - 1

    loads = [
        pltpu.make_async_copy(strips, sv, local_sem.at[0]),
        pltpu.make_async_copy(cotangent, cv, local_sem.at[1]),
    ]
    for part in range(2):
        for tap in range(9):
            loads.append(
                pltpu.make_async_copy(
                    kernels.at[part, tap], w.at[part, tap], weight_sem.at[part, tap]
                )
            )
    for load in loads:
        load.start()

    @pl.when(slab == 0)
    def _():
        for buf in (fin, gin):
            buf[:, 0:16, :] = jnp.zeros((CROPS, 16, C), BF16)

    @pl.when(slab == SLABS - 1)
    def _():
        for buf in (fin, gin):
            buf[:, DEEP - 16 : DEEP, :] = jnp.zeros((CROPS, 16, C), BF16)

    barrier = pltpu.get_barrier_semaphore()

    def greet(where):
        pl.semaphore_signal(barrier, inc=1, device_id=where, device_id_type=MESH)

    def image_of(d):
        return (s, slab, (img + d) % IMAGES)

    partner = (s, 2 * z + 1 - core, img)

    def chip_of(d):
        return (s, 2 * ((z + d) % CHIPS) + core, img)

    greeted = jnp.int32(0)
    for ds in (-1, 0, 1):
        for dj in (-1, 0, 1):
            if ds == 0 and dj == 0:
                continue
            ok = (s + ds >= 0) & (s + ds < SECTIONS) & (slab + dj >= 0) & (slab + dj < SLABS)

            @pl.when(ok)
            def _():
                greet((s + ds, slab + dj, img))

            greeted = greeted + jnp.where(ok, 1, 0)
    for d in range(1, IMAGES):
        greet(image_of(d))
    greet(partner)
    for d in range(1, CHIPS):
        greet(chip_of(d))
    i, j = iota((POS, POS), 0), iota((POS, POS), 1)
    swap = onehot((i // 8 == j % 8) & (i % 8 == j // 8))
    i, j = iota((C, 2 * HALF), 0), iota((C, 2 * HALF), 1)
    lane = j % 32
    side = (j // HALF + core) % 2
    pc[...] = onehot((lane < IN_SHARE) & (i == IN_SHARE * (2 * ((j % HALF) // 32) + side) + lane))
    lane = j % 128
    owner = (j // 128 + img) % IMAGES
    sel[...] = onehot((lane < OUT_SHARE) & (i == OUT_SHARE * owner + lane))
    i, j = iota((768, 512), 0), iota((768, 512), 1)
    lane = i % 32
    c6[...] = onehot(
        (lane < IN_SHARE)
        & ((i % 128) // 32 == j // 128)
        & (j % 128 == IN_SHARE * (i // 128) + lane)
    )

    acc[...] = jnp.zeros_like(acc)
    pl.semaphore_wait(barrier, greeted + IMAGES + (CHIPS - 1))

    def permuted(x, matrix):
        return jnp.dot(x, matrix, preferred_element_type=F32).astype(BF16)

    def spread(src, dst, send, recv, k, ds, center):
        base = 16 if src is dst else 0

        @pl.when(has_right)
        def _():
            pltpu.make_async_remote_copy(
                src_ref=src.at[k, pl.ds(base + POS - 16, 16)],
                dst_ref=dst.at[k, pl.ds(0, 16)],
                send_sem=send.at[k, 2],
                recv_sem=recv.at[k, 0],
                device_id=(s + ds, slab + 1, img),
                device_id_type=MESH,
            ).start()

        @pl.when(has_left)
        def _():
            pltpu.make_async_remote_copy(
                src_ref=src.at[k, pl.ds(base, 16)],
                dst_ref=dst.at[k, pl.ds(DEEP - 16, 16)],
                send_sem=send.at[k, 0],
                recv_sem=recv.at[k, 2],
                device_id=(s + ds, slab - 1, img),
                device_id_type=MESH,
            ).start()

        if center:
            pltpu.make_async_remote_copy(
                src_ref=src.at[k],
                dst_ref=dst.at[k, pl.ds(16, POS)],
                send_sem=send.at[k, 1],
                recv_sem=recv.at[k, 1],
                device_id=(s + ds, slab, img),
                device_id_type=MESH,
            ).start()

    def waited(ref, sem):
        pltpu.make_async_copy(ref, ref, sem).wait()

    def arrive(dst, recv, k, center):
        @pl.when(center)
        def _():
            waited(dst.at[k, pl.ds(16, POS)], recv.at[k, 1])

        @pl.when(has_left)
        def _():
            waited(dst.at[k, pl.ds(0, 16)], recv.at[k, 0])

        @pl.when(has_right)
        def _():
            waited(dst.at[k, pl.ds(DEEP - 16, 16)], recv.at[k, 2])

    def sent(src, send, k, center):
        base = 16 if center is None else 0
        if center is not None:
            waited(src.at[k], send.at[k, 1])

        @pl.when(has_right)
        def _():
            waited(src.at[k, pl.ds(base + POS - 16, 16)], send.at[k, 2])

        @pl.when(has_left)
        def _():
            waited(src.at[k, pl.ds(base, 16)], send.at[k, 0])

    loads[0].wait()
    loads[1].wait()

    @pl.when(s == 0)
    def _():
        def step(k, carry):
            fin[k, 16 : 16 + POS, :] = permuted(swap, sv[k])
            spread(fin, fin, edge_send, fr, k, 0, False)
            return carry

        lax.fori_loop(0, CROPS, step, 0)

    @pl.when(s == SECTIONS - 1)
    def _():
        def step(k, carry):
            gin[k, 16 : 16 + POS, :] = permuted(swap, cv[k])
            spread(gin, gin, edge_send, br, k, 0, False)
            return carry

        lax.fori_loop(0, CROPS, step, 0)

    for load in loads[2:]:
        load.wait()

    def transpose_weights():
        def step(n, carry):
            part, tap = n // 9, n % 9
            wt[part, 8 - tap] = w[part, tap].T
            return carry

        lax.fori_loop(0, 18, step, 0)

    pl.when(s > 0)(transpose_weights)

    row = iota((WIDE, C), 0)
    inside = jnp.logical_not(
        ((row < 8) & (slab == 0)) | ((row >= WIDE - 8) & (slab == SLABS - 1))
    )

    def share_field(a, k, wide):
        raw[a, k, IMAGES - 1] = wide
        for d in range(1, IMAGES):
            pltpu.make_async_remote_copy(
                src_ref=raw.at[a, k, IMAGES - 1],
                dst_ref=raw.at[a, k, d - 1],
                send_sem=raw_send.at[a, k],
                recv_sem=raw_recv.at[a, k],
                device_id=image_of(d),
                device_id_type=MESH,
            ).start()

    def relay_field(k):
        for a in range(2):
            waited(raw.at[a, k, pl.ds(0, IMAGES - 1)], raw_recv.at[a, k])
            for n in range(IMAGES):
                both = permuted(raw[a, k, n], pc[...])
                fg[a, k, n] = both[:, :HALF]
                fs[a, k, n] = both[:, HALF:]
            pltpu.make_async_remote_copy(
                src_ref=fs.at[a, k],
                dst_ref=fg.at[a, k, pl.ds(IMAGES, IMAGES)],
                send_sem=fg_send.at[a, k],
                recv_sem=fg_recv.at[a, k],
                device_id=partner,
                device_id_type=MESH,
            ).start()

    def share_grad(a, k, grad):
        chunks = permuted(grad, sel[...])
        gg[a, k, IMAGES - 1] = chunks[:, :128]
        for d in range(1, IMAGES):
            gs[a, k, d - 1] = chunks[:, 128 * d : 128 * (d + 1)]
            pltpu.make_async_remote_copy(
                src_ref=gs.at[a, k, d - 1],
                dst_ref=gg.at[a, k, d - 1],
                send_sem=gg_send.at[a, k],
                recv_sem=gg_recv.at[a, k],
                device_id=image_of(d),
                device_id_type=MESH,
            ).start()

    def relay_grad(a, k):
        waited(gg.at[a, k, pl.ds(0, IMAGES - 1)], gg_recv.at[a, k])
        pltpu.make_async_remote_copy(
            src_ref=gg.at[a, k, pl.ds(0, IMAGES)],
            dst_ref=gg.at[a, k, pl.ds(IMAGES, IMAGES)],
            send_sem=gr_send.at[a, k],
            recv_sem=gr_recv.at[a, k],
            device_id=partner,
            device_id_type=MESH,
        ).start()

    def forward(k, carry):
        arrive(fin, fr, k, s > 0)
        x = fin[k].astype(F32)
        hidden = conv(x, w, 0, WIDE)
        hid[k] = hidden
        active = jnp.where(inside, hidden * sigmoid(hidden), 0.0).astype(BF16)

        @pl.when(s < SECTIONS - 1)
        def _():
            result = x[16 : 16 + POS] + conv(active.astype(F32), w, 1, POS)
            fout[k] = result.astype(BF16)
            spread(fout, fin, fsend, fr, k, 1, True)

        share_field(0, k, x[8 : 8 + WIDE].astype(BF16))
        share_field(1, k, active)
        return carry

    lax.fori_loop(0, CROPS, forward, 0)
    pl.when(s == 0)(transpose_weights)

    def backward(k):
        arrive(gin, br, k, s < SECTIONS - 1)
        g = gin[k].astype(F32)
        grad_active = conv(g, wt, 1, WIDE)
        hidden = hid[k]
        q = sigmoid(hidden)
        slope = q * (1.0 + hidden * (1.0 - q))
        grad_hidden = jnp.where(inside, grad_active * slope, 0.0).astype(BF16)
        wide = grad_hidden.astype(F32)
        center = g[16 : 16 + POS]
        grad_in = (center + conv(wide, wt, 0, POS)).astype(BF16)
        gout[k] = grad_in

        @pl.when(s > 0)
        def _():
            spread(gout, gin, bsend, br, k, -1, True)

        gi[k] = permuted(swap, grad_in)
        pltpu.make_async_copy(gi.at[k], gi_out.at[k], gi_sem.at[k]).start()
        share_grad(1, k, center.astype(BF16))
        share_grad(0, k, wide[8 : 8 + POS].astype(BF16))

    def unfold(k):
        for a in range(2):
            waited(fg.at[a, k, pl.ds(IMAGES, IMAGES)], fg_recv.at[a, k])

            def source(m, carry):
                shifted = row_shifts(fg[a, k, m].astype(F32))
                for d in range(3):
                    for b in range(3):
                        cc[a, k, 3 * d + b, pl.ds(pl.multiple_of(m * POS, POS), POS), :] = shifted[d][
                            8 * b : 8 * b + POS
                        ].astype(BF16)
                return carry

            lax.fori_loop(0, PEERS, source, 0)

    def contract(a, k):
        waited(gg.at[a, k, pl.ds(IMAGES, IMAGES)], gr_recv.at[a, k])
        grads = gg[a, k].reshape(PEERS * POS, 128).T[:OUT_SHARE]
        for t in range(9):
            acc[a, t] += jnp.dot(grads, cc[a, k, t], preferred_element_type=F32)

    early = s < 2

    def unfold_step(n):
        @pl.when(n < CROPS)
        def _():
            relay_field(n)

        @pl.when(n > 0)
        def _():
            unfold(n - 1)

    def middle(i, carry):
        unfolding = jnp.where(early, i <= CROPS, i >= CROPS)

        @pl.when(unfolding)
        def _():
            unfold_step(jnp.where(early, i, i - CROPS))

        @pl.when(jnp.logical_not(unfolding))
        def _():
            backward(jnp.where(early, i - CROPS - 1, i))

        return carry

    lax.fori_loop(0, 2 * CROPS + 1, middle, 0)

    def pack(t):
        for p in range(6):
            a, tap = divmod(6 * t + p, 9)
            block = acc[a, tap].astype(BF16)
            for half in range(2):
                pkl[t, half, :, 128 * p : 128 * (p + 1)] = block[:, 128 * half : 128 * (half + 1)]
        packed = permuted(pkl[t].reshape(2 * OUT_SHARE, 768), c6[...]).reshape(2, OUT_SHARE, 512)
        for half in range(2):
            for q in range(4):
                pk[t, 4 * half + q] = packed[half, :, 128 * q : 128 * (q + 1)]
        for d in range(1, CHIPS):
            pltpu.make_async_remote_copy(
                src_ref=pk.at[t, (z + d) % CHIPS],
                dst_ref=rz.at[t, d - 1],
                send_sem=z_send.at[t],
                recv_sem=z_recv.at[t],
                device_id=chip_of(d),
                device_id_type=MESH,
            ).start()

    last = CROPS - 1

    def hand_over(k, carry):
        relay_grad(1, k)
        relay_grad(0, k)
        return carry

    lax.fori_loop(0, last, hand_over, 0)

    def tail(i, carry):
        @pl.when(i == 3)
        def _():
            relay_grad(1, last)

        @pl.when(i == 4)
        def _():
            relay_grad(0, last)

        upper = (i < 3) | (i == 5)
        crop = jnp.where(i < 3, i, jnp.where(i < 5, i - 3, jnp.where(i == 5, last, i - 4)))
        contract(jnp.where(upper, 1, 0), crop)

        @pl.when(i == 5)
        def _():
            pack(2)

        return carry

    lax.fori_loop(0, 2 * CROPS, tail, 0)
    pack(1)
    pack(0)

    for t in (2, 1, 0):
        waited(rz.at[t], z_recv.at[t])
        total = pk[t, z].astype(F32)
        for d in range(CHIPS - 1):
            total = total + rz[t, d].astype(F32)
        flipped = (total * scaling).T
        for p in range(6):
            a, tap = divmod(6 * t + p, 9)
            gk_out[a, tap] = flipped[IN_SHARE * p : IN_SHARE * (p + 1)]

    for t in range(3):
        waited(rz.at[t], z_send.at[t])

    def drain(k, carry):
        pltpu.make_async_copy(gi.at[k], gi_out.at[k], gi_sem.at[k]).wait()

        @pl.when(s == 0)
        def _():
            sent(fin, edge_send, k, None)

        @pl.when(s == SECTIONS - 1)
        def _():
            sent(gin, edge_send, k, None)

        @pl.when(s < SECTIONS - 1)
        def _():
            sent(fout, fsend, k, True)

        @pl.when(s > 0)
        def _():
            sent(gout, bsend, k, True)

        for a in range(2):
            waited(raw.at[a, k, pl.ds(0, IMAGES - 1)], raw_send.at[a, k])
            waited(fs.at[a, k], fg_send.at[a, k])
            waited(gs.at[a, k], gg_send.at[a, k])
            waited(gg.at[a, k, pl.ds(0, IMAGES)], gr_send.at[a, k])
        return carry

    lax.fori_loop(0, CROPS, drain, 0)


def shards(strips, kernels, cotangent):
    scaling = 1.0 / math.sqrt(IMAGES * CROPS * ROWS * COLS * SLABS)
    dma = pltpu.SemaphoreType.DMA
    vmem = pl.BlockSpec(memory_space=pltpu.VMEM)
    hbm = pl.BlockSpec(memory_space=pl.ANY)
    gk, gi = pl.pallas_call(
        lambda *refs: kernel(scaling, *refs),
        out_shape=(
            jax.ShapeDtypeStruct((2, 9, IN_SHARE, OUT_SHARE), F32),
            jax.ShapeDtypeStruct((CROPS, POS, C), BF16),
        ),
        in_specs=[hbm, hbm, hbm],
        out_specs=(vmem, hbm),
        scratch_shapes=[
            pltpu.VMEM((2, 9, C, C), BF16),
            pltpu.VMEM((2, 9, C, C), BF16),
            pltpu.VMEM((CROPS, POS, C), BF16),
            pltpu.VMEM((CROPS, POS, C), BF16),
            pltpu.VMEM((CROPS, POS, C), BF16),
            pltpu.VMEM((CROPS, DEEP, C), BF16),
            pltpu.VMEM((CROPS, DEEP, C), BF16),
            pltpu.VMEM((CROPS, POS, C), BF16),
            pltpu.VMEM((CROPS, POS, C), BF16),
            pltpu.VMEM((CROPS, WIDE, C), F32),
            pltpu.VMEM((2, CROPS, IMAGES, WIDE, C), BF16),
            pltpu.VMEM((2, CROPS, IMAGES, WIDE, HALF), BF16),
            pltpu.VMEM((2, CROPS, PEERS, WIDE, HALF), BF16),
            pltpu.VMEM((2, CROPS, IMAGES - 1, POS, 128), BF16),
            pltpu.VMEM((2, CROPS, PEERS, POS, 128), BF16),
            pltpu.VMEM((2, CROPS, 9, PEERS * POS, HALF), BF16),
            pltpu.VMEM((2, 9, OUT_SHARE, HALF), F32),
            pltpu.VMEM((3, 2, OUT_SHARE, 768), BF16),
            pltpu.VMEM((3, CHIPS, OUT_SHARE, 128), BF16),
            pltpu.VMEM((3, CHIPS - 1, OUT_SHARE, 128), BF16),
            pltpu.VMEM((C, 2 * HALF), BF16),
            pltpu.VMEM((C, 512), BF16),
            pltpu.VMEM((768, 512), BF16),
            dma((2,)),
            dma((2, 9)),
            dma((CROPS,)),
            dma((CROPS, 3)),
            dma((CROPS, 3)),
            dma((CROPS, 3)),
            dma((CROPS, 3)),
            dma((CROPS, 3)),
            dma((2, CROPS)),
            dma((2, CROPS)),
            dma((2, CROPS)),
            dma((2, CROPS)),
            dma((2, CROPS)),
            dma((2, CROPS)),
            dma((2, CROPS)),
            dma((2, CROPS)),
            dma((3,)),
            dma((3,)),
        ],
        compiler_params=pltpu.CompilerParams(
            collective_id=0, has_side_effects=True, vmem_limit_bytes=60 * 1024 * 1024
        ),
        name="residual_step",
    )(
        strips.reshape(CROPS, POS, C),
        kernels.reshape(2, 9, C, C),
        cotangent.reshape(CROPS, POS, C),
    )
    return gk[None], gi.reshape(1, 1, CROPS, ROWS, COLS, C)


def solution(mesh):
    return jax.shard_map(
        shards,
        mesh=mesh,
        in_specs=(
            P("img", None, None, "slab", None),
            P("section", None, None, None, None),
            P("img", None, None, "slab", None),
        ),
        out_specs=(
            P("section", None, None, "slab", "img"),
            P("section", "img", None, None, "slab", None),
        ),
        check_vma=False,
    )
```

```python
import math

import jax
import jax.numpy as jnp
from jax import lax
from jax.experimental import pallas as pl
from jax.experimental.pallas import tpu as pltpu
from jax.sharding import PartitionSpec as P

MESH = pl.DeviceIdType.MESH
F32 = jnp.float32
BF16 = jnp.bfloat16

C = 320
SECTIONS = 4
IMAGES = 4
CROPS = 4
CHIPS = 8
SLABS = 16
ROWS = 8
COLS = 8
POS = ROWS * COLS
WIDE = POS + 16
DEEP = POS + 32
OUT_SHARE = C // IMAGES
IN_SHARE = C // SLABS
HALF = 256
PEERS = 8


def iota(shape, dim):
    return lax.broadcasted_iota(jnp.int32, shape, dim)


def onehot(cond):
    return jnp.where(cond, 1.0, 0.0).astype(BF16)


def sigmoid(v):
    return 1.0 / (1.0 + jnp.exp(-v))


def row_shifts(x):
    count = x.shape[0]
    row = iota(x.shape, 0) % ROWS
    above = jnp.where(row == 0, 0.0, pltpu.roll(x, 1, 0))
    below = jnp.where(row == ROWS - 1, 0.0, pltpu.roll(x, count - 1, 0))
    return above, x, below


def conv(x, weights, part, count):
    shifted = row_shifts(x)
    total = None
    for a in range(3):
        for b in range(3):
            lhs = shifted[a][8 * b : 8 * b + count].astype(BF16)
            term = jnp.dot(lhs, weights[part, 3 * a + b], preferred_element_type=F32)
            total = term if total is None else total + term
    return total


def kernel(
    scaling,
    strips,
    kernels,
    cotangent,
    gk_out,
    gi_out,
    w,
    wt,
    sv,
    cv,
    gi,
    fin,
    gin,
    fout,
    gout,
    hid,
    raw,
    fs,
    fg,
    gs,
    gg,
    cc,
    acc,
    pkl,
    pk,
    rz,
    pc,
    sel,
    c6,
    local_sem,
    weight_sem,
    gi_sem,
    fr,
    fsend,
    br,
    bsend,
    edge_send,
    raw_recv,
    raw_send,
    fg_recv,
    fg_send,
    gg_recv,
    gg_send,
    gr_recv,
    gr_send,
    z_recv,
    z_send,
):
    s = lax.axis_index("section")
    slab = lax.axis_index("slab")
    img = lax.axis_index("img")
    z = slab // 2
    core = slab % 2
    has_left = slab > 0
    has_right = slab < SLABS - 1

    loads = [
        pltpu.make_async_copy(strips, sv, local_sem.at[0]),
        pltpu.make_async_copy(cotangent, cv, local_sem.at[1]),
    ]
    for part in range(2):
        for tap in range(9):
            loads.append(
                pltpu.make_async_copy(
                    kernels.at[part, tap], w.at[part, tap], weight_sem.at[part, tap]
                )
            )
    for load in loads:
        load.start()

    @pl.when(slab == 0)
    def _():
        for buf in (fin, gin):
            buf[:, 0:16, :] = jnp.zeros((CROPS, 16, C), BF16)

    @pl.when(slab == SLABS - 1)
    def _():
        for buf in (fin, gin):
            buf[:, DEEP - 16 : DEEP, :] = jnp.zeros((CROPS, 16, C), BF16)

    barrier = pltpu.get_barrier_semaphore()

    def greet(where):
        pl.semaphore_signal(barrier, inc=1, device_id=where, device_id_type=MESH)

    def image_of(d):
        return (s, slab, (img + d) % IMAGES)

    partner = (s, 2 * z + 1 - core, img)

    def chip_of(d):
        return (s, 2 * ((z + d) % CHIPS) + core, img)

    greeted = jnp.int32(0)
    for ds in (-1, 0, 1):
        for dj in (-1, 0, 1):
            if ds == 0 and dj == 0:
                continue
            ok = (s + ds >= 0) & (s + ds < SECTIONS) & (slab + dj >= 0) & (slab + dj < SLABS)

            @pl.when(ok)
            def _():
                greet((s + ds, slab + dj, img))

            greeted = greeted + jnp.where(ok, 1, 0)
    for d in range(1, IMAGES):
        greet(image_of(d))
    greet(partner)
    for d in range(1, CHIPS):
        greet(chip_of(d))
    i, j = iota((POS, POS), 0), iota((POS, POS), 1)
    swap = onehot((i // 8 == j % 8) & (i % 8 == j // 8))
    i, j = iota((C, 2 * HALF), 0), iota((C, 2 * HALF), 1)
    lane = j % 32
    side = (j // HALF + core) % 2
    pc[...] = onehot((lane < IN_SHARE) & (i == IN_SHARE * (2 * ((j % HALF) // 32) + side) + lane))
    lane = j % 128
    owner = (j // 128 + img) % IMAGES
    sel[...] = onehot((lane < OUT_SHARE) & (i == OUT_SHARE * owner + lane))
    i, j = iota((768, 512), 0), iota((768, 512), 1)
    lane = i % 32
    c6[...] = onehot(
        (lane < IN_SHARE)
        & ((i % 128) // 32 == j // 128)
        & (j % 128 == IN_SHARE * (i // 128) + lane)
    )

    acc[...] = jnp.zeros_like(acc)
    pl.semaphore_wait(barrier, greeted + IMAGES + (CHIPS - 1))

    def permuted(x, matrix):
        return jnp.dot(x, matrix, preferred_element_type=F32).astype(BF16)

    def spread(src, dst, send, recv, k, ds, center):
        base = 16 if src is dst else 0

        @pl.when(has_right)
        def _():
            pltpu.make_async_remote_copy(
                src_ref=src.at[k, pl.ds(base + POS - 16, 16)],
                dst_ref=dst.at[k, pl.ds(0, 16)],
                send_sem=send.at[k, 2],
                recv_sem=recv.at[k, 0],
                device_id=(s + ds, slab + 1, img),
                device_id_type=MESH,
            ).start()

        @pl.when(has_left)
        def _():
            pltpu.make_async_remote_copy(
                src_ref=src.at[k, pl.ds(base, 16)],
                dst_ref=dst.at[k, pl.ds(DEEP - 16, 16)],
                send_sem=send.at[k, 0],
                recv_sem=recv.at[k, 2],
                device_id=(s + ds, slab - 1, img),
                device_id_type=MESH,
            ).start()

        if center:
            pltpu.make_async_remote_copy(
                src_ref=src.at[k],
                dst_ref=dst.at[k, pl.ds(16, POS)],
                send_sem=send.at[k, 1],
                recv_sem=recv.at[k, 1],
                device_id=(s + ds, slab, img),
                device_id_type=MESH,
            ).start()

    def waited(ref, sem):
        pltpu.make_async_copy(ref, ref, sem).wait()

    def arrive(dst, recv, k, center):
        @pl.when(center)
        def _():
            waited(dst.at[k, pl.ds(16, POS)], recv.at[k, 1])

        @pl.when(has_left)
        def _():
            waited(dst.at[k, pl.ds(0, 16)], recv.at[k, 0])

        @pl.when(has_right)
        def _():
            waited(dst.at[k, pl.ds(DEEP - 16, 16)], recv.at[k, 2])

    def sent(src, send, k, center):
        base = 16 if center is None else 0
        if center is not None:
            waited(src.at[k], send.at[k, 1])

        @pl.when(has_right)
        def _():
            waited(src.at[k, pl.ds(base + POS - 16, 16)], send.at[k, 2])

        @pl.when(has_left)
        def _():
            waited(src.at[k, pl.ds(base, 16)], send.at[k, 0])

    loads[0].wait()
    loads[1].wait()

    @pl.when(s == 0)
    def _():
        def step(k, carry):
            fin[k, 16 : 16 + POS, :] = permuted(swap, sv[k])
            spread(fin, fin, edge_send, fr, k, 0, False)
            return carry

        lax.fori_loop(0, CROPS, step, 0)

    @pl.when(s == SECTIONS - 1)
    def _():
        def step(k, carry):
            gin[k, 16 : 16 + POS, :] = permuted(swap, cv[k])
            spread(gin, gin, edge_send, br, k, 0, False)
            return carry

        lax.fori_loop(0, CROPS, step, 0)

    for load in loads[2:]:
        load.wait()

    def transpose_weights():
        def step(n, carry):
            part, tap = n // 9, n % 9
            wt[part, 8 - tap] = w[part, tap].T
            return carry

        lax.fori_loop(0, 18, step, 0)

    pl.when(s > 0)(transpose_weights)

    row = iota((WIDE, C), 0)
    inside = jnp.logical_not(
        ((row < 8) & (slab == 0)) | ((row >= WIDE - 8) & (slab == SLABS - 1))
    )

    last = CROPS - 1

    def share_field(a, k, wide):
        raw[a, k, IMAGES - 1] = wide
        for d in range(1, IMAGES):
            pltpu.make_async_remote_copy(
                src_ref=raw.at[a, k, IMAGES - 1],
                dst_ref=raw.at[a, k, d - 1],
                send_sem=raw_send.at[a, k],
                recv_sem=raw_recv.at[a, k],
                device_id=image_of(d),
                device_id_type=MESH,
            ).start()

    def relay_field(k):
        for a in range(2):
            waited(raw.at[a, k, pl.ds(0, IMAGES - 1)], raw_recv.at[a, k])
            for n in range(IMAGES):
                both = permuted(raw[a, k, n], pc[...])
                fg[a, k, n] = both[:, :HALF]
                fs[a, k, n] = both[:, HALF:]
            pltpu.make_async_remote_copy(
                src_ref=fs.at[a, k],
                dst_ref=fg.at[a, k, pl.ds(IMAGES, IMAGES)],
                send_sem=fg_send.at[a, k],
                recv_sem=fg_recv.at[a, k],
                device_id=partner,
                device_id_type=MESH,
            ).start()

    def share_grad(a, k, chunks):
        gg[a, k, IMAGES - 1] = chunks[:, :128]
        for d in range(1, IMAGES):
            gs[a, k, d - 1] = chunks[:, 128 * d : 128 * (d + 1)]
            pltpu.make_async_remote_copy(
                src_ref=gs.at[a, k, d - 1],
                dst_ref=gg.at[a, k, d - 1],
                send_sem=gg_send.at[a, k],
                recv_sem=gg_recv.at[a, k],
                device_id=image_of(d),
                device_id_type=MESH,
            ).start()

    def relay_grad(a, k):
        waited(gg.at[a, k, pl.ds(0, IMAGES - 1)], gg_recv.at[a, k])
        pltpu.make_async_remote_copy(
            src_ref=gg.at[a, k, pl.ds(0, IMAGES)],
            dst_ref=gg.at[a, k, pl.ds(IMAGES, IMAGES)],
            send_sem=gr_send.at[a, k],
            recv_sem=gr_recv.at[a, k],
            device_id=partner,
            device_id_type=MESH,
        ).start()

    def forward(k):
        arrive(fin, fr, k, s > 0)
        x = fin[k].astype(F32)
        hidden = conv(x, w, 0, WIDE)
        hid[k] = hidden
        active = jnp.where(inside, hidden * sigmoid(hidden), 0.0).astype(BF16)

        @pl.when(s < SECTIONS - 1)
        def _():
            result = x[16 : 16 + POS] + conv(active.astype(F32), w, 1, POS)
            fout[k] = result.astype(BF16)
            spread(fout, fin, fsend, fr, k, 1, True)

        share_field(0, k, x[8 : 8 + WIDE].astype(BF16))
        share_field(1, k, active)

        @pl.when((s == 0) & (k == last))
        def _():
            transpose_weights()

    def backward(k):
        arrive(gin, br, k, s < SECTIONS - 1)
        g = gin[k].astype(F32)
        center = g[16 : 16 + POS]
        ahead = (s == 0) & (k == last)

        @pl.when(ahead)
        def _():
            share_grad(1, k, permuted(center.astype(BF16), sel[...]))

        grad_active = conv(g, wt, 1, WIDE)
        hidden = hid[k]
        q = sigmoid(hidden)
        slope = q * (1.0 + hidden * (1.0 - q))
        grad_hidden = jnp.where(inside, grad_active * slope, 0.0).astype(BF16)
        wide = grad_hidden.astype(F32)
        grad_in = (center + conv(wide, wt, 0, POS)).astype(BF16)
        gout[k] = grad_in

        @pl.when(s > 0)
        def _():
            spread(gout, gin, bsend, br, k, -1, True)

        gi[k] = permuted(swap, grad_in)
        pltpu.make_async_copy(gi.at[k], gi_out.at[k], gi_sem.at[k]).start()
        lower = wide[8 : 8 + POS].astype(BF16)
        chunks = permuted(jnp.concatenate([lower, center.astype(BF16)], axis=0), sel[...])
        share_grad(0, k, chunks[:POS])

        @pl.when(jnp.logical_not(ahead))
        def _():
            share_grad(1, k, chunks[POS:])

    def unfold(k):
        for a in range(2):
            waited(fg.at[a, k, pl.ds(IMAGES, IMAGES)], fg_recv.at[a, k])

            def source(m, carry):
                shifted = row_shifts(fg[a, k, m].astype(F32))
                for d in range(3):
                    for b in range(3):
                        cc[a, k, 3 * d + b, pl.ds(pl.multiple_of(m * POS, POS), POS), :] = shifted[d][
                            8 * b : 8 * b + POS
                        ].astype(BF16)
                return carry

            lax.fori_loop(0, PEERS, source, 0)

    def contract(a, k):
        waited(gg.at[a, k, pl.ds(IMAGES, IMAGES)], gr_recv.at[a, k])
        grads = gg[a, k].reshape(PEERS * POS, 128).T[:OUT_SHARE]
        for t in range(9):
            acc[a, t] += jnp.dot(grads, cc[a, k, t], preferred_element_type=F32)

    def unfold_step(n):
        @pl.when(n < CROPS)
        def _():
            relay_field(n)

        @pl.when(n > 0)
        def _():
            unfold(n - 1)

    at_end = s == SECTIONS - 1
    ahead_count = jnp.where(s == 0, CROPS + 1, jnp.where(s == 1, CROPS - 1, 0))

    def step(i, carry):
        back_from = CROPS + ahead_count
        is_forward = jnp.where(at_end, (i < 2 * CROPS) & (i % 2 == 0), i < CROPS)
        is_backward = jnp.where(
            at_end, (i < 2 * CROPS) & (i % 2 == 1), (i >= back_from) & (i < back_from + CROPS)
        )

        @pl.when(is_forward)
        def _():
            forward(jnp.where(at_end, i // 2, i))

        @pl.when(is_backward)
        def _():
            backward(jnp.where(at_end, i // 2, i - back_from))

        @pl.when(jnp.logical_not(is_forward | is_backward))
        def _():
            unfold_step(jnp.where(i < back_from, i - CROPS, i - 2 * CROPS))

        return carry

    lax.fori_loop(0, 3 * CROPS + 1, step, 0)

    def pack(t):
        for p in range(6):
            a, tap = divmod(6 * t + p, 9)
            block = acc[a, tap].astype(BF16)
            for half in range(2):
                pkl[t, half, :, 128 * p : 128 * (p + 1)] = block[:, 128 * half : 128 * (half + 1)]
        packed = permuted(pkl[t].reshape(2 * OUT_SHARE, 768), c6[...]).reshape(2, OUT_SHARE, 512)
        for half in range(2):
            for q in range(4):
                pk[t, 4 * half + q] = packed[half, :, 128 * q : 128 * (q + 1)]
        for d in (4, 3, 5, 2, 6, 1, 7):
            pltpu.make_async_remote_copy(
                src_ref=pk.at[t, (z + d) % CHIPS],
                dst_ref=rz.at[t, d - 1],
                send_sem=z_send.at[t],
                recv_sem=z_recv.at[t],
                device_id=chip_of(d),
                device_id_type=MESH,
            ).start()

    def hand_over(k, carry):
        relay_grad(1, k)
        relay_grad(0, k)
        return carry

    lax.fori_loop(0, last, hand_over, 0)

    def tail(i, carry):
        @pl.when(i == 3)
        def _():
            relay_grad(1, last)

        @pl.when(i == 4)
        def _():
            relay_grad(0, last)

        upper = (i < 3) | (i == 5)
        crop = jnp.where(i < 3, i, jnp.where(i < 5, i - 3, jnp.where(i == 5, last, i - 4)))
        contract(jnp.where(upper, 1, 0), crop)

        @pl.when(i == 5)
        def _():
            pack(2)

        return carry

    lax.fori_loop(0, 2 * CROPS, tail, 0)
    pack(1)
    pack(0)

    for t in (2, 1, 0):
        waited(rz.at[t], z_recv.at[t])
        total = pk[t, z].astype(F32)
        for d in range(CHIPS - 1):
            total = total + rz[t, d].astype(F32)
        flipped = (total * scaling).T
        for p in range(6):
            a, tap = divmod(6 * t + p, 9)
            gk_out[a, tap] = flipped[IN_SHARE * p : IN_SHARE * (p + 1)]

    for t in range(3):
        waited(rz.at[t], z_send.at[t])

    def drain(k, carry):
        pltpu.make_async_copy(gi.at[k], gi_out.at[k], gi_sem.at[k]).wait()

        @pl.when(s == 0)
        def _():
            sent(fin, edge_send, k, None)

        @pl.when(s == SECTIONS - 1)
        def _():
            sent(gin, edge_send, k, None)

        @pl.when(s < SECTIONS - 1)
        def _():
            sent(fout, fsend, k, True)

        @pl.when(s > 0)
        def _():
            sent(gout, bsend, k, True)

        for a in range(2):
            waited(raw.at[a, k, pl.ds(0, IMAGES - 1)], raw_send.at[a, k])
            waited(fs.at[a, k], fg_send.at[a, k])
            waited(gs.at[a, k], gg_send.at[a, k])
            waited(gg.at[a, k, pl.ds(0, IMAGES)], gr_send.at[a, k])
        return carry

    lax.fori_loop(0, CROPS, drain, 0)


def shards(strips, kernels, cotangent):
    scaling = 1.0 / math.sqrt(IMAGES * CROPS * ROWS * COLS * SLABS)
    dma = pltpu.SemaphoreType.DMA
    vmem = pl.BlockSpec(memory_space=pltpu.VMEM)
    hbm = pl.BlockSpec(memory_space=pl.ANY)
    gk, gi = pl.pallas_call(
        lambda *refs: kernel(scaling, *refs),
        out_shape=(
            jax.ShapeDtypeStruct((2, 9, IN_SHARE, OUT_SHARE), F32),
            jax.ShapeDtypeStruct((CROPS, POS, C), BF16),
        ),
        in_specs=[hbm, hbm, hbm],
        out_specs=(vmem, hbm),
        scratch_shapes=[
            pltpu.VMEM((2, 9, C, C), BF16),
            pltpu.VMEM((2, 9, C, C), BF16),
            pltpu.VMEM((CROPS, POS, C), BF16),
            pltpu.VMEM((CROPS, POS, C), BF16),
            pltpu.VMEM((CROPS, POS, C), BF16),
            pltpu.VMEM((CROPS, DEEP, C), BF16),
            pltpu.VMEM((CROPS, DEEP, C), BF16),
            pltpu.VMEM((CROPS, POS, C), BF16),
            pltpu.VMEM((CROPS, POS, C), BF16),
            pltpu.VMEM((CROPS, WIDE, C), F32),
            pltpu.VMEM((2, CROPS, IMAGES, WIDE, C), BF16),
            pltpu.VMEM((2, CROPS, IMAGES, WIDE, HALF), BF16),
            pltpu.VMEM((2, CROPS, PEERS, WIDE, HALF), BF16),
            pltpu.VMEM((2, CROPS, IMAGES - 1, POS, 128), BF16),
            pltpu.VMEM((2, CROPS, PEERS, POS, 128), BF16),
            pltpu.VMEM((2, CROPS, 9, PEERS * POS, HALF), BF16),
            pltpu.VMEM((2, 9, OUT_SHARE, HALF), F32),
            pltpu.VMEM((3, 2, OUT_SHARE, 768), BF16),
            pltpu.VMEM((3, CHIPS, OUT_SHARE, 128), BF16),
            pltpu.VMEM((3, CHIPS - 1, OUT_SHARE, 128), BF16),
            pltpu.VMEM((C, 2 * HALF), BF16),
            pltpu.VMEM((C, 512), BF16),
            pltpu.VMEM((768, 512), BF16),
            dma((2,)),
            dma((2, 9)),
            dma((CROPS,)),
            dma((CROPS, 3)),
            dma((CROPS, 3)),
            dma((CROPS, 3)),
            dma((CROPS, 3)),
            dma((CROPS, 3)),
            dma((2, CROPS)),
            dma((2, CROPS)),
            dma((2, CROPS)),
            dma((2, CROPS)),
            dma((2, CROPS)),
            dma((2, CROPS)),
            dma((2, CROPS)),
            dma((2, CROPS)),
            dma((3,)),
            dma((3,)),
        ],
        compiler_params=pltpu.CompilerParams(
            collective_id=0, has_side_effects=True, vmem_limit_bytes=60 * 1024 * 1024
        ),
        name="residual_step",
    )(
        strips.reshape(CROPS, POS, C),
        kernels.reshape(2, 9, C, C),
        cotangent.reshape(CROPS, POS, C),
    )
    return gk[None], gi.reshape(1, 1, CROPS, ROWS, COLS, C)


def solution(mesh):
    return jax.shard_map(
        shards,
        mesh=mesh,
        in_specs=(
            P("img", None, None, "slab", None),
            P("section", None, None, None, None),
            P("img", None, None, "slab", None),
        ),
        out_specs=(
            P("section", None, None, "slab", "img"),
            P("section", "img", None, None, "slab", None),
        ),
        check_vma=False,
    )
```

```python
import math

import jax
import jax.numpy as jnp
from jax import lax
from jax.experimental import pallas as pl
from jax.experimental.pallas import tpu as pltpu
from jax.sharding import PartitionSpec as P

MESH = pl.DeviceIdType.MESH
F32 = jnp.float32
BF16 = jnp.bfloat16

C = 320
SECTIONS = 4
IMAGES = 4
CROPS = 4
CHIPS = 8
SLABS = 16
ROWS = 8
COLS = 8
POS = ROWS * COLS
WIDE = POS + 16
DEEP = POS + 32
OUT_SHARE = C // IMAGES
IN_SHARE = C // SLABS
HALF = 256
PEERS = 8
PAIR = 640


def iota(shape, dim):
    return lax.broadcasted_iota(jnp.int32, shape, dim)


def onehot(cond):
    return jnp.where(cond, 1.0, 0.0).astype(BF16)


def sigmoid(v):
    return 1.0 / (1.0 + jnp.exp(-v))


def row_shifts(x):
    count = x.shape[0]
    row = iota(x.shape, 0) % ROWS
    above = jnp.where(row == 0, 0.0, pltpu.roll(x, 1, 0))
    below = jnp.where(row == ROWS - 1, 0.0, pltpu.roll(x, count - 1, 0))
    return above, x, below


def conv(x, weights, part, count):
    shifted = row_shifts(x)
    total = None
    for a in range(3):
        for b in range(3):
            lhs = shifted[a][8 * b : 8 * b + count].astype(BF16)
            term = jnp.dot(lhs, weights[part, 3 * a + b], preferred_element_type=F32)
            total = term if total is None else total + term
    return total


def kernel(
    scaling,
    strips,
    kernels,
    cotangent,
    gk_out,
    gi_out,
    w,
    wt,
    sv,
    cv,
    gi,
    fin,
    gin,
    fout,
    gout,
    hid,
    raw,
    fs,
    fg,
    gs,
    gg,
    cc,
    acc,
    pkl,
    pk,
    rz,
    pc,
    pct,
    sel,
    c6,
    local_sem,
    weight_sem,
    gi_sem,
    fr,
    fsend,
    br,
    bsend,
    edge_send,
    raw_recv,
    raw_send,
    fg_recv,
    fg_send,
    gg_recv,
    gg_send,
    gr_recv,
    gr_send,
    z_recv,
    z_send,
):
    s = lax.axis_index("section")
    slab = lax.axis_index("slab")
    img = lax.axis_index("img")
    z = slab // 2
    core = slab % 2
    has_left = slab > 0
    has_right = slab < SLABS - 1

    loads = [
        pltpu.make_async_copy(strips, sv, local_sem.at[0]),
        pltpu.make_async_copy(cotangent, cv, local_sem.at[1]),
    ]
    for part in range(2):
        for tap in range(9):
            loads.append(
                pltpu.make_async_copy(
                    kernels.at[part, tap], w.at[part, tap], weight_sem.at[part, tap]
                )
            )
    for load in loads:
        load.start()

    @pl.when(slab == 0)
    def _():
        for buf in (fin, gin):
            buf[:, 0:16, :] = jnp.zeros((CROPS, 16, C), BF16)

    @pl.when(slab == SLABS - 1)
    def _():
        for buf in (fin, gin):
            buf[:, DEEP - 16 : DEEP, :] = jnp.zeros((CROPS, 16, C), BF16)

    barrier = pltpu.get_barrier_semaphore()

    def greet(where):
        pl.semaphore_signal(barrier, inc=1, device_id=where, device_id_type=MESH)

    def image_of(d):
        return (s, slab, (img + d) % IMAGES)

    partner = (s, 2 * z + 1 - core, img)

    def chip_of(d):
        return (s, 2 * ((z + d) % CHIPS) + core, img)

    greeted = jnp.int32(0)
    for ds in (-1, 0, 1):
        for dj in (-1, 0, 1):
            if ds == 0 and dj == 0:
                continue
            ok = (s + ds >= 0) & (s + ds < SECTIONS) & (slab + dj >= 0) & (slab + dj < SLABS)

            @pl.when(ok)
            def _():
                greet((s + ds, slab + dj, img))

            greeted = greeted + jnp.where(ok, 1, 0)
    for d in range(1, IMAGES):
        greet(image_of(d))
    greet(partner)
    for d in range(1, CHIPS):
        greet(chip_of(d))
    i, j = iota((POS, POS), 0), iota((POS, POS), 1)
    swap = onehot((i // 8 == j % 8) & (i % 8 == j // 8))
    def chosen(first, shape):
        i, j = iota(shape, 0) + first, iota(shape, 1)
        lane = j % 32
        side = (j // HALF + core) % 2
        return (lane < IN_SHARE) & (i == IN_SHARE * (2 * ((j % HALF) // 32) + side) + lane)

    pc[...] = onehot(chosen(0, (256, 2 * HALF)))
    tail_row = iota((128, 2 * HALF), 0)
    pct[0] = onehot(chosen(256, (128, 2 * HALF)) & (tail_row < 64))
    pct[1] = onehot(chosen(192, (128, 2 * HALF)) & (tail_row >= 64))
    i, j = iota((C, 512), 0), iota((C, 512), 1)
    lane = j % 128
    owner = (j // 128 + img) % IMAGES
    sel[...] = onehot((lane < OUT_SHARE) & (i == OUT_SHARE * owner + lane))
    i, j = iota((768, 512), 0), iota((768, 512), 1)
    lane = i % 32
    c6[...] = onehot(
        (lane < IN_SHARE)
        & ((i % 128) // 32 == j // 128)
        & (j % 128 == IN_SHARE * (i // 128) + lane)
    )

    acc[...] = jnp.zeros_like(acc)
    pl.semaphore_wait(barrier, greeted + IMAGES + (CHIPS - 1))

    def permuted(x, matrix):
        return jnp.dot(x, matrix, preferred_element_type=F32).astype(BF16)

    def spread(src, dst, send, recv, k, ds, center):
        base = 16 if src is dst else 0

        @pl.when(has_right)
        def _():
            pltpu.make_async_remote_copy(
                src_ref=src.at[k, pl.ds(base + POS - 16, 16)],
                dst_ref=dst.at[k, pl.ds(0, 16)],
                send_sem=send.at[k, 2],
                recv_sem=recv.at[k, 0],
                device_id=(s + ds, slab + 1, img),
                device_id_type=MESH,
            ).start()

        @pl.when(has_left)
        def _():
            pltpu.make_async_remote_copy(
                src_ref=src.at[k, pl.ds(base, 16)],
                dst_ref=dst.at[k, pl.ds(DEEP - 16, 16)],
                send_sem=send.at[k, 0],
                recv_sem=recv.at[k, 2],
                device_id=(s + ds, slab - 1, img),
                device_id_type=MESH,
            ).start()

        if center:
            pltpu.make_async_remote_copy(
                src_ref=src.at[k],
                dst_ref=dst.at[k, pl.ds(16, POS)],
                send_sem=send.at[k, 1],
                recv_sem=recv.at[k, 1],
                device_id=(s + ds, slab, img),
                device_id_type=MESH,
            ).start()

    def waited(ref, sem):
        pltpu.make_async_copy(ref, ref, sem).wait()

    def arrive(dst, recv, k, center):
        @pl.when(center)
        def _():
            waited(dst.at[k, pl.ds(16, POS)], recv.at[k, 1])

        @pl.when(has_left)
        def _():
            waited(dst.at[k, pl.ds(0, 16)], recv.at[k, 0])

        @pl.when(has_right)
        def _():
            waited(dst.at[k, pl.ds(DEEP - 16, 16)], recv.at[k, 2])

    def sent(src, send, k, center):
        base = 16 if center is None else 0
        if center is not None:
            waited(src.at[k], send.at[k, 1])

        @pl.when(has_right)
        def _():
            waited(src.at[k, pl.ds(base + POS - 16, 16)], send.at[k, 2])

        @pl.when(has_left)
        def _():
            waited(src.at[k, pl.ds(base, 16)], send.at[k, 0])

    loads[0].wait()
    loads[1].wait()

    @pl.when(s == 0)
    def _():
        def step(k, carry):
            fin[k, 16 : 16 + POS, :] = permuted(swap, sv[k])
            spread(fin, fin, edge_send, fr, k, 0, False)
            return carry

        lax.fori_loop(0, CROPS, step, 0)

    @pl.when(s == SECTIONS - 1)
    def _():
        def step(k, carry):
            gin[k, 16 : 16 + POS, :] = permuted(swap, cv[k])
            spread(gin, gin, edge_send, br, k, 0, False)
            return carry

        lax.fori_loop(0, CROPS, step, 0)

    for load in loads[2:]:
        load.wait()

    def transpose_weights():
        def step(n, carry):
            part, tap = n // 9, n % 9
            wt[part, 8 - tap] = w[part, tap].T
            return carry

        lax.fori_loop(0, 18, step, 0)

    pl.when(s > 0)(transpose_weights)

    row = iota((WIDE, C), 0)
    inside = jnp.logical_not(
        ((row < 8) & (slab == 0)) | ((row >= WIDE - 8) & (slab == SLABS - 1))
    )

    last = CROPS - 1

    def share_fields(k, wide, active):
        mine = raw.at[k, IMAGES - 1]
        mine[:, 0:256] = wide[:, 0:256].astype(BF16)
        mine[:, 256:512] = active[:, 0:256]
        tails = jnp.concatenate([wide[:, 256:C], active[:, 256:C].astype(F32)], axis=1)
        mine[:, 512:PAIR] = tails.astype(BF16)
        for d in range(1, IMAGES):
            pltpu.make_async_remote_copy(
                src_ref=mine,
                dst_ref=raw.at[k, d - 1],
                send_sem=raw_send.at[k],
                recv_sem=raw_recv.at[k],
                device_id=image_of(d),
                device_id_type=MESH,
            ).start()

    def relay_field(k):
        waited(raw.at[k, pl.ds(0, IMAGES - 1)], raw_recv.at[k])
        for a in range(2):
            for n in range(IMAGES):
                both = (
                    jnp.dot(raw[k, n, :, 256 * a : 256 * (a + 1)], pc[...], preferred_element_type=F32)
                    + jnp.dot(raw[k, n, :, 512:PAIR], pct[a], preferred_element_type=F32)
                ).astype(BF16)
                fg[a, k, n] = both[:, :HALF]
                fs[a, k, n] = both[:, HALF:]
            pltpu.make_async_remote_copy(
                src_ref=fs.at[a, k],
                dst_ref=fg.at[a, k, pl.ds(IMAGES, IMAGES)],
                send_sem=fg_send.at[a, k],
                recv_sem=fg_recv.at[a, k],
                device_id=partner,
                device_id_type=MESH,
            ).start()

    def share_grad(a, k, chunks):
        gg[a, k, IMAGES - 1] = chunks[:, :128]
        for d in range(1, IMAGES):
            gs[a, k, d - 1] = chunks[:, 128 * d : 128 * (d + 1)]
            pltpu.make_async_remote_copy(
                src_ref=gs.at[a, k, d - 1],
                dst_ref=gg.at[a, k, d - 1],
                send_sem=gg_send.at[a, k],
                recv_sem=gg_recv.at[a, k],
                device_id=image_of(d),
                device_id_type=MESH,
            ).start()

    def relay_grad(a, k):
        waited(gg.at[a, k, pl.ds(0, IMAGES - 1)], gg_recv.at[a, k])
        pltpu.make_async_remote_copy(
            src_ref=gg.at[a, k, pl.ds(0, IMAGES)],
            dst_ref=gg.at[a, k, pl.ds(IMAGES, IMAGES)],
            send_sem=gr_send.at[a, k],
            recv_sem=gr_recv.at[a, k],
            device_id=partner,
            device_id_type=MESH,
        ).start()

    def forward(k):
        arrive(fin, fr, k, s > 0)
        x = fin[k].astype(F32)
        hidden = conv(x, w, 0, WIDE)
        hid[k] = hidden
        active = jnp.where(inside, hidden * sigmoid(hidden), 0.0).astype(BF16)

        @pl.when(s < SECTIONS - 1)
        def _():
            result = x[16 : 16 + POS] + conv(active.astype(F32), w, 1, POS)
            fout[k] = result.astype(BF16)
            spread(fout, fin, fsend, fr, k, 1, True)

        share_fields(k, x[8 : 8 + WIDE], active)

        @pl.when((s == 0) & (k == last))
        def _():
            transpose_weights()

    def backward(k):
        arrive(gin, br, k, s < SECTIONS - 1)
        g = gin[k].astype(F32)
        center = g[16 : 16 + POS]
        ahead = (s == 0) & (k == last)

        @pl.when(ahead)
        def _():
            share_grad(1, k, permuted(center.astype(BF16), sel[...]))

        grad_active = conv(g, wt, 1, WIDE)
        hidden = hid[k]
        q = sigmoid(hidden)
        slope = q * (1.0 + hidden * (1.0 - q))
        grad_hidden = jnp.where(inside, grad_active * slope, 0.0).astype(BF16)
        wide = grad_hidden.astype(F32)
        grad_in = (center + conv(wide, wt, 0, POS)).astype(BF16)
        gout[k] = grad_in

        @pl.when(s > 0)
        def _():
            spread(gout, gin, bsend, br, k, -1, True)

        gi[k] = permuted(swap, grad_in)
        pltpu.make_async_copy(gi.at[k], gi_out.at[k], gi_sem.at[k]).start()
        lower = wide[8 : 8 + POS].astype(BF16)
        chunks = permuted(jnp.concatenate([lower, center.astype(BF16)], axis=0), sel[...])
        share_grad(0, k, chunks[:POS])

        @pl.when(jnp.logical_not(ahead))
        def _():
            share_grad(1, k, chunks[POS:])

        @pl.when((s == 0) & (k >= 2))
        def _():
            relay_grad(1, k - 2)
            relay_grad(0, k - 2)

    def unfold(k):
        for a in range(2):
            waited(fg.at[a, k, pl.ds(IMAGES, IMAGES)], fg_recv.at[a, k])

            def source(m, carry):
                shifted = row_shifts(fg[a, k, m].astype(F32))
                for d in range(3):
                    for b in range(3):
                        cc[a, k, 3 * d + b, pl.ds(pl.multiple_of(m * POS, POS), POS), :] = shifted[d][
                            8 * b : 8 * b + POS
                        ].astype(BF16)
                return carry

            lax.fori_loop(0, PEERS, source, 0)

    def contract(a, k):
        waited(gg.at[a, k, pl.ds(IMAGES, IMAGES)], gr_recv.at[a, k])
        grads = gg[a, k].reshape(PEERS * POS, 128).T[:OUT_SHARE]
        for t in range(9):
            acc[a, t] += jnp.dot(grads, cc[a, k, t], preferred_element_type=F32)

    def unfold_step(n):
        @pl.when(n < CROPS)
        def _():
            relay_field(n)

        @pl.when(n > 0)
        def _():
            unfold(n - 1)

            @pl.when(s > 0)
            def _():
                relay_grad(1, n - 1)
                relay_grad(0, n - 1)

        @pl.when((s > 0) & (n > 1))
        def _():
            def each(a, carry):
                contract(a, n - 2)
                return carry

            lax.fori_loop(0, 2, each, 0)

    at_end = s == SECTIONS - 1
    ahead_count = jnp.where(s == 0, CROPS + 1, 0)

    def step(i, carry):
        back_from = CROPS + ahead_count
        is_forward = jnp.where(at_end, (i < 2 * CROPS) & (i % 2 == 0), i < CROPS)
        is_backward = jnp.where(
            at_end, (i < 2 * CROPS) & (i % 2 == 1), (i >= back_from) & (i < back_from + CROPS)
        )

        @pl.when(is_forward)
        def _():
            forward(jnp.where(at_end, i // 2, i))

        @pl.when(is_backward)
        def _():
            backward(jnp.where(at_end, i // 2, i - back_from))

        @pl.when(jnp.logical_not(is_forward | is_backward))
        def _():
            unfold_step(jnp.where(i < back_from, i - CROPS, i - 2 * CROPS))

        return carry

    lax.fori_loop(0, 3 * CROPS + 1, step, 0)

    def pack(t):
        for p in range(6):
            a, tap = divmod(6 * t + p, 9)
            block = acc[a, tap].astype(BF16)
            for half in range(2):
                pkl[t, half, :, 128 * p : 128 * (p + 1)] = block[:, 128 * half : 128 * (half + 1)]
        packed = permuted(pkl[t].reshape(2 * OUT_SHARE, 768), c6[...]).reshape(2, OUT_SHARE, 512)
        for half in range(2):
            for q in range(4):
                pk[t, 4 * half + q] = packed[half, :, 128 * q : 128 * (q + 1)]
        for d in (4, 3, 5, 2, 6, 1, 7):
            pltpu.make_async_remote_copy(
                src_ref=pk.at[t, (z + d) % CHIPS],
                dst_ref=rz.at[t, d - 1],
                send_sem=z_send.at[t],
                recv_sem=z_recv.at[t],
                device_id=chip_of(d),
                device_id_type=MESH,
            ).start()

    def tail(i, carry):
        first = s == 0

        @pl.when(first & (i == 2))
        def _():
            relay_grad(1, 2)
            relay_grad(0, 2)

        @pl.when(first & (i == 4))
        def _():
            relay_grad(1, last)

        @pl.when(first & (i == 6))
        def _():
            relay_grad(0, last)

        upper = ((i < 4) & (i % 2 == 0)) | (i == 4) | (i == 5)
        crop = jnp.where(i < 4, i // 2, jnp.where(i % 2 == 0, 2, last))

        @pl.when(first | (i != 6))
        def _():
            contract(jnp.where(upper, 1, 0), crop)

        @pl.when(i == 5)
        def _():
            pack(2)

        return carry

    lax.fori_loop(jnp.where(s == 0, 0, 5), 2 * CROPS, tail, 0)
    pack(1)
    pack(0)

    for t in (2, 1, 0):
        waited(rz.at[t], z_recv.at[t])
        total = pk[t, z].astype(F32)
        for d in range(CHIPS - 1):
            total = total + rz[t, d].astype(F32)
        gk_out[t] = (total * scaling).T

    for t in range(3):
        waited(rz.at[t], z_send.at[t])

    def drain(k, carry):
        pltpu.make_async_copy(gi.at[k], gi_out.at[k], gi_sem.at[k]).wait()

        @pl.when(s == 0)
        def _():
            sent(fin, edge_send, k, None)

        @pl.when(s == SECTIONS - 1)
        def _():
            sent(gin, edge_send, k, None)

        @pl.when(s < SECTIONS - 1)
        def _():
            sent(fout, fsend, k, True)

        @pl.when(s > 0)
        def _():
            sent(gout, bsend, k, True)

        waited(raw.at[k, pl.ds(0, IMAGES - 1)], raw_send.at[k])
        for a in range(2):
            waited(fs.at[a, k], fg_send.at[a, k])
            waited(gs.at[a, k], gg_send.at[a, k])
            waited(gg.at[a, k, pl.ds(0, IMAGES)], gr_send.at[a, k])
        return carry

    lax.fori_loop(0, CROPS, drain, 0)


def placed(gk, gi, gk_out, gi_out):
    gi_out[...] = gi[...]
    for n in range(18):
        a, tap = divmod(n, 9)
        t, p = divmod(n, 6)
        gk_out[tap, :, a, :] = gk[t, IN_SHARE * p : IN_SHARE * (p + 1), :]


def shards(strips, kernels, cotangent):
    scaling = 1.0 / math.sqrt(IMAGES * CROPS * ROWS * COLS * SLABS)
    dma = pltpu.SemaphoreType.DMA
    vmem = pl.BlockSpec(memory_space=pltpu.VMEM)
    hbm = pl.BlockSpec(memory_space=pl.ANY)
    gk, gi = pl.pallas_call(
        lambda *refs: kernel(scaling, *refs),
        out_shape=(
            jax.ShapeDtypeStruct((3, 128, OUT_SHARE), F32),
            jax.ShapeDtypeStruct((CROPS, POS, C), BF16),
        ),
        in_specs=[hbm, hbm, hbm],
        out_specs=(vmem, hbm),
        scratch_shapes=[
            pltpu.VMEM((2, 9, C, C), BF16),
            pltpu.VMEM((2, 9, C, C), BF16),
            pltpu.VMEM((CROPS, POS, C), BF16),
            pltpu.VMEM((CROPS, POS, C), BF16),
            pltpu.VMEM((CROPS, POS, C), BF16),
            pltpu.VMEM((CROPS, DEEP, C), BF16),
            pltpu.VMEM((CROPS, DEEP, C), BF16),
            pltpu.VMEM((CROPS, POS, C), BF16),
            pltpu.VMEM((CROPS, POS, C), BF16),
            pltpu.VMEM((CROPS, WIDE, C), F32),
            pltpu.VMEM((CROPS, IMAGES, WIDE, PAIR), BF16),
            pltpu.VMEM((2, CROPS, IMAGES, WIDE, HALF), BF16),
            pltpu.VMEM((2, CROPS, PEERS, WIDE, HALF), BF16),
            pltpu.VMEM((2, CROPS, IMAGES - 1, POS, 128), BF16),
            pltpu.VMEM((2, CROPS, PEERS, POS, 128), BF16),
            pltpu.VMEM((2, CROPS, 9, PEERS * POS, HALF), BF16),
            pltpu.VMEM((2, 9, OUT_SHARE, HALF), F32),
            pltpu.VMEM((3, 2, OUT_SHARE, 768), BF16),
            pltpu.VMEM((3, CHIPS, OUT_SHARE, 128), BF16),
            pltpu.VMEM((3, CHIPS - 1, OUT_SHARE, 128), BF16),
            pltpu.VMEM((256, 2 * HALF), BF16),
            pltpu.VMEM((2, 128, 2 * HALF), BF16),
            pltpu.VMEM((C, 512), BF16),
            pltpu.VMEM((768, 512), BF16),
            dma((2,)),
            dma((2, 9)),
            dma((CROPS,)),
            dma((CROPS, 3)),
            dma((CROPS, 3)),
            dma((CROPS, 3)),
            dma((CROPS, 3)),
            dma((CROPS, 3)),
            dma((CROPS,)),
            dma((CROPS,)),
            dma((2, CROPS)),
            dma((2, CROPS)),
            dma((2, CROPS)),
            dma((2, CROPS)),
            dma((2, CROPS)),
            dma((2, CROPS)),
            dma((3,)),
            dma((3,)),
        ],
        compiler_params=pltpu.CompilerParams(
            collective_id=0, has_side_effects=True, vmem_limit_bytes=60 * 1024 * 1024
        ),
        name="residual_step",
    )(
        strips.reshape(CROPS, POS, C),
        kernels.reshape(2, 9, C, C),
        cotangent.reshape(CROPS, POS, C),
    )
    gk, gi = pl.pallas_call(
        placed,
        out_shape=(
            jax.ShapeDtypeStruct((9, IN_SHARE, 2, OUT_SHARE), F32),
            jax.ShapeDtypeStruct((CROPS, POS, C), BF16),
        ),
        in_specs=[vmem, vmem],
        out_specs=(vmem, vmem),
        name="outputs",
    )(gk, gi)
    return jnp.transpose(gk, (2, 0, 1, 3))[None], gi.reshape(1, 1, CROPS, ROWS, COLS, C)


def solution(mesh):
    return jax.shard_map(
        shards,
        mesh=mesh,
        in_specs=(
            P("img", None, None, "slab", None),
            P("section", None, None, None, None),
            P("img", None, None, "slab", None),
        ),
        out_specs=(
            P("section", None, None, "slab", "img"),
            P("section", "img", None, None, "slab", None),
        ),
        check_vma=False,
    )
```

```python
import math

import jax
import jax.numpy as jnp
from jax import lax
from jax.experimental import pallas as pl
from jax.experimental.pallas import tpu as pltpu
from jax.sharding import PartitionSpec as P

MESH = pl.DeviceIdType.MESH
F32 = jnp.float32
BF16 = jnp.bfloat16

C = 320
SECTIONS = 4
IMAGES = 4
CROPS = 4
CHIPS = 8
SLABS = 16
ROWS = 8
COLS = 8
POS = ROWS * COLS
WIDE = POS + 16
DEEP = POS + 32
OUT_SHARE = C // IMAGES
IN_SHARE = C // SLABS
HALF = 256
PEERS = 8
PAIR = 640


def iota(shape, dim):
    return lax.broadcasted_iota(jnp.int32, shape, dim)


def onehot(cond):
    return jnp.where(cond, 1.0, 0.0).astype(BF16)


def sigmoid(v):
    return 1.0 / (1.0 + jnp.exp(-v))


def row_shifts(x):
    count = x.shape[0]
    row = iota(x.shape, 0) % ROWS
    above = jnp.where(row == 0, 0.0, pltpu.roll(x, 1, 0))
    below = jnp.where(row == ROWS - 1, 0.0, pltpu.roll(x, count - 1, 0))
    return above, x, below


def conv(x, weights, part, count):
    shifted = row_shifts(x)
    total = None
    for a in range(3):
        for b in range(3):
            lhs = shifted[a][8 * b : 8 * b + count].astype(BF16)
            term = jnp.dot(lhs, weights[part, 3 * a + b], preferred_element_type=F32)
            total = term if total is None else total + term
    return total


def kernel(
    scaling,
    strips,
    kernels,
    cotangent,
    gk_out,
    gi_out,
    w,
    wt,
    sv,
    cv,
    fin,
    gin,
    fout,
    gout,
    hid,
    raw,
    fs,
    fg,
    gs,
    gg,
    cc,
    acc,
    pkl,
    pk,
    rz,
    pc,
    pct,
    sel,
    c6,
    local_sem,
    weight_sem,
    fr,
    fsend,
    br,
    bsend,
    edge_send,
    raw_recv,
    raw_send,
    fg_recv,
    fg_send,
    gg_recv,
    gg_send,
    gr_recv,
    gr_send,
    z_recv,
    z_send,
):
    s = lax.axis_index("section")
    slab = lax.axis_index("slab")
    img = lax.axis_index("img")
    z = slab // 2
    core = slab % 2
    has_left = slab > 0
    has_right = slab < SLABS - 1

    loads = [
        pltpu.make_async_copy(strips, sv, local_sem.at[0]),
        pltpu.make_async_copy(cotangent, cv, local_sem.at[1]),
    ]
    for part in range(2):
        for tap in range(9):
            loads.append(
                pltpu.make_async_copy(
                    kernels.at[part, tap], w.at[part, tap], weight_sem.at[part, tap]
                )
            )
    for load in loads:
        load.start()

    @pl.when(slab == 0)
    def _():
        for buf in (fin, gin):
            buf[:, 0:16, :] = jnp.zeros((CROPS, 16, C), BF16)

    @pl.when(slab == SLABS - 1)
    def _():
        for buf in (fin, gin):
            buf[:, DEEP - 16 : DEEP, :] = jnp.zeros((CROPS, 16, C), BF16)

    barrier = pltpu.get_barrier_semaphore()

    def greet(where):
        pl.semaphore_signal(barrier, inc=1, device_id=where, device_id_type=MESH)

    def image_of(d):
        return (s, slab, (img + d) % IMAGES)

    partner = (s, 2 * z + 1 - core, img)

    def chip_of(d):
        return (s, 2 * ((z + d) % CHIPS) + core, img)

    greeted = jnp.int32(0)
    for ds in (-1, 0, 1):
        for dj in (-1, 0, 1):
            if ds == 0 and dj == 0:
                continue
            ok = (s + ds >= 0) & (s + ds < SECTIONS) & (slab + dj >= 0) & (slab + dj < SLABS)

            @pl.when(ok)
            def _():
                greet((s + ds, slab + dj, img))

            greeted = greeted + jnp.where(ok, 1, 0)
    for d in range(1, IMAGES):
        greet(image_of(d))
    greet(partner)
    for d in range(1, CHIPS):
        greet(chip_of(d))
    i, j = iota((POS, POS), 0), iota((POS, POS), 1)
    swap = onehot((i // 8 == j % 8) & (i % 8 == j // 8))
    def chosen(first, shape):
        i, j = iota(shape, 0) + first, iota(shape, 1)
        lane = j % 32
        side = (j // HALF + core) % 2
        return (lane < IN_SHARE) & (i == IN_SHARE * (2 * ((j % HALF) // 32) + side) + lane)

    pc[...] = onehot(chosen(0, (256, 2 * HALF)))
    tail_row = iota((128, 2 * HALF), 0)
    pct[0] = onehot(chosen(256, (128, 2 * HALF)) & (tail_row < 64))
    pct[1] = onehot(chosen(192, (128, 2 * HALF)) & (tail_row >= 64))
    i, j = iota((C, 512), 0), iota((C, 512), 1)
    lane = j % 128
    owner = (j // 128 + img) % IMAGES
    sel[...] = onehot((lane < OUT_SHARE) & (i == OUT_SHARE * owner + lane))
    i, j = iota((768, 512), 0), iota((768, 512), 1)
    lane = i % 32
    c6[...] = onehot(
        (lane < IN_SHARE)
        & ((i % 128) // 32 == j // 128)
        & (j % 128 == IN_SHARE * (i // 128) + lane)
    )

    acc[...] = jnp.zeros_like(acc)
    pl.semaphore_wait(barrier, greeted + IMAGES + (CHIPS - 1))

    def permuted(x, matrix):
        return jnp.dot(x, matrix, preferred_element_type=F32).astype(BF16)

    def spread(src, dst, send, recv, k, ds, center):
        base = 16 if src is dst else 0

        @pl.when(has_right)
        def _():
            pltpu.make_async_remote_copy(
                src_ref=src.at[k, pl.ds(base + POS - 16, 16)],
                dst_ref=dst.at[k, pl.ds(0, 16)],
                send_sem=send.at[k, 2],
                recv_sem=recv.at[k, 0],
                device_id=(s + ds, slab + 1, img),
                device_id_type=MESH,
            ).start()

        @pl.when(has_left)
        def _():
            pltpu.make_async_remote_copy(
                src_ref=src.at[k, pl.ds(base, 16)],
                dst_ref=dst.at[k, pl.ds(DEEP - 16, 16)],
                send_sem=send.at[k, 0],
                recv_sem=recv.at[k, 2],
                device_id=(s + ds, slab - 1, img),
                device_id_type=MESH,
            ).start()

        if center:
            pltpu.make_async_remote_copy(
                src_ref=src.at[k],
                dst_ref=dst.at[k, pl.ds(16, POS)],
                send_sem=send.at[k, 1],
                recv_sem=recv.at[k, 1],
                device_id=(s + ds, slab, img),
                device_id_type=MESH,
            ).start()

    def waited(ref, sem):
        pltpu.make_async_copy(ref, ref, sem).wait()

    def arrive(dst, recv, k, center):
        @pl.when(center)
        def _():
            waited(dst.at[k, pl.ds(16, POS)], recv.at[k, 1])

        @pl.when(has_left)
        def _():
            waited(dst.at[k, pl.ds(0, 16)], recv.at[k, 0])

        @pl.when(has_right)
        def _():
            waited(dst.at[k, pl.ds(DEEP - 16, 16)], recv.at[k, 2])

    def sent(src, send, k, center):
        base = 16 if center is None else 0
        if center is not None:
            waited(src.at[k], send.at[k, 1])

        @pl.when(has_right)
        def _():
            waited(src.at[k, pl.ds(base + POS - 16, 16)], send.at[k, 2])

        @pl.when(has_left)
        def _():
            waited(src.at[k, pl.ds(base, 16)], send.at[k, 0])

    loads[0].wait()
    loads[1].wait()

    def share_grad(a, k, chunks):
        gg[a, k, IMAGES - 1] = chunks[:, :128]
        for d in range(1, IMAGES):
            gs[a, k, d - 1] = chunks[:, 128 * d : 128 * (d + 1)]
            pltpu.make_async_remote_copy(
                src_ref=gs.at[a, k, d - 1],
                dst_ref=gg.at[a, k, d - 1],
                send_sem=gg_send.at[a, k],
                recv_sem=gg_recv.at[a, k],
                device_id=image_of(d),
                device_id_type=MESH,
            ).start()

    @pl.when(s == 0)
    def _():
        def step(k, carry):
            fin[k, 16 : 16 + POS, :] = permuted(swap, sv[k])
            spread(fin, fin, edge_send, fr, k, 0, False)
            return carry

        lax.fori_loop(0, CROPS, step, 0)

    @pl.when(s == SECTIONS - 1)
    def _():
        def step(k, carry):
            center = permuted(swap, cv[k])
            gin[k, 16 : 16 + POS, :] = center
            spread(gin, gin, edge_send, br, k, 0, False)
            share_grad(1, k, permuted(center, sel[...]))
            return carry

        lax.fori_loop(0, CROPS, step, 0)

    for load in loads[2:]:
        load.wait()

    def transpose_weights():
        def step(n, carry):
            part, tap = n // 9, n % 9
            wt[part, 8 - tap] = w[part, tap].T
            return carry

        lax.fori_loop(0, 18, step, 0)

    pl.when(s > 0)(transpose_weights)

    row = iota((WIDE, C), 0)
    inside = jnp.logical_not(
        ((row < 8) & (slab == 0)) | ((row >= WIDE - 8) & (slab == SLABS - 1))
    )

    last = CROPS - 1

    def share_fields(k, wide, active):
        mine = raw.at[k, IMAGES - 1]
        mine[:, 0:256] = wide[:, 0:256].astype(BF16)
        mine[:, 256:512] = active[:, 0:256]
        tails = jnp.concatenate([wide[:, 256:C], active[:, 256:C].astype(F32)], axis=1)
        mine[:, 512:PAIR] = tails.astype(BF16)
        for d in range(1, IMAGES):
            pltpu.make_async_remote_copy(
                src_ref=mine,
                dst_ref=raw.at[k, d - 1],
                send_sem=raw_send.at[k],
                recv_sem=raw_recv.at[k],
                device_id=image_of(d),
                device_id_type=MESH,
            ).start()

    def relay_field(k):
        waited(raw.at[k, pl.ds(0, IMAGES - 1)], raw_recv.at[k])
        for a in range(2):
            for n in range(IMAGES):
                both = (
                    jnp.dot(raw[k, n, :, 256 * a : 256 * (a + 1)], pc[...], preferred_element_type=F32)
                    + jnp.dot(raw[k, n, :, 512:PAIR], pct[a], preferred_element_type=F32)
                ).astype(BF16)
                fg[a, k, n] = both[:, :HALF]
                fs[a, k, n] = both[:, HALF:]
            pltpu.make_async_remote_copy(
                src_ref=fs.at[a, k],
                dst_ref=fg.at[a, k, pl.ds(IMAGES, IMAGES)],
                send_sem=fg_send.at[a, k],
                recv_sem=fg_recv.at[a, k],
                device_id=partner,
                device_id_type=MESH,
            ).start()

    def relay_grad(a, k):
        waited(gg.at[a, k, pl.ds(0, IMAGES - 1)], gg_recv.at[a, k])
        pltpu.make_async_remote_copy(
            src_ref=gg.at[a, k, pl.ds(0, IMAGES)],
            dst_ref=gg.at[a, k, pl.ds(IMAGES, IMAGES)],
            send_sem=gr_send.at[a, k],
            recv_sem=gr_recv.at[a, k],
            device_id=partner,
            device_id_type=MESH,
        ).start()

    def forward(k):
        arrive(fin, fr, k, s > 0)
        x = fin[k].astype(F32)
        hidden = conv(x, w, 0, WIDE)
        hid[k] = hidden
        active = jnp.where(inside, hidden * sigmoid(hidden), 0.0).astype(BF16)

        @pl.when(s < SECTIONS - 1)
        def _():
            result = x[16 : 16 + POS] + conv(active.astype(F32), w, 1, POS)
            fout[k] = result.astype(BF16)
            spread(fout, fin, fsend, fr, k, 1, True)

        share_fields(k, x[8 : 8 + WIDE], active)

        @pl.when((s == 0) & (k == last))
        def _():
            transpose_weights()

    def backward(k):
        arrive(gin, br, k, s < SECTIONS - 1)
        g = gin[k].astype(F32)
        center = g[16 : 16 + POS]
        at_last = (s == 0) & (k == last)
        shared = at_last | (s == SECTIONS - 1)

        @pl.when(at_last)
        def _():
            share_grad(1, k, permuted(center.astype(BF16), sel[...]))

        grad_active = conv(g, wt, 1, WIDE)
        hidden = hid[k]
        q = sigmoid(hidden)
        slope = q * (1.0 + hidden * (1.0 - q))
        grad_hidden = jnp.where(inside, grad_active * slope, 0.0).astype(BF16)
        wide = grad_hidden.astype(F32)
        grad_in = (center + conv(wide, wt, 0, POS)).astype(BF16)
        gout[k] = grad_in

        @pl.when(s > 0)
        def _():
            spread(gout, gin, bsend, br, k, -1, True)

        gi_out[k] = permuted(swap, grad_in)
        lower = wide[8 : 8 + POS].astype(BF16)
        chunks = permuted(jnp.concatenate([lower, center.astype(BF16)], axis=0), sel[...])
        share_grad(0, k, chunks[:POS])

        @pl.when(jnp.logical_not(shared))
        def _():
            share_grad(1, k, chunks[POS:])

        @pl.when((s == 0) & (k >= 2))
        def _():
            relay_grad(1, k - 2)
            relay_grad(0, k - 2)

    def unfold(k):
        for a in range(2):
            waited(fg.at[a, k, pl.ds(IMAGES, IMAGES)], fg_recv.at[a, k])

            def source(m, carry):
                shifted = row_shifts(fg[a, k, m].astype(F32))
                for d in range(3):
                    for b in range(3):
                        cc[a, k, 3 * d + b, pl.ds(pl.multiple_of(m * POS, POS), POS), :] = shifted[d][
                            8 * b : 8 * b + POS
                        ].astype(BF16)
                return carry

            lax.fori_loop(0, PEERS, source, 0)

    def contract(a, k):
        waited(gg.at[a, k, pl.ds(IMAGES, IMAGES)], gr_recv.at[a, k])
        grads = gg[a, k].reshape(PEERS * POS, 128).T[:OUT_SHARE]
        for t in range(9):
            acc[a, t] += jnp.dot(grads, cc[a, k, t], preferred_element_type=F32)

    ahead_count = jnp.where(s == 0, CROPS + 1, jnp.where(s == 1, CROPS - 1, 0))

    def unfold_step(n, early):
        late = jnp.logical_not(early)

        @pl.when(late & (n > 1))
        def _():
            def each(a, carry):
                contract(a, n - 2)
                return carry

            lax.fori_loop(0, 2, each, 0)

        todo = early | (n >= ahead_count)

        @pl.when(todo & (n > 0))
        def _():
            unfold(n - 1)

        @pl.when(late & (n > 0))
        def _():
            relay_grad(1, n - 1)
            relay_grad(0, n - 1)

        @pl.when(todo & (n < CROPS))
        def _():
            relay_field(n)

    at_end = s == SECTIONS - 1

    def step(i, carry):
        back_from = CROPS + ahead_count
        is_forward = jnp.where(at_end, (i < 2 * CROPS) & (i % 2 == 0), i < CROPS)
        is_backward = jnp.where(
            at_end, (i < 2 * CROPS) & (i % 2 == 1), (i >= back_from) & (i < back_from + CROPS)
        )

        @pl.when(is_forward)
        def _():
            forward(jnp.where(at_end, i // 2, i))

        @pl.when(is_backward)
        def _():
            backward(jnp.where(at_end, i // 2, i - back_from))

        @pl.when(jnp.logical_not(is_forward | is_backward))
        def _():
            early = i < back_from
            unfold_step(jnp.where(early, i - CROPS, i - back_from - CROPS), early)

        return carry

    lax.fori_loop(0, 3 * CROPS + 1 + jnp.where(s == 1, ahead_count, 0), step, 0)

    def pack(t):
        for p in range(6):
            a, tap = divmod(6 * t + p, 9)
            block = acc[a, tap].astype(BF16)
            for half in range(2):
                pkl[t, half, :, 128 * p : 128 * (p + 1)] = block[:, 128 * half : 128 * (half + 1)]
        packed = permuted(pkl[t].reshape(2 * OUT_SHARE, 768), c6[...]).reshape(2, OUT_SHARE, 512)
        for half in range(2):
            for q in range(4):
                pk[t, 4 * half + q] = packed[half, :, 128 * q : 128 * (q + 1)]
        for d in (4, 3, 5, 2, 6, 1, 7):
            pltpu.make_async_remote_copy(
                src_ref=pk.at[t, (z + d) % CHIPS],
                dst_ref=rz.at[t, d - 1],
                send_sem=z_send.at[t],
                recv_sem=z_recv.at[t],
                device_id=chip_of(d),
                device_id_type=MESH,
            ).start()

    def tail(i, carry):
        first = s == 0

        @pl.when(first & (i == 2))
        def _():
            relay_grad(1, 2)
            relay_grad(0, 2)

        @pl.when(first & (i == 4))
        def _():
            relay_grad(1, last)

        @pl.when(first & (i == 6))
        def _():
            relay_grad(0, last)

        upper = ((i < 4) & (i % 2 == 0)) | (i == 4) | (i == 5)
        crop = jnp.where(i < 4, i // 2, jnp.where(i % 2 == 0, 2, last))

        @pl.when(first | (i != 6))
        def _():
            contract(jnp.where(upper, 1, 0), crop)

        @pl.when(i == 5)
        def _():
            pack(2)

        return carry

    lax.fori_loop(jnp.where(s == 0, 0, 5), 2 * CROPS, tail, 0)
    pack(1)
    pack(0)

    for t in (2, 1, 0):
        waited(rz.at[t], z_recv.at[t])
        total = pk[t, z].astype(F32)
        for d in range(CHIPS - 1):
            total = total + rz[t, d].astype(F32)
        gk_out[t] = (total * scaling).T

    for t in range(3):
        waited(rz.at[t], z_send.at[t])

    def drain(k, carry):
        @pl.when(s == 0)
        def _():
            sent(fin, edge_send, k, None)

        @pl.when(s == SECTIONS - 1)
        def _():
            sent(gin, edge_send, k, None)

        @pl.when(s < SECTIONS - 1)
        def _():
            sent(fout, fsend, k, True)

        @pl.when(s > 0)
        def _():
            sent(gout, bsend, k, True)

        waited(raw.at[k, pl.ds(0, IMAGES - 1)], raw_send.at[k])
        for a in range(2):
            waited(fs.at[a, k], fg_send.at[a, k])
            waited(gs.at[a, k], gg_send.at[a, k])
            waited(gg.at[a, k, pl.ds(0, IMAGES)], gr_send.at[a, k])
        return carry

    lax.fori_loop(0, CROPS, drain, 0)


def placed(gk, gi, gk_out, gi_out):
    gi_out[...] = gi[...]
    for n in range(18):
        a, tap = divmod(n, 9)
        t, p = divmod(n, 6)
        gk_out[tap, :, a, :] = gk[t, IN_SHARE * p : IN_SHARE * (p + 1), :]


def shards(strips, kernels, cotangent):
    scaling = 1.0 / math.sqrt(IMAGES * CROPS * ROWS * COLS * SLABS)
    dma = pltpu.SemaphoreType.DMA
    vmem = pl.BlockSpec(memory_space=pltpu.VMEM)
    hbm = pl.BlockSpec(memory_space=pl.ANY)
    gk, gi = pl.pallas_call(
        lambda *refs: kernel(scaling, *refs),
        out_shape=(
            pltpu.VMEM((3, 128, OUT_SHARE), F32),
            pltpu.VMEM((CROPS, POS, C), BF16),
        ),
        in_specs=[hbm, hbm, hbm],
        out_specs=(vmem, vmem),
        scratch_shapes=[
            pltpu.VMEM((2, 9, C, C), BF16),
            pltpu.VMEM((2, 9, C, C), BF16),
            pltpu.VMEM((CROPS, POS, C), BF16),
            pltpu.VMEM((CROPS, POS, C), BF16),
            pltpu.VMEM((CROPS, DEEP, C), BF16),
            pltpu.VMEM((CROPS, DEEP, C), BF16),
            pltpu.VMEM((CROPS, POS, C), BF16),
            pltpu.VMEM((CROPS, POS, C), BF16),
            pltpu.VMEM((CROPS, WIDE, C), F32),
            pltpu.VMEM((CROPS, IMAGES, WIDE, PAIR), BF16),
            pltpu.VMEM((2, CROPS, IMAGES, WIDE, HALF), BF16),
            pltpu.VMEM((2, CROPS, PEERS, WIDE, HALF), BF16),
            pltpu.VMEM((2, CROPS, IMAGES - 1, POS, 128), BF16),
            pltpu.VMEM((2, CROPS, PEERS, POS, 128), BF16),
            pltpu.VMEM((2, CROPS, 9, PEERS * POS, HALF), BF16),
            pltpu.VMEM((2, 9, OUT_SHARE, HALF), F32),
            pltpu.VMEM((3, 2, OUT_SHARE, 768), BF16),
            pltpu.VMEM((3, CHIPS, OUT_SHARE, 128), BF16),
            pltpu.VMEM((3, CHIPS - 1, OUT_SHARE, 128), BF16),
            pltpu.VMEM((256, 2 * HALF), BF16),
            pltpu.VMEM((2, 128, 2 * HALF), BF16),
            pltpu.VMEM((C, 512), BF16),
            pltpu.VMEM((768, 512), BF16),
            dma((2,)),
            dma((2, 9)),
            dma((CROPS, 3)),
            dma((CROPS, 3)),
            dma((CROPS, 3)),
            dma((CROPS, 3)),
            dma((CROPS, 3)),
            dma((CROPS,)),
            dma((CROPS,)),
            dma((2, CROPS)),
            dma((2, CROPS)),
            dma((2, CROPS)),
            dma((2, CROPS)),
            dma((2, CROPS)),
            dma((2, CROPS)),
            dma((3,)),
            dma((3,)),
        ],
        compiler_params=pltpu.CompilerParams(
            collective_id=0, has_side_effects=True, vmem_limit_bytes=60 * 1024 * 1024
        ),
        name="residual_step",
    )(
        strips.reshape(CROPS, POS, C),
        kernels.reshape(2, 9, C, C),
        cotangent.reshape(CROPS, POS, C),
    )
    gk, gi = pl.pallas_call(
        placed,
        out_shape=(
            jax.ShapeDtypeStruct((9, IN_SHARE, 2, OUT_SHARE), F32),
            jax.ShapeDtypeStruct((CROPS, POS, C), BF16),
        ),
        in_specs=[vmem, vmem],
        out_specs=(vmem, vmem),
        name="outputs",
    )(
        pltpu.with_memory_space_constraint(gk, pltpu.VMEM),
        pltpu.with_memory_space_constraint(gi, pltpu.VMEM),
    )
    return jnp.transpose(gk, (2, 0, 1, 3))[None], gi.reshape(1, 1, CROPS, ROWS, COLS, C)


def solution(mesh):
    return jax.shard_map(
        shards,
        mesh=mesh,
        in_specs=(
            P("img", None, None, "slab", None),
            P("section", None, None, None, None),
            P("img", None, None, "slab", None),
        ),
        out_specs=(
            P("section", None, None, "slab", "img"),
            P("section", "img", None, None, "slab", None),
        ),
        check_vma=False,
    )
```

```python
import math

import jax
import jax.numpy as jnp
from jax import lax
from jax.experimental import pallas as pl
from jax.experimental.pallas import tpu as pltpu
from jax.sharding import PartitionSpec as P

MESH = pl.DeviceIdType.MESH
F32 = jnp.float32
BF16 = jnp.bfloat16

C = 320
SECTIONS = 4
IMAGES = 4
CROPS = 4
CHIPS = 8
SLABS = 16
ROWS = 8
COLS = 8
POS = ROWS * COLS
WIDE = POS + 16
DEEP = POS + 32
OUT_SHARE = C // IMAGES
IN_SHARE = C // SLABS
HALF = 256
PEERS = 8
PAIR = 640


def iota(shape, dim):
    return lax.broadcasted_iota(jnp.int32, shape, dim)


def onehot(cond):
    return jnp.where(cond, 1.0, 0.0).astype(BF16)


def sigmoid(v):
    return 1.0 / (1.0 + jnp.exp(-v))


def row_shifts(x):
    count = x.shape[0]
    row = iota(x.shape, 0) % ROWS
    above = jnp.where(row == 0, 0.0, pltpu.roll(x, 1, 0))
    below = jnp.where(row == ROWS - 1, 0.0, pltpu.roll(x, count - 1, 0))
    return above, x, below


def conv(x, weights, part, count):
    shifted = row_shifts(x)
    total = None
    for a in range(3):
        for b in range(3):
            lhs = shifted[a][8 * b : 8 * b + count].astype(BF16)
            term = jnp.dot(lhs, weights[part, 3 * a + b], preferred_element_type=F32)
            total = term if total is None else total + term
    return total


def kernel(
    scaling,
    strips,
    kernels,
    cotangent,
    gk_out,
    gi_out,
    w,
    wt,
    sv,
    cv,
    fin,
    gin,
    fout,
    gout,
    hid,
    raw,
    fs,
    fg,
    gs,
    gg,
    cc,
    acc,
    pkl,
    pk,
    rz,
    pc,
    pct,
    sel,
    c6,
    local_sem,
    weight_sem,
    fr,
    fsend,
    br,
    bsend,
    edge_send,
    raw_recv,
    raw_send,
    fg_recv,
    fg_send,
    gg_recv,
    gg_send,
    gr_recv,
    gr_send,
    z_recv,
    z_send,
    token,
):
    s = lax.axis_index("section")
    slab = lax.axis_index("slab")
    img = lax.axis_index("img")
    z = slab // 2
    core = slab % 2
    has_left = slab > 0
    has_right = slab < SLABS - 1

    loads = [
        pltpu.make_async_copy(strips, sv, local_sem.at[0]),
        pltpu.make_async_copy(cotangent, cv, local_sem.at[1]),
    ]
    for part in range(2):
        for tap in range(9):
            loads.append(
                pltpu.make_async_copy(
                    kernels.at[part, tap], w.at[part, tap], weight_sem
                )
            )
    for load in loads:
        load.start()

    @pl.when(slab == 0)
    def _():
        for buf in (fin, gin):
            buf[:, 0:16, :] = jnp.zeros((CROPS, 16, C), BF16)

    @pl.when(slab == SLABS - 1)
    def _():
        for buf in (fin, gin):
            buf[:, DEEP - 16 : DEEP, :] = jnp.zeros((CROPS, 16, C), BF16)

    barrier = pltpu.get_barrier_semaphore()

    def greet(where):
        pl.semaphore_signal(barrier, inc=1, device_id=where, device_id_type=MESH)

    def image_of(d):
        return (s, slab, (img + d) % IMAGES)

    partner = (s, 2 * z + 1 - core, img)

    def chip_of(d):
        return (s, 2 * ((z + d) % CHIPS) + core, img)

    greeted = jnp.int32(0)
    for ds in (-1, 0, 1):
        for dj in (-1, 0, 1):
            if ds == 0 and dj == 0:
                continue
            ok = (s + ds >= 0) & (s + ds < SECTIONS) & (slab + dj >= 0) & (slab + dj < SLABS)

            @pl.when(ok)
            def _():
                greet((s + ds, slab + dj, img))

            greeted = greeted + jnp.where(ok, 1, 0)
    for d in range(1, IMAGES):
        greet(image_of(d))
    greet(partner)
    for d in (1, CHIPS - 1):
        greet(chip_of(d))
    i, j = iota((POS, POS), 0), iota((POS, POS), 1)
    swap = onehot((i // 8 == j % 8) & (i % 8 == j // 8))
    def chosen(first, shape):
        i, j = iota(shape, 0) + first, iota(shape, 1)
        lane = j % 32
        side = (j // HALF + core) % 2
        return (lane < IN_SHARE) & (i == IN_SHARE * (2 * ((j % HALF) // 32) + side) + lane)

    pc[...] = onehot(chosen(0, (256, 2 * HALF)))
    tail_row = iota((128, 2 * HALF), 0)
    pct[0] = onehot(chosen(256, (128, 2 * HALF)) & (tail_row < 64))
    pct[1] = onehot(chosen(192, (128, 2 * HALF)) & (tail_row >= 64))
    i, j = iota((C, 512), 0), iota((C, 512), 1)
    lane = j % 128
    owner = (j // 128 + img) % IMAGES
    sel[...] = onehot((lane < OUT_SHARE) & (i == OUT_SHARE * owner + lane))
    i, j = iota((768, 512), 0), iota((768, 512), 1)
    lane = i % 32
    c6[...] = onehot(
        (lane < IN_SHARE)
        & ((i % 128) // 32 == j // 128)
        & (j % 128 == IN_SHARE * (i // 128) + lane)
    )

    acc[...] = jnp.zeros_like(acc)
    pl.semaphore_wait(barrier, greeted + IMAGES + 2)

    def permuted(x, matrix):
        return jnp.dot(x, matrix, preferred_element_type=F32).astype(BF16)

    def spread(src, dst, send, recv, k, ds, center):
        base = 16 if src is dst else 0

        @pl.when(has_right)
        def _():
            pltpu.make_async_remote_copy(
                src_ref=src.at[k, pl.ds(base + POS - 16, 16)],
                dst_ref=dst.at[k, pl.ds(0, 16)],
                send_sem=send.at[2],
                recv_sem=recv.at[k],
                device_id=(s + ds, slab + 1, img),
                device_id_type=MESH,
            ).start()

        @pl.when(has_left)
        def _():
            pltpu.make_async_remote_copy(
                src_ref=src.at[k, pl.ds(base, 16)],
                dst_ref=dst.at[k, pl.ds(DEEP - 16, 16)],
                send_sem=send.at[0],
                recv_sem=recv.at[k],
                device_id=(s + ds, slab - 1, img),
                device_id_type=MESH,
            ).start()

        if center:
            pltpu.make_async_remote_copy(
                src_ref=src.at[k],
                dst_ref=dst.at[k, pl.ds(16, POS)],
                send_sem=send.at[1],
                recv_sem=recv.at[k],
                device_id=(s + ds, slab, img),
                device_id_type=MESH,
            ).start()

    def waited(ref, sem):
        pltpu.make_async_copy(ref, ref, sem).wait()

    inner = has_left & has_right

    def arrive(dst, recv, k, center):
        other = jnp.logical_not(center)
        for case, rows in (
            (center & inner, DEEP),
            (center & jnp.logical_not(inner), DEEP - 16),
            (other & inner, 32),
            (other & jnp.logical_not(inner), 16),
        ):

            @pl.when(case)
            def _():
                waited(dst.at[k, pl.ds(0, rows)], recv.at[k])

    def sent(src, send, center):
        if center:
            waited(src, send.at[1])

        @pl.when(has_right)
        def _():
            waited(src.at[:, pl.ds(0, 16)], send.at[2])

        @pl.when(has_left)
        def _():
            waited(src.at[:, pl.ds(0, 16)], send.at[0])

    loads[0].wait()
    loads[1].wait()

    def share_grad(a, k, chunks):
        gg[a, k, IMAGES - 1] = chunks[:, :128]
        for d in range(1, IMAGES):
            gs[a, k, d - 1] = chunks[:, 128 * d : 128 * (d + 1)]
            pltpu.make_async_remote_copy(
                src_ref=gs.at[a, k, d - 1],
                dst_ref=gg.at[a, k, d - 1],
                send_sem=gg_send,
                recv_sem=gg_recv.at[a, k],
                device_id=image_of(d),
                device_id_type=MESH,
            ).start()

    @pl.when(s == 0)
    def _():
        def step(k, carry):
            fin[k, 16 : 16 + POS, :] = permuted(swap, sv[k])
            spread(fin, fin, edge_send, fr, k, 0, False)
            return carry

        lax.fori_loop(0, CROPS, step, 0)

    @pl.when(s == SECTIONS - 1)
    def _():
        def step(k, carry):
            center = permuted(swap, cv[k])
            gin[k, 16 : 16 + POS, :] = center
            spread(gin, gin, edge_send, br, k, 0, False)
            share_grad(1, k, permuted(center, sel[...]))
            return carry

        lax.fori_loop(0, CROPS, step, 0)

    waited(w, weight_sem)

    def transpose_weights():
        def step(n, carry):
            part, tap = n // 9, n % 9
            wt[part, 8 - tap] = w[part, tap].T
            return carry

        lax.fori_loop(0, 18, step, 0)

    pl.when(s > 0)(transpose_weights)

    row = iota((WIDE, C), 0)
    inside = jnp.logical_not(
        ((row < 8) & (slab == 0)) | ((row >= WIDE - 8) & (slab == SLABS - 1))
    )

    last = CROPS - 1

    def share_fields(k, wide, active):
        mine = raw.at[k, IMAGES - 1]
        mine[:, 0:256] = wide[:, 0:256].astype(BF16)
        mine[:, 256:512] = active[:, 0:256]
        tails = jnp.concatenate([wide[:, 256:C], active[:, 256:C].astype(F32)], axis=1)
        mine[:, 512:PAIR] = tails.astype(BF16)
        for d in range(1, IMAGES):
            pltpu.make_async_remote_copy(
                src_ref=mine,
                dst_ref=raw.at[k, d - 1],
                send_sem=raw_send,
                recv_sem=raw_recv.at[k],
                device_id=image_of(d),
                device_id_type=MESH,
            ).start()

    def relay_field(k):
        waited(raw.at[k, pl.ds(0, IMAGES - 1)], raw_recv.at[k])
        for a in range(2):
            for n in range(IMAGES):
                both = (
                    jnp.dot(raw[k, n, :, 256 * a : 256 * (a + 1)], pc[...], preferred_element_type=F32)
                    + jnp.dot(raw[k, n, :, 512:PAIR], pct[a], preferred_element_type=F32)
                ).astype(BF16)
                fg[a, k, n] = both[:, :HALF]
                fs[a, k, n] = both[:, HALF:]
            pltpu.make_async_remote_copy(
                src_ref=fs.at[a, k],
                dst_ref=fg.at[a, k, pl.ds(IMAGES, IMAGES)],
                send_sem=fg_send,
                recv_sem=fg_recv.at[a, k],
                device_id=partner,
                device_id_type=MESH,
            ).start()

    def relay_grad(a, k):
        waited(gg.at[a, k, pl.ds(0, IMAGES - 1)], gg_recv.at[a, k])
        pltpu.make_async_remote_copy(
            src_ref=gg.at[a, k, pl.ds(0, IMAGES)],
            dst_ref=gg.at[a, k, pl.ds(IMAGES, IMAGES)],
            send_sem=gr_send,
            recv_sem=gr_recv.at[a, k],
            device_id=partner,
            device_id_type=MESH,
        ).start()

    def forward(k):
        arrive(fin, fr, k, s > 0)
        x = fin[k].astype(F32)
        hidden = conv(x, w, 0, WIDE)
        hid[k] = hidden
        active = jnp.where(inside, hidden * sigmoid(hidden), 0.0).astype(BF16)

        @pl.when(s < SECTIONS - 1)
        def _():
            result = x[16 : 16 + POS] + conv(active.astype(F32), w, 1, POS)
            fout[k] = result.astype(BF16)
            spread(fout, fin, fsend, fr, k, 1, True)

        share_fields(k, x[8 : 8 + WIDE], active)

        @pl.when((s == 0) & (k == last))
        def _():
            transpose_weights()

    def backward(k):
        arrive(gin, br, k, s < SECTIONS - 1)
        g = gin[k].astype(F32)
        center = g[16 : 16 + POS]
        at_last = (s == 0) & (k == last)
        shared = at_last | (s == SECTIONS - 1)

        @pl.when(at_last)
        def _():
            share_grad(1, k, permuted(center.astype(BF16), sel[...]))

        grad_active = conv(g, wt, 1, WIDE)
        hidden = hid[k]
        q = sigmoid(hidden)
        slope = q * (1.0 + hidden * (1.0 - q))
        grad_hidden = jnp.where(inside, grad_active * slope, 0.0).astype(BF16)
        wide = grad_hidden.astype(F32)
        grad_in = (center + conv(wide, wt, 0, POS)).astype(BF16)
        gout[k] = grad_in

        @pl.when(s > 0)
        def _():
            spread(gout, gin, bsend, br, k, -1, True)

        gi_out[k] = permuted(swap, grad_in)
        lower = wide[8 : 8 + POS].astype(BF16)
        chunks = permuted(jnp.concatenate([lower, center.astype(BF16)], axis=0), sel[...])
        share_grad(0, k, chunks[:POS])

        @pl.when(jnp.logical_not(shared))
        def _():
            share_grad(1, k, chunks[POS:])

        @pl.when((s == 0) & (k >= 2))
        def _():
            relay_grad(1, k - 2)
            relay_grad(0, k - 2)

    def unfold(k):
        for a in range(2):
            waited(fg.at[a, k, pl.ds(IMAGES, IMAGES)], fg_recv.at[a, k])

            def source(m, carry):
                shifted = row_shifts(fg[a, k, m].astype(F32))
                for d in range(3):
                    for b in range(3):
                        cc[a, k, 3 * d + b, pl.ds(pl.multiple_of(m * POS, POS), POS), :] = shifted[d][
                            8 * b : 8 * b + POS
                        ].astype(BF16)
                return carry

            lax.fori_loop(0, PEERS, source, 0)

    def contract(a, k):
        waited(gg.at[a, k, pl.ds(IMAGES, IMAGES)], gr_recv.at[a, k])
        grads = gg[a, k].reshape(PEERS * POS, 128).T[:OUT_SHARE]
        for t in range(9):
            acc[a, t] += jnp.dot(grads, cc[a, k, t], preferred_element_type=F32)

    ahead_count = jnp.where(s == 0, CROPS + 1, jnp.where(s == 1, CROPS - 1, 0))

    def unfold_step(n, early):
        late = jnp.logical_not(early)

        @pl.when(late & (n > 1))
        def _():
            def each(a, carry):
                contract(a, n - 2)
                return carry

            lax.fori_loop(0, 2, each, 0)

        todo = early | (n >= ahead_count)

        @pl.when(todo & (n > 0))
        def _():
            unfold(n - 1)

        @pl.when(late & (n > 0))
        def _():
            relay_grad(1, n - 1)
            relay_grad(0, n - 1)

        @pl.when(todo & (n < CROPS))
        def _():
            relay_field(n)

    at_end = s == SECTIONS - 1

    def step(i, carry):
        turn = i - CROPS

        @pl.when((turn > 0) & (turn <= 3))
        def _():
            pl.semaphore_wait(token.at[turn - 1], 2)

        @pl.when((turn >= 0) & (turn < 3))
        def _():
            for d in (1, CHIPS - 1):
                pl.semaphore_signal(
                    token.at[turn], inc=1, device_id=chip_of(d), device_id_type=MESH
                )

        back_from = CROPS + ahead_count
        is_forward = jnp.where(at_end, (i < 2 * CROPS) & (i % 2 == 0), i < CROPS)
        is_backward = jnp.where(
            at_end, (i < 2 * CROPS) & (i % 2 == 1), (i >= back_from) & (i < back_from + CROPS)
        )

        @pl.when(is_forward)
        def _():
            forward(jnp.where(at_end, i // 2, i))

        @pl.when(is_backward)
        def _():
            backward(jnp.where(at_end, i // 2, i - back_from))

        @pl.when(jnp.logical_not(is_forward | is_backward))
        def _():
            early = i < back_from
            unfold_step(jnp.where(early, i - CROPS, i - back_from - CROPS), early)

        return carry

    lax.fori_loop(0, 3 * CROPS + 1 + jnp.where(s == 1, ahead_count, 0), step, 0)

    def pack(t):
        for p in range(6):
            a, tap = divmod(6 * t + p, 9)
            block = acc[a, tap].astype(BF16)
            for half in range(2):
                pkl[t, half, :, 128 * p : 128 * (p + 1)] = block[:, 128 * half : 128 * (half + 1)]
        packed = permuted(pkl[t].reshape(2 * OUT_SHARE, 768), c6[...]).reshape(2, OUT_SHARE, 512)
        for half in range(2):
            for q in range(4):
                pk[t, 4 * half + q] = packed[half, :, 128 * q : 128 * (q + 1)]
        for d in (4, 3, 5, 2, 6, 1, 7):
            pltpu.make_async_remote_copy(
                src_ref=pk.at[t, (z + d) % CHIPS],
                dst_ref=rz.at[t, d - 1],
                send_sem=z_send,
                recv_sem=z_recv.at[t],
                device_id=chip_of(d),
                device_id_type=MESH,
            ).start()

    def tail(i, carry):
        first = s == 0

        @pl.when(first & (i == 2))
        def _():
            relay_grad(1, 2)
            relay_grad(0, 2)

        @pl.when(first & (i == 4))
        def _():
            relay_grad(1, last)

        @pl.when(first & (i == 6))
        def _():
            relay_grad(0, last)

        upper = ((i < 4) & (i % 2 == 0)) | (i == 4) | (i == 5)
        crop = jnp.where(i < 4, i // 2, jnp.where(i % 2 == 0, 2, last))

        @pl.when(first | (i != 6))
        def _():
            contract(jnp.where(upper, 1, 0), crop)

        @pl.when(i == 5)
        def _():
            pack(2)

        return carry

    lax.fori_loop(jnp.where(s == 0, 0, 5), 2 * CROPS, tail, 0)
    pack(1)
    pack(0)

    for t in (2, 1, 0):
        waited(rz.at[t], z_recv.at[t])
        total = pk[t, z].astype(F32)
        for d in range(CHIPS - 1):
            total = total + rz[t, d].astype(F32)
        gk_out[t] = (total * scaling).T

    waited(rz, z_send)
    waited(raw.at[:, pl.ds(0, IMAGES - 1)], raw_send)
    waited(fs, fg_send)
    waited(gs, gg_send)
    waited(gg.at[:, :, pl.ds(0, IMAGES)], gr_send)

    @pl.when(s == 0)
    def _():
        sent(fin, edge_send, False)

    @pl.when(s == SECTIONS - 1)
    def _():
        sent(gin, edge_send, False)

    @pl.when(s < SECTIONS - 1)
    def _():
        sent(fout, fsend, True)

    @pl.when(s > 0)
    def _():
        sent(gout, bsend, True)


def placed(gk, gi, gk_out, gi_out):
    gi_out[...] = gi[...]
    for n in range(18):
        a, tap = divmod(n, 9)
        t, p = divmod(n, 6)
        gk_out[tap, :, a, :] = gk[t, IN_SHARE * p : IN_SHARE * (p + 1), :]


def shards(strips, kernels, cotangent):
    scaling = 1.0 / math.sqrt(IMAGES * CROPS * ROWS * COLS * SLABS)
    dma = pltpu.SemaphoreType.DMA
    vmem = pl.BlockSpec(memory_space=pltpu.VMEM)
    hbm = pl.BlockSpec(memory_space=pl.ANY)
    gk, gi = pl.pallas_call(
        lambda *refs: kernel(scaling, *refs),
        out_shape=(
            pltpu.VMEM((3, 128, OUT_SHARE), F32),
            pltpu.VMEM((CROPS, POS, C), BF16),
        ),
        in_specs=[hbm, hbm, hbm],
        out_specs=(vmem, vmem),
        scratch_shapes=[
            pltpu.VMEM((2, 9, C, C), BF16),
            pltpu.VMEM((2, 9, C, C), BF16),
            pltpu.VMEM((CROPS, POS, C), BF16),
            pltpu.VMEM((CROPS, POS, C), BF16),
            pltpu.VMEM((CROPS, DEEP, C), BF16),
            pltpu.VMEM((CROPS, DEEP, C), BF16),
            pltpu.VMEM((CROPS, POS, C), BF16),
            pltpu.VMEM((CROPS, POS, C), BF16),
            pltpu.VMEM((CROPS, WIDE, C), F32),
            pltpu.VMEM((CROPS, IMAGES, WIDE, PAIR), BF16),
            pltpu.VMEM((2, CROPS, IMAGES, WIDE, HALF), BF16),
            pltpu.VMEM((2, CROPS, PEERS, WIDE, HALF), BF16),
            pltpu.VMEM((2, CROPS, IMAGES - 1, POS, 128), BF16),
            pltpu.VMEM((2, CROPS, PEERS, POS, 128), BF16),
            pltpu.VMEM((2, CROPS, 9, PEERS * POS, HALF), BF16),
            pltpu.VMEM((2, 9, OUT_SHARE, HALF), F32),
            pltpu.VMEM((3, 2, OUT_SHARE, 768), BF16),
            pltpu.VMEM((3, CHIPS, OUT_SHARE, 128), BF16),
            pltpu.VMEM((3, CHIPS - 1, OUT_SHARE, 128), BF16),
            pltpu.VMEM((256, 2 * HALF), BF16),
            pltpu.VMEM((2, 128, 2 * HALF), BF16),
            pltpu.VMEM((C, 512), BF16),
            pltpu.VMEM((768, 512), BF16),
            dma((2,)),
            dma,
            dma((CROPS,)),
            dma((3,)),
            dma((CROPS,)),
            dma((3,)),
            dma((3,)),
            dma((CROPS,)),
            dma,
            dma((2, CROPS)),
            dma,
            dma((2, CROPS)),
            dma,
            dma((2, CROPS)),
            dma,
            dma((3,)),
            dma,
            pltpu.SemaphoreType.REGULAR((3,)),
        ],
        compiler_params=pltpu.CompilerParams(
            collective_id=0, has_side_effects=True, vmem_limit_bytes=60 * 1024 * 1024
        ),
        name="residual_step",
    )(
        strips.reshape(CROPS, POS, C),
        kernels.reshape(2, 9, C, C),
        cotangent.reshape(CROPS, POS, C),
    )
    gk, gi = pl.pallas_call(
        placed,
        out_shape=(
            jax.ShapeDtypeStruct((9, IN_SHARE, 2, OUT_SHARE), F32),
            jax.ShapeDtypeStruct((CROPS, POS, C), BF16),
        ),
        in_specs=[vmem, vmem],
        out_specs=(vmem, vmem),
        name="outputs",
    )(
        pltpu.with_memory_space_constraint(gk, pltpu.VMEM),
        pltpu.with_memory_space_constraint(gi, pltpu.VMEM),
    )
    return jnp.transpose(gk, (2, 0, 1, 3))[None], gi.reshape(1, 1, CROPS, ROWS, COLS, C)


def solution(mesh):
    return jax.shard_map(
        shards,
        mesh=mesh,
        in_specs=(
            P("img", None, None, "slab", None),
            P("section", None, None, None, None),
            P("img", None, None, "slab", None),
        ),
        out_specs=(
            P("section", None, None, "slab", "img"),
            P("section", "img", None, None, "slab", None),
        ),
        check_vma=False,
    )
```

```python
import math

import jax
import jax.numpy as jnp
from jax import lax
from jax.experimental import pallas as pl
from jax.experimental.pallas import tpu as pltpu
from jax.sharding import PartitionSpec as P

MESH = pl.DeviceIdType.MESH
F32 = jnp.float32
BF16 = jnp.bfloat16

C = 320
SECTIONS = 4
IMAGES = 4
CROPS = 4
CHIPS = 8
SLABS = 16
ROWS = 8
COLS = 8
POS = ROWS * COLS
WIDE = POS + 16
DEEP = POS + 32
OUT_SHARE = C // IMAGES
IN_SHARE = C // SLABS
HALF = 256
PEERS = 8
PAIR = 640


def iota(shape, dim):
    return lax.broadcasted_iota(jnp.int32, shape, dim)


def onehot(cond):
    return jnp.where(cond, 1.0, 0.0).astype(BF16)


def sigmoid(v):
    return 1.0 / (1.0 + jnp.exp(-v))


def row_shifts(x):
    count = x.shape[0]
    row = iota(x.shape, 0) % ROWS
    above = jnp.where(row == 0, 0.0, pltpu.roll(x, 1, 0))
    below = jnp.where(row == ROWS - 1, 0.0, pltpu.roll(x, count - 1, 0))
    return above, x, below


def conv(x, weights, part, count):
    shifted = row_shifts(x)
    total = None
    for a in range(3):
        for b in range(3):
            lhs = shifted[a][8 * b : 8 * b + count].astype(BF16)
            term = jnp.dot(lhs, weights[part, 3 * a + b], preferred_element_type=F32)
            total = term if total is None else total + term
    return total


def kernel(
    scaling,
    strips,
    kernels,
    cotangent,
    gk_out,
    gi_out,
    w,
    wt,
    sv,
    cv,
    fin,
    gin,
    fout,
    gout,
    hid,
    raw,
    fs,
    fg,
    gs,
    us,
    gg,
    cc,
    acc,
    pkl,
    pk,
    rz,
    pc,
    pct,
    sel,
    c6,
    local_sem,
    weight_sem,
    fr,
    fsend,
    br,
    bsend,
    edge_send,
    raw_recv,
    raw_send,
    fg_recv,
    fg_send,
    gg_recv,
    gg_send,
    up_send,
    gr_recv,
    gr_send,
    z_recv,
    z_send,
    token,
):
    s = lax.axis_index("section")
    slab = lax.axis_index("slab")
    img = lax.axis_index("img")
    z = slab // 2
    core = slab % 2
    has_left = slab > 0
    has_right = slab < SLABS - 1

    loads = [
        pltpu.make_async_copy(strips, sv, local_sem.at[0]),
        pltpu.make_async_copy(cotangent, cv, local_sem.at[1]),
    ]
    for part in range(2):
        for tap in range(9):
            loads.append(
                pltpu.make_async_copy(
                    kernels.at[part, tap], w.at[part, tap], weight_sem
                )
            )
    for load in loads:
        load.start()

    @pl.when(slab == 0)
    def _():
        for buf in (fin, gin):
            buf[:, 0:16, :] = jnp.zeros((CROPS, 16, C), BF16)

    @pl.when(slab == SLABS - 1)
    def _():
        for buf in (fin, gin):
            buf[:, DEEP - 16 : DEEP, :] = jnp.zeros((CROPS, 16, C), BF16)

    barrier = pltpu.get_barrier_semaphore()

    def greet(where):
        pl.semaphore_signal(barrier, inc=1, device_id=where, device_id_type=MESH)

    def image_of(d):
        return (s, slab, (img + d) % IMAGES)

    partner = (s, 2 * z + 1 - core, img)

    def chip_of(d):
        return (s, 2 * ((z + d) % CHIPS) + core, img)

    greeted = jnp.int32(0)
    for ds in (-1, 0, 1):
        for dj in (-1, 0, 1):
            if ds == 0 and dj == 0:
                continue
            ok = (s + ds >= 0) & (s + ds < SECTIONS) & (slab + dj >= 0) & (slab + dj < SLABS)

            @pl.when(ok)
            def _():
                greet((s + ds, slab + dj, img))

            greeted = greeted + jnp.where(ok, 1, 0)
    for d in range(1, IMAGES):
        greet(image_of(d))
    greet(partner)
    for d in (1, CHIPS - 1):
        greet(chip_of(d))
    i, j = iota((POS, POS), 0), iota((POS, POS), 1)
    swap = onehot((i // 8 == j % 8) & (i % 8 == j // 8))
    def chosen(first, shape):
        i, j = iota(shape, 0) + first, iota(shape, 1)
        lane = j % 32
        side = (j // HALF + core) % 2
        return (lane < IN_SHARE) & (i == IN_SHARE * (2 * ((j % HALF) // 32) + side) + lane)

    pc[...] = onehot(chosen(0, (256, 2 * HALF)))
    tail_row = iota((128, 2 * HALF), 0)
    pct[0] = onehot(chosen(256, (128, 2 * HALF)) & (tail_row < 64))
    pct[1] = onehot(chosen(192, (128, 2 * HALF)) & (tail_row >= 64))
    i, j = iota((C, 512), 0), iota((C, 512), 1)
    lane = j % 128
    owner = (j // 128 + img) % IMAGES
    sel[...] = onehot((lane < OUT_SHARE) & (i == OUT_SHARE * owner + lane))
    i, j = iota((768, 512), 0), iota((768, 512), 1)
    lane = i % 32
    c6[...] = onehot(
        (lane < IN_SHARE)
        & ((i % 128) // 32 == j // 128)
        & (j % 128 == IN_SHARE * (i // 128) + lane)
    )

    acc[...] = jnp.zeros_like(acc)
    pl.semaphore_wait(barrier, greeted + IMAGES + 2)

    def permuted(x, matrix):
        return jnp.dot(x, matrix, preferred_element_type=F32).astype(BF16)

    def spread(src, dst, send, recv, k, ds, center):
        base = 16 if src is dst else 0

        @pl.when(has_right)
        def _():
            pltpu.make_async_remote_copy(
                src_ref=src.at[k, pl.ds(base + POS - 16, 16)],
                dst_ref=dst.at[k, pl.ds(0, 16)],
                send_sem=send.at[2],
                recv_sem=recv.at[k],
                device_id=(s + ds, slab + 1, img),
                device_id_type=MESH,
            ).start()

        @pl.when(has_left)
        def _():
            pltpu.make_async_remote_copy(
                src_ref=src.at[k, pl.ds(base, 16)],
                dst_ref=dst.at[k, pl.ds(DEEP - 16, 16)],
                send_sem=send.at[0],
                recv_sem=recv.at[k],
                device_id=(s + ds, slab - 1, img),
                device_id_type=MESH,
            ).start()

        if center:
            pltpu.make_async_remote_copy(
                src_ref=src.at[k],
                dst_ref=dst.at[k, pl.ds(16, POS)],
                send_sem=send.at[1],
                recv_sem=recv.at[k],
                device_id=(s + ds, slab, img),
                device_id_type=MESH,
            ).start()

    def waited(ref, sem):
        pltpu.make_async_copy(ref, ref, sem).wait()

    inner = has_left & has_right

    def arrive(dst, recv, k, center):
        other = jnp.logical_not(center)
        for case, rows in (
            (center & inner, DEEP),
            (center & jnp.logical_not(inner), DEEP - 16),
            (other & inner, 32),
            (other & jnp.logical_not(inner), 16),
        ):

            @pl.when(case)
            def _():
                waited(dst.at[k, pl.ds(0, rows)], recv.at[k])

    def sent(src, send, center):
        if center:
            waited(src, send.at[1])

        @pl.when(has_right)
        def _():
            waited(src.at[:, pl.ds(0, 16)], send.at[2])

        @pl.when(has_left)
        def _():
            waited(src.at[:, pl.ds(0, 16)], send.at[0])

    loads[0].wait()
    loads[1].wait()

    def share_grad(a, k, chunks):
        gg[a, k, IMAGES - 1] = chunks[:, :128]
        for d in range(1, IMAGES):
            gs[a, k, d - 1] = chunks[:, 128 * d : 128 * (d + 1)]
            pltpu.make_async_remote_copy(
                src_ref=gs.at[a, k, d - 1],
                dst_ref=gg.at[a, k, d - 1],
                send_sem=gg_send.at[a],
                recv_sem=gg_recv.at[a, k],
                device_id=image_of(d),
                device_id_type=MESH,
            ).start()

    @pl.when(s == 0)
    def _():
        def step(k, carry):
            fin[k, 16 : 16 + POS, :] = permuted(swap, sv[k])
            spread(fin, fin, edge_send, fr, k, 0, False)
            return carry

        lax.fori_loop(0, CROPS, step, 0)

    @pl.when(s == SECTIONS - 1)
    def _():
        def step(k, carry):
            center = permuted(swap, cv[k])
            gin[k, 16 : 16 + POS, :] = center
            spread(gin, gin, edge_send, br, k, 0, False)
            share_grad(1, k, permuted(center, sel[...]))
            return carry

        lax.fori_loop(0, CROPS, step, 0)

    waited(w, weight_sem)

    def transpose_weights():
        def step(n, carry):
            part, tap = n // 9, n % 9
            wt[part, 8 - tap] = w[part, tap].T
            return carry

        lax.fori_loop(0, 18, step, 0)

    pl.when(s > 0)(transpose_weights)

    row = iota((WIDE, C), 0)
    inside = jnp.logical_not(
        ((row < 8) & (slab == 0)) | ((row >= WIDE - 8) & (slab == SLABS - 1))
    )

    last = CROPS - 1

    def share_fields(k, wide, active):
        mine = raw.at[k, IMAGES - 1]
        mine[:, 0:256] = wide[:, 0:256].astype(BF16)
        mine[:, 256:512] = active[:, 0:256]
        tails = jnp.concatenate([wide[:, 256:C], active[:, 256:C].astype(F32)], axis=1)
        mine[:, 512:PAIR] = tails.astype(BF16)
        for d in range(1, IMAGES):
            pltpu.make_async_remote_copy(
                src_ref=mine,
                dst_ref=raw.at[k, d - 1],
                send_sem=raw_send,
                recv_sem=raw_recv.at[k],
                device_id=image_of(d),
                device_id_type=MESH,
            ).start()

    def relay_field(k):
        waited(raw.at[k, pl.ds(0, IMAGES - 1)], raw_recv.at[k])
        for a in range(2):
            for n in range(IMAGES):
                both = (
                    jnp.dot(raw[k, n, :, 256 * a : 256 * (a + 1)], pc[...], preferred_element_type=F32)
                    + jnp.dot(raw[k, n, :, 512:PAIR], pct[a], preferred_element_type=F32)
                ).astype(BF16)
                fg[a, k, n] = both[:, :HALF]
                fs[a, k, n] = both[:, HALF:]
            pltpu.make_async_remote_copy(
                src_ref=fs.at[a, k],
                dst_ref=fg.at[a, k, pl.ds(IMAGES, IMAGES)],
                send_sem=fg_send,
                recv_sem=fg_recv.at[a, k],
                device_id=partner,
                device_id_type=MESH,
            ).start()

    def relay_grad(a, k, slots=IMAGES - 1):
        waited(gg.at[a, k, pl.ds(0, slots)], gg_recv.at[a, k])
        pltpu.make_async_remote_copy(
            src_ref=gg.at[a, k, pl.ds(0, IMAGES)],
            dst_ref=gg.at[a, k, pl.ds(IMAGES, IMAGES)],
            send_sem=gr_send,
            recv_sem=gr_recv.at[a, k],
            device_id=partner,
            device_id_type=MESH,
        ).start()

    def forward(k):
        arrive(fin, fr, k, s > 0)
        x = fin[k].astype(F32)
        hidden = conv(x, w, 0, WIDE)
        hid[k] = hidden
        active = jnp.where(inside, hidden * sigmoid(hidden), 0.0).astype(BF16)

        @pl.when(s < SECTIONS - 1)
        def _():
            result = x[16 : 16 + POS] + conv(active.astype(F32), w, 1, POS)
            fout[k] = result.astype(BF16)
            spread(fout, fin, fsend, fr, k, 1, True)

        share_fields(k, x[8 : 8 + WIDE], active)

        @pl.when((s == 0) & (k == last))
        def _():
            transpose_weights()

    def backward(k):
        arrive(gin, br, k, s < SECTIONS - 1)
        g = gin[k].astype(F32)
        center = g[16 : 16 + POS]
        shared = ((s == 0) & (k == last)) | (s == SECTIONS - 1)
        grad_active = conv(g, wt, 1, WIDE)
        hidden = hid[k]
        q = sigmoid(hidden)
        slope = q * (1.0 + hidden * (1.0 - q))
        grad_hidden = jnp.where(inside, grad_active * slope, 0.0).astype(BF16)
        wide = grad_hidden.astype(F32)
        grad_in = (center + conv(wide, wt, 0, POS)).astype(BF16)
        gout[k] = grad_in

        @pl.when(s > 0)
        def _():
            spread(gout, gin, bsend, br, k, -1, True)

        @pl.when((s == 1) & (k == last))
        def _():
            above = permuted(grad_in, sel[...])
            for d in range(IMAGES):
                us[d] = above[:, 128 * d : 128 * (d + 1)]
                pltpu.make_async_remote_copy(
                    src_ref=us.at[d],
                    dst_ref=gg.at[1, k, (d + IMAGES - 1) % IMAGES],
                    send_sem=up_send,
                    recv_sem=gg_recv.at[1, k],
                    device_id=(s - 1, slab, (img + d) % IMAGES),
                    device_id_type=MESH,
                ).start()

        gi_out[k] = permuted(swap, grad_in)
        lower = wide[8 : 8 + POS].astype(BF16)
        chunks = permuted(jnp.concatenate([lower, center.astype(BF16)], axis=0), sel[...])
        share_grad(0, k, chunks[:POS])

        @pl.when(jnp.logical_not(shared))
        def _():
            share_grad(1, k, chunks[POS:])

        @pl.when((s == 0) & (k >= 2))
        def _():
            relay_grad(1, k - 2)
            relay_grad(0, k - 2)

    def unfold(k):
        for a in range(2):
            waited(fg.at[a, k, pl.ds(IMAGES, IMAGES)], fg_recv.at[a, k])

            def source(m, carry):
                shifted = row_shifts(fg[a, k, m].astype(F32))
                for d in range(3):
                    for b in range(3):
                        cc[a, k, 3 * d + b, pl.ds(pl.multiple_of(m * POS, POS), POS), :] = shifted[d][
                            8 * b : 8 * b + POS
                        ].astype(BF16)
                return carry

            lax.fori_loop(0, PEERS, source, 0)

    def contract(a, k):
        waited(gg.at[a, k, pl.ds(IMAGES, IMAGES)], gr_recv.at[a, k])
        grads = gg[a, k].reshape(PEERS * POS, 128).T[:OUT_SHARE]
        for t in range(9):
            acc[a, t] += jnp.dot(grads, cc[a, k, t], preferred_element_type=F32)

    ahead_count = jnp.where(s == 0, CROPS + 1, jnp.where(s == 1, CROPS - 1, 0))

    def unfold_step(n, early):
        late = jnp.logical_not(early)

        @pl.when(late & (n > 1))
        def _():
            def each(a, carry):
                contract(a, n - 2)
                return carry

            lax.fori_loop(0, 2, each, 0)

        todo = early | (n >= ahead_count)

        @pl.when(todo & (n > 0))
        def _():
            unfold(n - 1)

        @pl.when(late & (n > 0))
        def _():
            relay_grad(1, n - 1)
            relay_grad(0, n - 1)

        @pl.when(todo & (n < CROPS))
        def _():
            relay_field(n)

    at_end = s == SECTIONS - 1

    def step(i, carry):
        turn = i - jnp.where(s == 0, CROPS, 2 * CROPS + ahead_count)

        @pl.when((turn > 0) & (turn <= 3))
        def _():
            pl.semaphore_wait(token.at[turn - 1], 2)

        @pl.when((turn >= 0) & (turn < 3))
        def _():
            for d in (1, CHIPS - 1):
                pl.semaphore_signal(
                    token.at[turn], inc=1, device_id=chip_of(d), device_id_type=MESH
                )

        back_from = CROPS + ahead_count
        is_forward = jnp.where(at_end, (i < 2 * CROPS) & (i % 2 == 0), i < CROPS)
        is_backward = jnp.where(
            at_end, (i < 2 * CROPS) & (i % 2 == 1), (i >= back_from) & (i < back_from + CROPS)
        )

        @pl.when(is_forward)
        def _():
            forward(jnp.where(at_end, i // 2, i))

        @pl.when(is_backward)
        def _():
            backward(jnp.where(at_end, i // 2, i - back_from))

        @pl.when(jnp.logical_not(is_forward | is_backward))
        def _():
            early = i < back_from
            unfold_step(jnp.where(early, i - CROPS, i - back_from - CROPS), early)

        return carry

    lax.fori_loop(0, 3 * CROPS + 1 + jnp.where(s == 1, ahead_count, 0), step, 0)

    def pack(t):
        for p in range(6):
            a, tap = divmod(6 * t + p, 9)
            block = acc[a, tap].astype(BF16)
            for half in range(2):
                pkl[t, half, :, 128 * p : 128 * (p + 1)] = block[:, 128 * half : 128 * (half + 1)]
        packed = permuted(pkl[t].reshape(2 * OUT_SHARE, 768), c6[...]).reshape(2, OUT_SHARE, 512)
        for half in range(2):
            for q in range(4):
                pk[t, 4 * half + q] = packed[half, :, 128 * q : 128 * (q + 1)]
        for d in (4, 3, 5, 2, 6, 1, 7):
            pltpu.make_async_remote_copy(
                src_ref=pk.at[t, (z + d) % CHIPS],
                dst_ref=rz.at[t, d - 1],
                send_sem=z_send,
                recv_sem=z_recv.at[t],
                device_id=chip_of(d),
                device_id_type=MESH,
            ).start()

    def tail(i, carry):
        first = s == 0

        @pl.when(first & (i == 2))
        def _():
            relay_grad(1, 2)
            relay_grad(0, 2)

        @pl.when(first & (i == 4))
        def _():
            relay_grad(1, last, IMAGES)

        @pl.when(first & (i == 6))
        def _():
            relay_grad(0, last)

        upper = ((i < 4) & (i % 2 == 0)) | (i == 4) | (i == 5)
        crop = jnp.where(i < 4, i // 2, jnp.where(i % 2 == 0, 2, last))

        @pl.when(first | (i != 6))
        def _():
            contract(jnp.where(upper, 1, 0), crop)

        @pl.when(i == 5)
        def _():
            pack(2)

        return carry

    lax.fori_loop(jnp.where(s == 0, 0, 5), 2 * CROPS, tail, 0)
    pack(1)
    pack(0)

    for t in (2, 1, 0):
        waited(rz.at[t], z_recv.at[t])
        total = pk[t, z].astype(F32)
        for d in range(CHIPS - 1):
            total = total + rz[t, d].astype(F32)
        gk_out[t] = (total * scaling).T

    waited(rz, z_send)
    waited(raw.at[:, pl.ds(0, IMAGES - 1)], raw_send)
    waited(fs, fg_send)
    waited(gs.at[0], gg_send.at[0])

    @pl.when(s == 0)
    def _():
        waited(gs.at[1, pl.ds(0, last)], gg_send.at[1])

    @pl.when(s > 0)
    def _():
        waited(gs.at[1], gg_send.at[1])

    @pl.when(s == 1)
    def _():
        waited(us, up_send)

    waited(gg.at[:, :, pl.ds(0, IMAGES)], gr_send)

    @pl.when(s == 0)
    def _():
        sent(fin, edge_send, False)

    @pl.when(s == SECTIONS - 1)
    def _():
        sent(gin, edge_send, False)

    @pl.when(s < SECTIONS - 1)
    def _():
        sent(fout, fsend, True)

    @pl.when(s > 0)
    def _():
        sent(gout, bsend, True)


def placed(gk, gi, gk_out, gi_out):
    gi_out[...] = gi[...]
    for n in range(18):
        a, tap = divmod(n, 9)
        t, p = divmod(n, 6)
        gk_out[tap, :, a, :] = gk[t, IN_SHARE * p : IN_SHARE * (p + 1), :]


def shards(strips, kernels, cotangent):
    scaling = 1.0 / math.sqrt(IMAGES * CROPS * ROWS * COLS * SLABS)
    dma = pltpu.SemaphoreType.DMA
    vmem = pl.BlockSpec(memory_space=pltpu.VMEM)
    hbm = pl.BlockSpec(memory_space=pl.ANY)
    gk, gi = pl.pallas_call(
        lambda *refs: kernel(scaling, *refs),
        out_shape=(
            pltpu.VMEM((3, 128, OUT_SHARE), F32),
            pltpu.VMEM((CROPS, POS, C), BF16),
        ),
        in_specs=[hbm, hbm, hbm],
        out_specs=(vmem, vmem),
        scratch_shapes=[
            pltpu.VMEM((2, 9, C, C), BF16),
            pltpu.VMEM((2, 9, C, C), BF16),
            pltpu.VMEM((CROPS, POS, C), BF16),
            pltpu.VMEM((CROPS, POS, C), BF16),
            pltpu.VMEM((CROPS, DEEP, C), BF16),
            pltpu.VMEM((CROPS, DEEP, C), BF16),
            pltpu.VMEM((CROPS, POS, C), BF16),
            pltpu.VMEM((CROPS, POS, C), BF16),
            pltpu.VMEM((CROPS, WIDE, C), F32),
            pltpu.VMEM((CROPS, IMAGES, WIDE, PAIR), BF16),
            pltpu.VMEM((2, CROPS, IMAGES, WIDE, HALF), BF16),
            pltpu.VMEM((2, CROPS, PEERS, WIDE, HALF), BF16),
            pltpu.VMEM((2, CROPS, IMAGES - 1, POS, 128), BF16),
            pltpu.VMEM((IMAGES, POS, 128), BF16),
            pltpu.VMEM((2, CROPS, PEERS, POS, 128), BF16),
            pltpu.VMEM((2, CROPS, 9, PEERS * POS, HALF), BF16),
            pltpu.VMEM((2, 9, OUT_SHARE, HALF), F32),
            pltpu.VMEM((3, 2, OUT_SHARE, 768), BF16),
            pltpu.VMEM((3, CHIPS, OUT_SHARE, 128), BF16),
            pltpu.VMEM((3, CHIPS - 1, OUT_SHARE, 128), BF16),
            pltpu.VMEM((256, 2 * HALF), BF16),
            pltpu.VMEM((2, 128, 2 * HALF), BF16),
            pltpu.VMEM((C, 512), BF16),
            pltpu.VMEM((768, 512), BF16),
            dma((2,)),
            dma,
            dma((CROPS,)),
            dma((3,)),
            dma((CROPS,)),
            dma((3,)),
            dma((3,)),
            dma((CROPS,)),
            dma,
            dma((2, CROPS)),
            dma,
            dma((2, CROPS)),
            dma((2,)),
            dma,
            dma((2, CROPS)),
            dma,
            dma((3,)),
            dma,
            pltpu.SemaphoreType.REGULAR((3,)),
        ],
        compiler_params=pltpu.CompilerParams(
            collective_id=0, has_side_effects=True, vmem_limit_bytes=60 * 1024 * 1024
        ),
        name="residual_step",
    )(
        strips.reshape(CROPS, POS, C),
        kernels.reshape(2, 9, C, C),
        cotangent.reshape(CROPS, POS, C),
    )
    gk, gi = pl.pallas_call(
        placed,
        out_shape=(
            jax.ShapeDtypeStruct((9, IN_SHARE, 2, OUT_SHARE), F32),
            jax.ShapeDtypeStruct((CROPS, POS, C), BF16),
        ),
        in_specs=[vmem, vmem],
        out_specs=(vmem, vmem),
        name="outputs",
    )(
        pltpu.with_memory_space_constraint(gk, pltpu.VMEM),
        pltpu.with_memory_space_constraint(gi, pltpu.VMEM),
    )
    return jnp.transpose(gk, (2, 0, 1, 3))[None], gi.reshape(1, 1, CROPS, ROWS, COLS, C)


def solution(mesh):
    return jax.shard_map(
        shards,
        mesh=mesh,
        in_specs=(
            P("img", None, None, "slab", None),
            P("section", None, None, None, None),
            P("img", None, None, "slab", None),
        ),
        out_specs=(
            P("section", None, None, "slab", "img"),
            P("section", "img", None, None, "slab", None),
        ),
        check_vma=False,
    )
```

```python
import math

import jax
import jax.numpy as jnp
from jax import lax
from jax.experimental import pallas as pl
from jax.experimental.pallas import tpu as pltpu
from jax.sharding import PartitionSpec as P

MESH = pl.DeviceIdType.MESH
F32 = jnp.float32
BF16 = jnp.bfloat16

C = 320
SECTIONS = 4
IMAGES = 4
CROPS = 4
CHIPS = 8
SLABS = 16
ROWS = 8
COLS = 8
POS = ROWS * COLS
WIDE = POS + 16
DEEP = POS + 32
OUT_SHARE = C // IMAGES
IN_SHARE = C // SLABS
HALF = 256
PEERS = 8
DIRECT = (3, 5, 2, 6, 1, 7)
PAIR = 640


def iota(shape, dim):
    return lax.broadcasted_iota(jnp.int32, shape, dim)


def onehot(cond):
    return jnp.where(cond, 1.0, 0.0).astype(BF16)


def sigmoid(v):
    return 1.0 / (1.0 + jnp.exp(-v))


def row_shifts(x):
    count = x.shape[0]
    row = iota(x.shape, 0) % ROWS
    above = jnp.where(row == 0, 0.0, pltpu.roll(x, 1, 0))
    below = jnp.where(row == ROWS - 1, 0.0, pltpu.roll(x, count - 1, 0))
    return above, x, below


def conv(x, weights, part, count):
    shifted = row_shifts(x)
    total = None
    for a in range(3):
        for b in range(3):
            lhs = shifted[a][8 * b : 8 * b + count].astype(BF16)
            term = jnp.dot(lhs, weights[part, 3 * a + b], preferred_element_type=F32)
            total = term if total is None else total + term
    return total


def kernel(
    scaling,
    strips,
    kernels,
    cotangent,
    gk_out,
    gi_out,
    w,
    wt,
    sv,
    cv,
    fin,
    gin,
    fout,
    gout,
    hid,
    raw,
    fs,
    fg,
    gs,
    us,
    gg,
    cc,
    acc,
    pkl,
    pk,
    rz,
    far,
    pc,
    pct,
    sel,
    c6,
    local_sem,
    weight_sem,
    fr,
    fsend,
    br,
    bsend,
    edge_send,
    raw_recv,
    raw_send,
    fg_recv,
    fg_send,
    gg_recv,
    gg_send,
    up_send,
    gr_recv,
    gr_send,
    z_recv,
    far_recv,
    z_send,
    token,
):
    s = lax.axis_index("section")
    slab = lax.axis_index("slab")
    img = lax.axis_index("img")
    z = slab // 2
    core = slab % 2
    has_left = slab > 0
    has_right = slab < SLABS - 1

    loads = [
        pltpu.make_async_copy(strips, sv, local_sem.at[0]),
        pltpu.make_async_copy(cotangent, cv, local_sem.at[1]),
    ]
    for part in range(2):
        for tap in range(9):
            loads.append(
                pltpu.make_async_copy(
                    kernels.at[part, tap], w.at[part, tap], weight_sem
                )
            )
    for load in loads:
        load.start()

    @pl.when(slab == 0)
    def _():
        for buf in (fin, gin):
            buf[:, 0:16, :] = jnp.zeros((CROPS, 16, C), BF16)

    @pl.when(slab == SLABS - 1)
    def _():
        for buf in (fin, gin):
            buf[:, DEEP - 16 : DEEP, :] = jnp.zeros((CROPS, 16, C), BF16)

    barrier = pltpu.get_barrier_semaphore()

    def greet(where):
        pl.semaphore_signal(barrier, inc=1, device_id=where, device_id_type=MESH)

    def image_of(d):
        return (s, slab, (img + d) % IMAGES)

    partner = (s, 2 * z + 1 - core, img)

    def chip_of(d):
        return (s, 2 * ((z + d) % CHIPS) + core, img)

    greeted = jnp.int32(0)
    for ds in (-1, 0, 1):
        for dj in (-1, 0, 1):
            if ds == 0 and dj == 0:
                continue
            ok = (s + ds >= 0) & (s + ds < SECTIONS) & (slab + dj >= 0) & (slab + dj < SLABS)

            @pl.when(ok)
            def _():
                greet((s + ds, slab + dj, img))

            greeted = greeted + jnp.where(ok, 1, 0)
    for d in range(1, IMAGES):
        greet(image_of(d))
    greet(partner)
    for d in (1, CHIPS - 1):
        greet(chip_of(d))
    i, j = iota((POS, POS), 0), iota((POS, POS), 1)
    swap = onehot((i // 8 == j % 8) & (i % 8 == j // 8))
    def chosen(first, shape):
        i, j = iota(shape, 0) + first, iota(shape, 1)
        lane = j % 32
        side = (j // HALF + core) % 2
        return (lane < IN_SHARE) & (i == IN_SHARE * (2 * ((j % HALF) // 32) + side) + lane)

    pc[...] = onehot(chosen(0, (256, 2 * HALF)))
    tail_row = iota((128, 2 * HALF), 0)
    pct[0] = onehot(chosen(256, (128, 2 * HALF)) & (tail_row < 64))
    pct[1] = onehot(chosen(192, (128, 2 * HALF)) & (tail_row >= 64))
    i, j = iota((C, 512), 0), iota((C, 512), 1)
    lane = j % 128
    owner = (j // 128 + img) % IMAGES
    sel[...] = onehot((lane < OUT_SHARE) & (i == OUT_SHARE * owner + lane))
    i, j = iota((768, 512), 0), iota((768, 512), 1)
    lane = i % 32
    c6[...] = onehot(
        (lane < IN_SHARE)
        & ((i % 128) // 32 == j // 128)
        & (j % 128 == IN_SHARE * (i // 128) + lane)
    )

    acc[...] = jnp.zeros_like(acc)
    pl.semaphore_wait(barrier, greeted + IMAGES + 2)

    def permuted(x, matrix):
        return jnp.dot(x, matrix, preferred_element_type=F32).astype(BF16)

    def spread(src, dst, send, recv, k, ds, center):
        base = 16 if src is dst else 0

        @pl.when(has_right)
        def _():
            pltpu.make_async_remote_copy(
                src_ref=src.at[k, pl.ds(base + POS - 16, 16)],
                dst_ref=dst.at[k, pl.ds(0, 16)],
                send_sem=send.at[2],
                recv_sem=recv.at[k],
                device_id=(s + ds, slab + 1, img),
                device_id_type=MESH,
            ).start()

        @pl.when(has_left)
        def _():
            pltpu.make_async_remote_copy(
                src_ref=src.at[k, pl.ds(base, 16)],
                dst_ref=dst.at[k, pl.ds(DEEP - 16, 16)],
                send_sem=send.at[0],
                recv_sem=recv.at[k],
                device_id=(s + ds, slab - 1, img),
                device_id_type=MESH,
            ).start()

        if center:
            pltpu.make_async_remote_copy(
                src_ref=src.at[k],
                dst_ref=dst.at[k, pl.ds(16, POS)],
                send_sem=send.at[1],
                recv_sem=recv.at[k],
                device_id=(s + ds, slab, img),
                device_id_type=MESH,
            ).start()

    def waited(ref, sem):
        pltpu.make_async_copy(ref, ref, sem).wait()

    inner = has_left & has_right

    def arrive(dst, recv, k, center):
        other = jnp.logical_not(center)
        for case, rows in (
            (center & inner, DEEP),
            (center & jnp.logical_not(inner), DEEP - 16),
            (other & inner, 32),
            (other & jnp.logical_not(inner), 16),
        ):

            @pl.when(case)
            def _():
                waited(dst.at[k, pl.ds(0, rows)], recv.at[k])

    def sent(src, send, center):
        if center:
            waited(src, send.at[1])

        @pl.when(has_right)
        def _():
            waited(src.at[:, pl.ds(0, 16)], send.at[2])

        @pl.when(has_left)
        def _():
            waited(src.at[:, pl.ds(0, 16)], send.at[0])

    loads[0].wait()
    loads[1].wait()

    def share_grad(a, k, chunks):
        gg[a, k, IMAGES - 1] = chunks[:, :128]
        for d in range(1, IMAGES):
            gs[a, k, d - 1] = chunks[:, 128 * d : 128 * (d + 1)]
            pltpu.make_async_remote_copy(
                src_ref=gs.at[a, k, d - 1],
                dst_ref=gg.at[a, k, d - 1],
                send_sem=gg_send.at[a],
                recv_sem=gg_recv.at[a, k],
                device_id=image_of(d),
                device_id_type=MESH,
            ).start()

    @pl.when(s == 0)
    def _():
        def step(k, carry):
            fin[k, 16 : 16 + POS, :] = permuted(swap, sv[k])
            spread(fin, fin, edge_send, fr, k, 0, False)
            return carry

        lax.fori_loop(0, CROPS, step, 0)

    @pl.when(s == SECTIONS - 1)
    def _():
        def step(k, carry):
            center = permuted(swap, cv[k])
            gin[k, 16 : 16 + POS, :] = center
            spread(gin, gin, edge_send, br, k, 0, False)
            share_grad(1, k, permuted(center, sel[...]))
            return carry

        lax.fori_loop(0, CROPS, step, 0)

    waited(w, weight_sem)

    def transpose_weights():
        def step(n, carry):
            part, tap = n // 9, n % 9
            wt[part, 8 - tap] = w[part, tap].T
            return carry

        lax.fori_loop(0, 18, step, 0)

    pl.when(s > 0)(transpose_weights)

    row = iota((WIDE, C), 0)
    inside = jnp.logical_not(
        ((row < 8) & (slab == 0)) | ((row >= WIDE - 8) & (slab == SLABS - 1))
    )

    last = CROPS - 1

    def share_fields(k, wide, active):
        mine = raw.at[k, IMAGES - 1]
        mine[:, 0:256] = wide[:, 0:256].astype(BF16)
        mine[:, 256:512] = active[:, 0:256]
        tails = jnp.concatenate([wide[:, 256:C], active[:, 256:C].astype(F32)], axis=1)
        mine[:, 512:PAIR] = tails.astype(BF16)
        for d in range(1, IMAGES):
            pltpu.make_async_remote_copy(
                src_ref=mine,
                dst_ref=raw.at[k, d - 1],
                send_sem=raw_send,
                recv_sem=raw_recv.at[k],
                device_id=image_of(d),
                device_id_type=MESH,
            ).start()

    def relay_field(k):
        waited(raw.at[k, pl.ds(0, IMAGES - 1)], raw_recv.at[k])
        for a in range(2):
            for n in range(IMAGES):
                both = (
                    jnp.dot(raw[k, n, :, 256 * a : 256 * (a + 1)], pc[...], preferred_element_type=F32)
                    + jnp.dot(raw[k, n, :, 512:PAIR], pct[a], preferred_element_type=F32)
                ).astype(BF16)
                fg[a, k, n] = both[:, :HALF]
                fs[a, k, n] = both[:, HALF:]
            pltpu.make_async_remote_copy(
                src_ref=fs.at[a, k],
                dst_ref=fg.at[a, k, pl.ds(IMAGES, IMAGES)],
                send_sem=fg_send,
                recv_sem=fg_recv.at[a, k],
                device_id=partner,
                device_id_type=MESH,
            ).start()

    def relay_grad(a, k, slots=IMAGES - 1):
        waited(gg.at[a, k, pl.ds(0, slots)], gg_recv.at[a, k])
        pltpu.make_async_remote_copy(
            src_ref=gg.at[a, k, pl.ds(0, IMAGES)],
            dst_ref=gg.at[a, k, pl.ds(IMAGES, IMAGES)],
            send_sem=gr_send,
            recv_sem=gr_recv.at[a, k],
            device_id=partner,
            device_id_type=MESH,
        ).start()

    def forward(k):
        arrive(fin, fr, k, s > 0)
        x = fin[k].astype(F32)
        hidden = conv(x, w, 0, WIDE)
        hid[k] = hidden
        active = jnp.where(inside, hidden * sigmoid(hidden), 0.0).astype(BF16)

        @pl.when(s < SECTIONS - 1)
        def _():
            result = x[16 : 16 + POS] + conv(active.astype(F32), w, 1, POS)
            fout[k] = result.astype(BF16)
            spread(fout, fin, fsend, fr, k, 1, True)

        share_fields(k, x[8 : 8 + WIDE], active)

        @pl.when((s == 0) & (k == last))
        def _():
            transpose_weights()

    def backward(k):
        arrive(gin, br, k, s < SECTIONS - 1)
        g = gin[k].astype(F32)
        center = g[16 : 16 + POS]
        shared = ((s == 0) & (k == last)) | (s == SECTIONS - 1)
        grad_active = conv(g, wt, 1, WIDE)
        hidden = hid[k]
        q = sigmoid(hidden)
        slope = q * (1.0 + hidden * (1.0 - q))
        grad_hidden = jnp.where(inside, grad_active * slope, 0.0).astype(BF16)
        wide = grad_hidden.astype(F32)
        grad_in = (center + conv(wide, wt, 0, POS)).astype(BF16)
        gout[k] = grad_in

        @pl.when(s > 0)
        def _():
            spread(gout, gin, bsend, br, k, -1, True)

        @pl.when((s == 1) & (k == last))
        def _():
            above = permuted(grad_in, sel[...])
            for d in range(IMAGES):
                us[d] = above[:, 128 * d : 128 * (d + 1)]
                pltpu.make_async_remote_copy(
                    src_ref=us.at[d],
                    dst_ref=gg.at[1, k, (d + IMAGES - 1) % IMAGES],
                    send_sem=up_send,
                    recv_sem=gg_recv.at[1, k],
                    device_id=(s - 1, slab, (img + d) % IMAGES),
                    device_id_type=MESH,
                ).start()

        gi_out[k] = permuted(swap, grad_in)
        lower = wide[8 : 8 + POS].astype(BF16)
        chunks = permuted(jnp.concatenate([lower, center.astype(BF16)], axis=0), sel[...])
        share_grad(0, k, chunks[:POS])

        @pl.when(jnp.logical_not(shared))
        def _():
            share_grad(1, k, chunks[POS:])

        @pl.when((s <= 1) & (k >= 2))
        def _():
            relay_grad(1, k - 2)
            relay_grad(0, k - 2)

    def unfold(k):
        for a in range(2):
            waited(fg.at[a, k, pl.ds(IMAGES, IMAGES)], fg_recv.at[a, k])

            def source(m, carry):
                shifted = row_shifts(fg[a, k, m].astype(F32))
                for d in range(3):
                    for b in range(3):
                        cc[a, k, 3 * d + b, pl.ds(pl.multiple_of(m * POS, POS), POS), :] = shifted[d][
                            8 * b : 8 * b + POS
                        ].astype(BF16)
                return carry

            lax.fori_loop(0, PEERS, source, 0)

    def contract(a, k):
        waited(gg.at[a, k, pl.ds(IMAGES, IMAGES)], gr_recv.at[a, k])
        grads = gg[a, k].reshape(PEERS * POS, 128).T[:OUT_SHARE]
        for t in range(9):
            acc[a, t] += jnp.dot(grads, cc[a, k, t], preferred_element_type=F32)

    ahead_count = jnp.where(s == 0, CROPS + 1, jnp.where(s == 1, CROPS - 1, 0))

    def unfold_step(n, early):
        late = jnp.logical_not(early)

        @pl.when(late & (n > 1))
        def _():
            def each(a, carry):
                contract(a, n - 2)
                return carry

            lax.fori_loop(0, 2, each, 0)

        todo = early | (n >= ahead_count)

        @pl.when(todo & (n > 0))
        def _():
            unfold(n - 1)

        @pl.when(late & (n > jnp.where(s == 1, 2, 0)))
        def _():
            relay_grad(1, n - 1)
            relay_grad(0, n - 1)

        @pl.when(todo & (n < CROPS))
        def _():
            relay_field(n)

    at_end = s == SECTIONS - 1

    def step(i, carry):
        turn = i - jnp.where(s == 0, CROPS, 2 * CROPS + ahead_count)

        @pl.when((turn > 0) & (turn <= 3))
        def _():
            pl.semaphore_wait(token.at[turn - 1], 2)

        @pl.when((turn >= 0) & (turn < 3))
        def _():
            for d in (1, CHIPS - 1):
                pl.semaphore_signal(
                    token.at[turn], inc=1, device_id=chip_of(d), device_id_type=MESH
                )

        back_from = CROPS + ahead_count
        is_forward = jnp.where(at_end, (i < 2 * CROPS) & (i % 2 == 0), i < CROPS)
        is_backward = jnp.where(
            at_end, (i < 2 * CROPS) & (i % 2 == 1), (i >= back_from) & (i < back_from + CROPS)
        )

        @pl.when(is_forward)
        def _():
            forward(jnp.where(at_end, i // 2, i))

        @pl.when(is_backward)
        def _():
            backward(jnp.where(at_end, i // 2, i - back_from))

        @pl.when(jnp.logical_not(is_forward | is_backward))
        def _():
            early = i < back_from
            unfold_step(jnp.where(early, i - CROPS, i - back_from - CROPS), early)

        return carry

    lax.fori_loop(0, 3 * CROPS + 1 + jnp.where(s == 1, ahead_count, 0), step, 0)

    def send_block(block, t, d, dst, recv):
        pltpu.make_async_remote_copy(
            src_ref=pk.at[t, block],
            dst_ref=dst,
            send_sem=z_send,
            recv_sem=recv,
            device_id=chip_of(d),
            device_id_type=MESH,
        ).start()

    def pack(t):
        for p in range(6):
            a, tap = divmod(6 * t + p, 9)
            block = acc[a, tap].astype(BF16)
            for half in range(2):
                pkl[t, half, :, 128 * p : 128 * (p + 1)] = block[:, 128 * half : 128 * (half + 1)]
        packed = permuted(pkl[t].reshape(2 * OUT_SHARE, 768), c6[...]).reshape(2, OUT_SHARE, 512)
        for half in range(2):
            for q in range(4):
                pk[t, 4 * half + q] = packed[half, :, 128 * q : 128 * (q + 1)]
        near, held = (1, 3) if t % 2 == 0 else (7, 5)
        send_block((z + 4) % CHIPS, t, near, far.at[t], far_recv.at[t])
        for slot, d in enumerate(DIRECT):
            if d != held:
                send_block((z + d) % CHIPS, t, d, rz.at[t, slot], z_recv.at[t])

    def merge(t):
        held = 3 if t % 2 == 0 else 5
        waited(far.at[t], far_recv.at[t])
        mine = pk.at[t, (z + held) % CHIPS]
        mine[...] = (mine[...].astype(F32) + far[t].astype(F32)).astype(BF16)
        send_block((z + held) % CHIPS, t, held, rz.at[t, DIRECT.index(held)], z_recv.at[t])

    def tail(i, carry):
        first = s == 0

        @pl.when(first & (i == 2))
        def _():
            relay_grad(1, 2)
            relay_grad(0, 2)

        @pl.when(first & (i == 4))
        def _():
            relay_grad(1, last, IMAGES)

        @pl.when(first & (i == 6))
        def _():
            relay_grad(0, last)

        upper = ((i < 4) & (i % 2 == 0)) | (i == 4) | (i == 5)
        crop = jnp.where(i < 4, i // 2, jnp.where(i % 2 == 0, 2, last))

        @pl.when(first | (i != 6))
        def _():
            contract(jnp.where(upper, 1, 0), crop)

        @pl.when(i == 5)
        def _():
            pack(2)

        return carry

    lax.fori_loop(jnp.where(s == 0, 0, 5), 2 * CROPS, tail, 0)
    pack(1)
    pack(0)
    merge(2)
    merge(1)
    merge(0)

    for t in (2, 1, 0):
        waited(rz.at[t], z_recv.at[t])
        total = pk[t, z].astype(F32)
        for slot in range(len(DIRECT)):
            total = total + rz[t, slot].astype(F32)
        gk_out[t] = (total * scaling).T

    waited(pk.at[:, pl.ds(0, CHIPS - 1)], z_send)
    waited(raw.at[:, pl.ds(0, IMAGES - 1)], raw_send)
    waited(fs, fg_send)
    waited(gs.at[0], gg_send.at[0])

    @pl.when(s == 0)
    def _():
        waited(gs.at[1, pl.ds(0, last)], gg_send.at[1])

    @pl.when(s > 0)
    def _():
        waited(gs.at[1], gg_send.at[1])

    @pl.when(s == 1)
    def _():
        waited(us, up_send)

    waited(gg.at[:, :, pl.ds(0, IMAGES)], gr_send)

    @pl.when(s == 0)
    def _():
        sent(fin, edge_send, False)

    @pl.when(s == SECTIONS - 1)
    def _():
        sent(gin, edge_send, False)

    @pl.when(s < SECTIONS - 1)
    def _():
        sent(fout, fsend, True)

    @pl.when(s > 0)
    def _():
        sent(gout, bsend, True)


def placed(gk, gi, gk_out, gi_out):
    gi_out[...] = gi[...]
    for n in range(18):
        a, tap = divmod(n, 9)
        t, p = divmod(n, 6)
        gk_out[tap, :, a, :] = gk[t, IN_SHARE * p : IN_SHARE * (p + 1), :]


def shards(strips, kernels, cotangent):
    scaling = 1.0 / math.sqrt(IMAGES * CROPS * ROWS * COLS * SLABS)
    dma = pltpu.SemaphoreType.DMA
    vmem = pl.BlockSpec(memory_space=pltpu.VMEM)
    hbm = pl.BlockSpec(memory_space=pl.ANY)
    gk, gi = pl.pallas_call(
        lambda *refs: kernel(scaling, *refs),
        out_shape=(
            pltpu.VMEM((3, 128, OUT_SHARE), F32),
            pltpu.VMEM((CROPS, POS, C), BF16),
        ),
        in_specs=[hbm, hbm, hbm],
        out_specs=(vmem, vmem),
        scratch_shapes=[
            pltpu.VMEM((2, 9, C, C), BF16),
            pltpu.VMEM((2, 9, C, C), BF16),
            pltpu.VMEM((CROPS, POS, C), BF16),
            pltpu.VMEM((CROPS, POS, C), BF16),
            pltpu.VMEM((CROPS, DEEP, C), BF16),
            pltpu.VMEM((CROPS, DEEP, C), BF16),
            pltpu.VMEM((CROPS, POS, C), BF16),
            pltpu.VMEM((CROPS, POS, C), BF16),
            pltpu.VMEM((CROPS, WIDE, C), F32),
            pltpu.VMEM((CROPS, IMAGES, WIDE, PAIR), BF16),
            pltpu.VMEM((2, CROPS, IMAGES, WIDE, HALF), BF16),
            pltpu.VMEM((2, CROPS, PEERS, WIDE, HALF), BF16),
            pltpu.VMEM((2, CROPS, IMAGES - 1, POS, 128), BF16),
            pltpu.VMEM((IMAGES, POS, 128), BF16),
            pltpu.VMEM((2, CROPS, PEERS, POS, 128), BF16),
            pltpu.VMEM((2, CROPS, 9, PEERS * POS, HALF), BF16),
            pltpu.VMEM((2, 9, OUT_SHARE, HALF), F32),
            pltpu.VMEM((3, 2, OUT_SHARE, 768), BF16),
            pltpu.VMEM((3, CHIPS, OUT_SHARE, 128), BF16),
            pltpu.VMEM((3, len(DIRECT), OUT_SHARE, 128), BF16),
            pltpu.VMEM((3, OUT_SHARE, 128), BF16),
            pltpu.VMEM((256, 2 * HALF), BF16),
            pltpu.VMEM((2, 128, 2 * HALF), BF16),
            pltpu.VMEM((C, 512), BF16),
            pltpu.VMEM((768, 512), BF16),
            dma((2,)),
            dma,
            dma((CROPS,)),
            dma((3,)),
            dma((CROPS,)),
            dma((3,)),
            dma((3,)),
            dma((CROPS,)),
            dma,
            dma((2, CROPS)),
            dma,
            dma((2, CROPS)),
            dma((2,)),
            dma,
            dma((2, CROPS)),
            dma,
            dma((3,)),
            dma((3,)),
            dma,
            pltpu.SemaphoreType.REGULAR((3,)),
        ],
        compiler_params=pltpu.CompilerParams(
            collective_id=0, has_side_effects=True, vmem_limit_bytes=60 * 1024 * 1024
        ),
        name="residual_step",
    )(
        strips.reshape(CROPS, POS, C),
        kernels.reshape(2, 9, C, C),
        cotangent.reshape(CROPS, POS, C),
    )
    gk, gi = pl.pallas_call(
        placed,
        out_shape=(
            jax.ShapeDtypeStruct((9, IN_SHARE, 2, OUT_SHARE), F32),
            jax.ShapeDtypeStruct((CROPS, POS, C), BF16),
        ),
        in_specs=[vmem, vmem],
        out_specs=(vmem, vmem),
        name="outputs",
    )(
        pltpu.with_memory_space_constraint(gk, pltpu.VMEM),
        pltpu.with_memory_space_constraint(gi, pltpu.VMEM),
    )
    return jnp.transpose(gk, (2, 0, 1, 3))[None], gi.reshape(1, 1, CROPS, ROWS, COLS, C)


def solution(mesh):
    return jax.shard_map(
        shards,
        mesh=mesh,
        in_specs=(
            P("img", None, None, "slab", None),
            P("section", None, None, None, None),
            P("img", None, None, "slab", None),
        ),
        out_specs=(
            P("section", None, None, "slab", "img"),
            P("section", "img", None, None, "slab", None),
        ),
        check_vma=False,
    )
```

```python
import math

import jax
import jax.numpy as jnp
from jax import lax
from jax.experimental import pallas as pl
from jax.experimental.pallas import tpu as pltpu
from jax.sharding import PartitionSpec as P

MESH = pl.DeviceIdType.MESH
F32 = jnp.float32
BF16 = jnp.bfloat16

C = 320
SECTIONS = 4
IMAGES = 4
CROPS = 4
CHIPS = 8
SLABS = 16
ROWS = 8
COLS = 8
POS = ROWS * COLS
WIDE = POS + 16
DEEP = POS + 32
OUT_SHARE = C // IMAGES
IN_SHARE = C // SLABS
HALF = 256
PEERS = 8
DIRECT = (3, 5, 2, 6, 1, 7)
PAIR = 640


def iota(shape, dim):
    return lax.broadcasted_iota(jnp.int32, shape, dim)


def onehot(cond):
    return jnp.where(cond, 1.0, 0.0).astype(BF16)


def sigmoid(v):
    return 1.0 / (1.0 + jnp.exp(-v))


def row_shifts(x):
    count = x.shape[0]
    row = iota(x.shape, 0) % ROWS
    above = jnp.where(row == 0, 0.0, pltpu.roll(x, 1, 0))
    below = jnp.where(row == ROWS - 1, 0.0, pltpu.roll(x, count - 1, 0))
    return above, x, below


def conv(x, weights, part, count):
    shifted = row_shifts(x)
    total = None
    for a in range(3):
        for b in range(3):
            lhs = shifted[a][8 * b : 8 * b + count].astype(BF16)
            term = jnp.dot(lhs, weights[part, 3 * a + b], preferred_element_type=F32)
            total = term if total is None else total + term
    return total


def kernel(
    scaling,
    strips,
    kernels,
    cotangent,
    gk_out,
    gi_out,
    w,
    wt,
    sv,
    cv,
    fin,
    gin,
    fout,
    gout,
    hid,
    raw,
    fs,
    fg,
    gs,
    us,
    gg,
    cc,
    acc,
    pkl,
    pk,
    rz,
    far,
    pc,
    pct,
    sel,
    c6,
    local_sem,
    weight_sem,
    fr,
    fsend,
    br,
    bsend,
    edge_send,
    raw_recv,
    raw_send,
    fg_recv,
    fg_send,
    gg_recv,
    gg_send,
    up_send,
    gr_recv,
    gr_send,
    z_recv,
    far_recv,
    z_send,
    token,
):
    s = lax.axis_index("section")
    slab = lax.axis_index("slab")
    img = lax.axis_index("img")
    z = slab // 2
    core = slab % 2
    has_left = slab > 0
    has_right = slab < SLABS - 1

    loads = [
        pltpu.make_async_copy(strips, sv, local_sem.at[0]),
        pltpu.make_async_copy(cotangent, cv, local_sem.at[1]),
    ]
    for part in range(2):
        for tap in range(9):
            loads.append(
                pltpu.make_async_copy(
                    kernels.at[part, tap], w.at[part, tap], weight_sem
                )
            )
    for load in loads:
        load.start()

    @pl.when(slab == 0)
    def _():
        for buf in (fin, gin):
            buf[:, 0:16, :] = jnp.zeros((CROPS, 16, C), BF16)

    @pl.when(slab == SLABS - 1)
    def _():
        for buf in (fin, gin):
            buf[:, DEEP - 16 : DEEP, :] = jnp.zeros((CROPS, 16, C), BF16)

    barrier = pltpu.get_barrier_semaphore()

    def greet(where):
        pl.semaphore_signal(barrier, inc=1, device_id=where, device_id_type=MESH)

    def image_of(d):
        return (s, slab, (img + d) % IMAGES)

    partner = (s, 2 * z + 1 - core, img)

    def chip_of(d):
        return (s, 2 * ((z + d) % CHIPS) + core, img)

    greeted = jnp.int32(0)
    for ds in (-1, 0, 1):
        for dj in (-1, 0, 1):
            if ds == 0 and dj == 0:
                continue
            ok = (s + ds >= 0) & (s + ds < SECTIONS) & (slab + dj >= 0) & (slab + dj < SLABS)

            @pl.when(ok)
            def _():
                greet((s + ds, slab + dj, img))

            greeted = greeted + jnp.where(ok, 1, 0)
    for d in range(1, IMAGES):
        greet(image_of(d))
    greet(partner)
    for d in (1, CHIPS - 1):
        greet(chip_of(d))
    i, j = iota((POS, POS), 0), iota((POS, POS), 1)
    swap = onehot((i // 8 == j % 8) & (i % 8 == j // 8))
    def chosen(first, shape):
        i, j = iota(shape, 0) + first, iota(shape, 1)
        lane = j % 32
        side = (j // HALF + core) % 2
        return (lane < IN_SHARE) & (i == IN_SHARE * (2 * ((j % HALF) // 32) + side) + lane)

    pc[...] = onehot(chosen(0, (256, 2 * HALF)))
    tail_row = iota((128, 2 * HALF), 0)
    pct[0] = onehot(chosen(256, (128, 2 * HALF)) & (tail_row < 64))
    pct[1] = onehot(chosen(192, (128, 2 * HALF)) & (tail_row >= 64))
    i, j = iota((C, 512), 0), iota((C, 512), 1)
    lane = j % 128
    owner = (j // 128 + img) % IMAGES
    sel[...] = onehot((lane < OUT_SHARE) & (i == OUT_SHARE * owner + lane))
    i, j = iota((768, 512), 0), iota((768, 512), 1)
    lane = i % 32
    c6[...] = onehot(
        (lane < IN_SHARE)
        & ((i % 128) // 32 == j // 128)
        & (j % 128 == IN_SHARE * (i // 128) + lane)
    )

    acc[...] = jnp.zeros_like(acc)
    pl.semaphore_wait(barrier, greeted + IMAGES + 2)

    def permuted(x, matrix):
        return jnp.dot(x, matrix, preferred_element_type=F32).astype(BF16)

    def spread(src, dst, send, recv, k, ds, center):
        base = 16 if src is dst else 0

        @pl.when(has_right)
        def _():
            pltpu.make_async_remote_copy(
                src_ref=src.at[k, pl.ds(base + POS - 16, 16)],
                dst_ref=dst.at[k, pl.ds(0, 16)],
                send_sem=send.at[2],
                recv_sem=recv.at[k],
                device_id=(s + ds, slab + 1, img),
                device_id_type=MESH,
            ).start()

        @pl.when(has_left)
        def _():
            pltpu.make_async_remote_copy(
                src_ref=src.at[k, pl.ds(base, 16)],
                dst_ref=dst.at[k, pl.ds(DEEP - 16, 16)],
                send_sem=send.at[0],
                recv_sem=recv.at[k],
                device_id=(s + ds, slab - 1, img),
                device_id_type=MESH,
            ).start()

        if center:
            pltpu.make_async_remote_copy(
                src_ref=src.at[k],
                dst_ref=dst.at[k, pl.ds(16, POS)],
                send_sem=send.at[1],
                recv_sem=recv.at[k],
                device_id=(s + ds, slab, img),
                device_id_type=MESH,
            ).start()

    def waited(ref, sem):
        pltpu.make_async_copy(ref, ref, sem).wait()

    inner = has_left & has_right

    def arrive(dst, recv, k, center):
        other = jnp.logical_not(center)
        for case, rows in (
            (center & inner, DEEP),
            (center & jnp.logical_not(inner), DEEP - 16),
            (other & inner, 32),
            (other & jnp.logical_not(inner), 16),
        ):

            @pl.when(case)
            def _():
                waited(dst.at[k, pl.ds(0, rows)], recv.at[k])

    def sent(src, send, center):
        if center:
            waited(src, send.at[1])

        @pl.when(has_right)
        def _():
            waited(src.at[:, pl.ds(0, 16)], send.at[2])

        @pl.when(has_left)
        def _():
            waited(src.at[:, pl.ds(0, 16)], send.at[0])

    loads[0].wait()
    loads[1].wait()

    def share_grad(a, k, chunks):
        gg[a, k, IMAGES - 1] = chunks[:, :128]
        for d in range(1, IMAGES):
            gs[a, k, d - 1] = chunks[:, 128 * d : 128 * (d + 1)]
            pltpu.make_async_remote_copy(
                src_ref=gs.at[a, k, d - 1],
                dst_ref=gg.at[a, k, d - 1],
                send_sem=gg_send.at[a],
                recv_sem=gg_recv.at[a, k],
                device_id=image_of(d),
                device_id_type=MESH,
            ).start()

    @pl.when(s == 0)
    def _():
        def step(k, carry):
            fin[k, 16 : 16 + POS, :] = permuted(swap, sv[k])
            spread(fin, fin, edge_send, fr, k, 0, False)
            return carry

        lax.fori_loop(0, CROPS, step, 0)

    @pl.when(s == SECTIONS - 1)
    def _():
        def step(k, carry):
            center = permuted(swap, cv[k])
            gin[k, 16 : 16 + POS, :] = center
            spread(gin, gin, edge_send, br, k, 0, False)
            share_grad(1, k, permuted(center, sel[...]))
            return carry

        lax.fori_loop(0, CROPS, step, 0)

    waited(w, weight_sem)

    def transpose_weights():
        def step(n, carry):
            part, tap = n // 9, n % 9
            wt[part, 8 - tap] = w[part, tap].T
            return carry

        lax.fori_loop(0, 18, step, 0)

    pl.when(s > 0)(transpose_weights)

    row = iota((WIDE, C), 0)
    inside = jnp.logical_not(
        ((row < 8) & (slab == 0)) | ((row >= WIDE - 8) & (slab == SLABS - 1))
    )

    last = CROPS - 1

    def share_fields(k, wide, active):
        mine = raw.at[k, IMAGES - 1]
        mine[:, 0:256] = wide[:, 0:256].astype(BF16)
        mine[:, 256:512] = active[:, 0:256]
        tails = jnp.concatenate([wide[:, 256:C], active[:, 256:C].astype(F32)], axis=1)
        mine[:, 512:PAIR] = tails.astype(BF16)
        for d in range(1, IMAGES):
            pltpu.make_async_remote_copy(
                src_ref=mine,
                dst_ref=raw.at[k, d - 1],
                send_sem=raw_send,
                recv_sem=raw_recv.at[k],
                device_id=image_of(d),
                device_id_type=MESH,
            ).start()

    def relay_field(k):
        waited(raw.at[k, pl.ds(0, IMAGES - 1)], raw_recv.at[k])
        for a in range(2):
            for n in range(IMAGES):
                both = (
                    jnp.dot(raw[k, n, :, 256 * a : 256 * (a + 1)], pc[...], preferred_element_type=F32)
                    + jnp.dot(raw[k, n, :, 512:PAIR], pct[a], preferred_element_type=F32)
                ).astype(BF16)
                fg[a, k, n] = both[:, :HALF]
                fs[a, k, n] = both[:, HALF:]
            pltpu.make_async_remote_copy(
                src_ref=fs.at[a, k],
                dst_ref=fg.at[a, k, pl.ds(IMAGES, IMAGES)],
                send_sem=fg_send,
                recv_sem=fg_recv.at[a, k],
                device_id=partner,
                device_id_type=MESH,
            ).start()

    def relay_grad(a, k, slots=IMAGES - 1):
        waited(gg.at[a, k, pl.ds(0, slots)], gg_recv.at[a, k])
        pltpu.make_async_remote_copy(
            src_ref=gg.at[a, k, pl.ds(0, IMAGES)],
            dst_ref=gg.at[a, k, pl.ds(IMAGES, IMAGES)],
            send_sem=gr_send,
            recv_sem=gr_recv.at[a, k],
            device_id=partner,
            device_id_type=MESH,
        ).start()

    def forward(k):
        arrive(fin, fr, k, s > 0)
        x = fin[k].astype(F32)
        hidden = conv(x, w, 0, WIDE)
        hid[k] = hidden
        active = jnp.where(inside, hidden * sigmoid(hidden), 0.0).astype(BF16)

        @pl.when(s < SECTIONS - 1)
        def _():
            result = x[16 : 16 + POS] + conv(active.astype(F32), w, 1, POS)
            fout[k] = result.astype(BF16)
            spread(fout, fin, fsend, fr, k, 1, True)

        share_fields(k, x[8 : 8 + WIDE], active)

        @pl.when((s == 0) & (k == last))
        def _():
            transpose_weights()

    def backward(k):
        arrive(gin, br, k, s < SECTIONS - 1)
        g = gin[k].astype(F32)
        center = g[16 : 16 + POS]
        shared = ((s == 0) & (k == last)) | (s == SECTIONS - 1)
        grad_active = conv(g, wt, 1, WIDE)
        hidden = hid[k]
        q = sigmoid(hidden)
        slope = q * (1.0 + hidden * (1.0 - q))
        grad_hidden = jnp.where(inside, grad_active * slope, 0.0).astype(BF16)
        wide = grad_hidden.astype(F32)
        grad_in = (center + conv(wide, wt, 0, POS)).astype(BF16)
        gout[k] = grad_in

        @pl.when(s > 0)
        def _():
            spread(gout, gin, bsend, br, k, -1, True)

        @pl.when((s == 1) & (k == last))
        def _():
            above = permuted(grad_in, sel[...])
            for d in range(IMAGES):
                us[d] = above[:, 128 * d : 128 * (d + 1)]
                pltpu.make_async_remote_copy(
                    src_ref=us.at[d],
                    dst_ref=gg.at[1, k, (d + IMAGES - 1) % IMAGES],
                    send_sem=up_send,
                    recv_sem=gg_recv.at[1, k],
                    device_id=(s - 1, slab, (img + d) % IMAGES),
                    device_id_type=MESH,
                ).start()

        gi_out[k] = permuted(swap, grad_in)
        lower = wide[8 : 8 + POS].astype(BF16)
        chunks = permuted(jnp.concatenate([lower, center.astype(BF16)], axis=0), sel[...])
        share_grad(0, k, chunks[:POS])

        @pl.when(jnp.logical_not(shared))
        def _():
            share_grad(1, k, chunks[POS:])

        @pl.when((s <= 1) & (k >= 2))
        def _():
            relay_grad(1, k - 2)
            relay_grad(0, k - 2)

    def unfold(k):
        for a in range(2):
            waited(fg.at[a, k, pl.ds(IMAGES, IMAGES)], fg_recv.at[a, k])

            def source(m, carry):
                shifted = row_shifts(fg[a, k, m].astype(F32))
                for d in range(3):
                    for b in range(3):
                        cc[a, k, 3 * d + b, pl.ds(pl.multiple_of(m * POS, POS), POS), :] = shifted[d][
                            8 * b : 8 * b + POS
                        ].astype(BF16)
                return carry

            lax.fori_loop(0, PEERS, source, 0)

    def contract(a, k):
        waited(gg.at[a, k, pl.ds(IMAGES, IMAGES)], gr_recv.at[a, k])
        grads = gg[a, k].reshape(PEERS * POS, 128).T[:OUT_SHARE]
        for t in range(9):
            acc[a, t] += jnp.dot(grads, cc[a, k, t], preferred_element_type=F32)

    ahead_count = jnp.where(s == 0, CROPS + 1, jnp.where(s == 1, CROPS - 1, 0))

    def unfold_step(n, early):
        late = jnp.logical_not(early)

        @pl.when(late & (n > 1))
        def _():
            def each(a, carry):
                contract(a, n - 2)
                return carry

            lax.fori_loop(0, 2, each, 0)

        todo = early | (n >= ahead_count)

        @pl.when(todo & (n > 0))
        def _():
            unfold(n - 1)

        @pl.when(late & (n > jnp.where(s == 1, 2, 0)))
        def _():
            relay_grad(1, n - 1)
            relay_grad(0, n - 1)

        @pl.when(todo & (n < CROPS))
        def _():
            relay_field(n)

    at_end = s == SECTIONS - 1

    def step(i, carry):
        def vouch(turn):
            for d in (1, CHIPS - 1):
                pl.semaphore_signal(
                    token.at[turn], inc=1, device_id=chip_of(d), device_id_type=MESH
                )

        @pl.when((s >= 2) & (i == 0))
        def _():
            for turn in range(3):
                vouch(turn)
                pl.semaphore_wait(token.at[turn], 2)

        turn = i - CROPS

        @pl.when((s < 2) & (turn > 0) & (turn <= 3))
        def _():
            pl.semaphore_wait(token.at[turn - 1], 2)

        @pl.when((s < 2) & (turn >= 0) & (turn < 3))
        def _():
            vouch(turn)

        back_from = CROPS + ahead_count
        is_forward = jnp.where(at_end, (i < 2 * CROPS) & (i % 2 == 0), i < CROPS)
        is_backward = jnp.where(
            at_end, (i < 2 * CROPS) & (i % 2 == 1), (i >= back_from) & (i < back_from + CROPS)
        )

        @pl.when(is_forward)
        def _():
            forward(jnp.where(at_end, i // 2, i))

        @pl.when(is_backward)
        def _():
            backward(jnp.where(at_end, i // 2, i - back_from))

        @pl.when(jnp.logical_not(is_forward | is_backward))
        def _():
            early = i < back_from
            unfold_step(jnp.where(early, i - CROPS, i - back_from - CROPS), early)

        return carry

    lax.fori_loop(0, 3 * CROPS + 1 + jnp.where(s == 1, ahead_count, 0), step, 0)

    def send_block(block, t, d, dst, recv):
        pltpu.make_async_remote_copy(
            src_ref=pk.at[t, block],
            dst_ref=dst,
            send_sem=z_send,
            recv_sem=recv,
            device_id=chip_of(d),
            device_id_type=MESH,
        ).start()

    def pack(t):
        for p in range(6):
            a, tap = divmod(6 * t + p, 9)
            block = acc[a, tap].astype(BF16)
            for half in range(2):
                pkl[t, half, :, 128 * p : 128 * (p + 1)] = block[:, 128 * half : 128 * (half + 1)]
        packed = permuted(pkl[t].reshape(2 * OUT_SHARE, 768), c6[...]).reshape(2, OUT_SHARE, 512)
        for half in range(2):
            for q in range(4):
                pk[t, 4 * half + q] = packed[half, :, 128 * q : 128 * (q + 1)]
        send_block((z + 4) % CHIPS, t, 1 if t % 2 == 0 else 7, far.at[t], far_recv.at[t])

    def direct(t):
        held = 3 if t % 2 == 0 else 5
        for slot, d in enumerate(DIRECT):
            if d != held:
                send_block((z + d) % CHIPS, t, d, rz.at[t, slot], z_recv.at[t])

    def merge(t):
        held = 3 if t % 2 == 0 else 5
        waited(far.at[t], far_recv.at[t])
        mine = pk.at[t, (z + held) % CHIPS]
        mine[...] = (mine[...].astype(F32) + far[t].astype(F32)).astype(BF16)
        send_block((z + held) % CHIPS, t, held, rz.at[t, DIRECT.index(held)], z_recv.at[t])

    def tail(i, carry):
        first = s == 0

        @pl.when(first & (i == 2))
        def _():
            relay_grad(1, 2)
            relay_grad(0, 2)

        @pl.when(first & (i == 4))
        def _():
            relay_grad(1, last, IMAGES)

        @pl.when(first & (i == 6))
        def _():
            relay_grad(0, last)

        upper = ((i < 4) & (i % 2 == 0)) | (i == 4) | (i == 5)
        crop = jnp.where(i < 4, i // 2, jnp.where(i % 2 == 0, 2, last))

        @pl.when(first | (i != 6))
        def _():
            contract(jnp.where(upper, 1, 0), crop)

        @pl.when(i == 5)
        def _():
            pack(2)
            direct(2)

        return carry

    lax.fori_loop(jnp.where(s == 0, 0, 5), 2 * CROPS, tail, 0)
    pack(1)
    pack(0)
    direct(1)
    direct(0)
    merge(2)
    merge(1)
    merge(0)

    for t in (2, 0, 1):
        waited(rz.at[t], z_recv.at[t])
        total = pk[t, z].astype(F32)
        for slot in range(len(DIRECT)):
            total = total + rz[t, slot].astype(F32)
        gk_out[t] = (total * scaling).T

    waited(pk.at[:, pl.ds(0, CHIPS - 1)], z_send)
    waited(raw.at[:, pl.ds(0, IMAGES - 1)], raw_send)
    waited(fs, fg_send)
    waited(gs.at[0], gg_send.at[0])

    @pl.when(s == 0)
    def _():
        waited(gs.at[1, pl.ds(0, last)], gg_send.at[1])

    @pl.when(s > 0)
    def _():
        waited(gs.at[1], gg_send.at[1])

    @pl.when(s == 1)
    def _():
        waited(us, up_send)

    waited(gg.at[:, :, pl.ds(0, IMAGES)], gr_send)

    @pl.when(s == 0)
    def _():
        sent(fin, edge_send, False)

    @pl.when(s == SECTIONS - 1)
    def _():
        sent(gin, edge_send, False)

    @pl.when(s < SECTIONS - 1)
    def _():
        sent(fout, fsend, True)

    @pl.when(s > 0)
    def _():
        sent(gout, bsend, True)


def placed(gk, gi, gk_out, gi_out):
    gi_out[...] = gi[...]
    for n in range(18):
        a, tap = divmod(n, 9)
        t, p = divmod(n, 6)
        gk_out[tap, :, a, :] = gk[t, IN_SHARE * p : IN_SHARE * (p + 1), :]


def shards(strips, kernels, cotangent):
    scaling = 1.0 / math.sqrt(IMAGES * CROPS * ROWS * COLS * SLABS)
    dma = pltpu.SemaphoreType.DMA
    vmem = pl.BlockSpec(memory_space=pltpu.VMEM)
    hbm = pl.BlockSpec(memory_space=pl.ANY)
    gk, gi = pl.pallas_call(
        lambda *refs: kernel(scaling, *refs),
        out_shape=(
            pltpu.VMEM((3, 128, OUT_SHARE), F32),
            pltpu.VMEM((CROPS, POS, C), BF16),
        ),
        in_specs=[hbm, hbm, hbm],
        out_specs=(vmem, vmem),
        scratch_shapes=[
            pltpu.VMEM((2, 9, C, C), BF16),
            pltpu.VMEM((2, 9, C, C), BF16),
            pltpu.VMEM((CROPS, POS, C), BF16),
            pltpu.VMEM((CROPS, POS, C), BF16),
            pltpu.VMEM((CROPS, DEEP, C), BF16),
            pltpu.VMEM((CROPS, DEEP, C), BF16),
            pltpu.VMEM((CROPS, POS, C), BF16),
            pltpu.VMEM((CROPS, POS, C), BF16),
            pltpu.VMEM((CROPS, WIDE, C), F32),
            pltpu.VMEM((CROPS, IMAGES, WIDE, PAIR), BF16),
            pltpu.VMEM((2, CROPS, IMAGES, WIDE, HALF), BF16),
            pltpu.VMEM((2, CROPS, PEERS, WIDE, HALF), BF16),
            pltpu.VMEM((2, CROPS, IMAGES - 1, POS, 128), BF16),
            pltpu.VMEM((IMAGES, POS, 128), BF16),
            pltpu.VMEM((2, CROPS, PEERS, POS, 128), BF16),
            pltpu.VMEM((2, CROPS, 9, PEERS * POS, HALF), BF16),
            pltpu.VMEM((2, 9, OUT_SHARE, HALF), F32),
            pltpu.VMEM((3, 2, OUT_SHARE, 768), BF16),
            pltpu.VMEM((3, CHIPS, OUT_SHARE, 128), BF16),
            pltpu.VMEM((3, len(DIRECT), OUT_SHARE, 128), BF16),
            pltpu.VMEM((3, OUT_SHARE, 128), BF16),
            pltpu.VMEM((256, 2 * HALF), BF16),
            pltpu.VMEM((2, 128, 2 * HALF), BF16),
            pltpu.VMEM((C, 512), BF16),
            pltpu.VMEM((768, 512), BF16),
            dma((2,)),
            dma,
            dma((CROPS,)),
            dma((3,)),
            dma((CROPS,)),
            dma((3,)),
            dma((3,)),
            dma((CROPS,)),
            dma,
            dma((2, CROPS)),
            dma,
            dma((2, CROPS)),
            dma((2,)),
            dma,
            dma((2, CROPS)),
            dma,
            dma((3,)),
            dma((3,)),
            dma,
            pltpu.SemaphoreType.REGULAR((3,)),
        ],
        compiler_params=pltpu.CompilerParams(
            collective_id=0, has_side_effects=True, vmem_limit_bytes=60 * 1024 * 1024
        ),
        name="residual_step",
    )(
        strips.reshape(CROPS, POS, C),
        kernels.reshape(2, 9, C, C),
        cotangent.reshape(CROPS, POS, C),
    )
    gk, gi = pl.pallas_call(
        placed,
        out_shape=(
            jax.ShapeDtypeStruct((9, IN_SHARE, 2, OUT_SHARE), F32),
            jax.ShapeDtypeStruct((CROPS, POS, C), BF16),
        ),
        in_specs=[vmem, vmem],
        out_specs=(vmem, vmem),
        name="outputs",
    )(
        pltpu.with_memory_space_constraint(gk, pltpu.VMEM),
        pltpu.with_memory_space_constraint(gi, pltpu.VMEM),
    )
    return jnp.transpose(gk, (2, 0, 1, 3))[None], gi.reshape(1, 1, CROPS, ROWS, COLS, C)


def solution(mesh):
    return jax.shard_map(
        shards,
        mesh=mesh,
        in_specs=(
            P("img", None, None, "slab", None),
            P("section", None, None, None, None),
            P("img", None, None, "slab", None),
        ),
        out_specs=(
            P("section", None, None, "slab", "img"),
            P("section", "img", None, None, "slab", None),
        ),
        check_vma=False,
    )
```

```python
import math

import jax
import jax.numpy as jnp
from jax import lax
from jax.experimental import pallas as pl
from jax.experimental.pallas import tpu as pltpu
from jax.sharding import PartitionSpec as P

MESH = pl.DeviceIdType.MESH
F32 = jnp.float32
BF16 = jnp.bfloat16

C = 320
SECTIONS = 4
IMAGES = 4
CROPS = 4
CHIPS = 8
SLABS = 16
ROWS = 8
COLS = 8
POS = ROWS * COLS
WIDE = POS + 16
DEEP = POS + 32
OUT_SHARE = C // IMAGES
IN_SHARE = C // SLABS
HALF = 256
PEERS = 8
DIRECT = (3, 5, 2, 6, 1, 7)
PAIR = 640


def iota(shape, dim):
    return lax.broadcasted_iota(jnp.int32, shape, dim)


def onehot(cond):
    return jnp.where(cond, 1.0, 0.0).astype(BF16)


def sigmoid(v):
    return 1.0 / (1.0 + jnp.exp(-v))


def row_shifts(x):
    count = x.shape[0]
    row = iota(x.shape, 0) % ROWS
    above = jnp.where(row == 0, 0.0, pltpu.roll(x, 1, 0))
    below = jnp.where(row == ROWS - 1, 0.0, pltpu.roll(x, count - 1, 0))
    return above, x, below


def conv(x, weights, part, count):
    shifted = row_shifts(x)
    total = None
    for a in range(3):
        for b in range(3):
            lhs = shifted[a][8 * b : 8 * b + count].astype(BF16)
            term = jnp.dot(lhs, weights[part, 3 * a + b], preferred_element_type=F32)
            total = term if total is None else total + term
    return total


def kernel(
    scaling,
    strips,
    kernels,
    cotangent,
    gk_out,
    gi_out,
    w,
    wt,
    sv,
    cv,
    fin,
    gin,
    fout,
    gout,
    hid,
    raw,
    fs,
    fg,
    gs,
    us,
    gg,
    cc,
    acc,
    pkl,
    pk,
    rz,
    far,
    pc,
    pct,
    sel,
    c6,
    local_sem,
    weight_sem,
    fr,
    fsend,
    br,
    bsend,
    edge_send,
    raw_recv,
    raw_send,
    fg_recv,
    fg_send,
    gg_recv,
    gg_send,
    up_send,
    gr_recv,
    gr_send,
    z_recv,
    far_recv,
    z_send,
    token,
):
    s = lax.axis_index("section")
    slab = lax.axis_index("slab")
    img = lax.axis_index("img")
    z = slab // 2
    core = slab % 2
    has_left = slab > 0
    has_right = slab < SLABS - 1

    loads = [
        pltpu.make_async_copy(strips, sv, local_sem.at[0]),
        pltpu.make_async_copy(cotangent, cv, local_sem.at[1]),
    ]
    for part in range(2):
        for tap in range(9):
            loads.append(
                pltpu.make_async_copy(
                    kernels.at[part, tap], w.at[part, tap], weight_sem
                )
            )
    for load in loads:
        load.start()

    @pl.when(slab == 0)
    def _():
        for buf in (fin, gin):
            buf[:, 0:16, :] = jnp.zeros((CROPS, 16, C), BF16)

    @pl.when(slab == SLABS - 1)
    def _():
        for buf in (fin, gin):
            buf[:, DEEP - 16 : DEEP, :] = jnp.zeros((CROPS, 16, C), BF16)

    barrier = pltpu.get_barrier_semaphore()

    def greet(where):
        pl.semaphore_signal(barrier, inc=1, device_id=where, device_id_type=MESH)

    def image_of(d):
        return (s, slab, (img + d) % IMAGES)

    partner = (s, 2 * z + 1 - core, img)

    def chip_of(d):
        return (s, 2 * ((z + d) % CHIPS) + core, img)

    greeted = jnp.int32(0)
    for ds in (-1, 0, 1):
        for dj in (-1, 0, 1):
            if ds == 0 and dj == 0:
                continue
            ok = (s + ds >= 0) & (s + ds < SECTIONS) & (slab + dj >= 0) & (slab + dj < SLABS)

            @pl.when(ok)
            def _():
                greet((s + ds, slab + dj, img))

            greeted = greeted + jnp.where(ok, 1, 0)
    for d in range(1, IMAGES):
        greet(image_of(d))
    greet(partner)
    for d in (1, CHIPS - 1):
        greet(chip_of(d))
    i, j = iota((POS, POS), 0), iota((POS, POS), 1)
    swap = onehot((i // 8 == j % 8) & (i % 8 == j // 8))
    def chosen(first, shape):
        i, j = iota(shape, 0) + first, iota(shape, 1)
        lane = j % 32
        side = (j // HALF + core) % 2
        return (lane < IN_SHARE) & (i == IN_SHARE * (2 * ((j % HALF) // 32) + side) + lane)

    pc[...] = onehot(chosen(0, (256, 2 * HALF)))
    tail_row = iota((128, 2 * HALF), 0)
    pct[0] = onehot(chosen(256, (128, 2 * HALF)) & (tail_row < 64))
    pct[1] = onehot(chosen(192, (128, 2 * HALF)) & (tail_row >= 64))
    i, j = iota((C, 512), 0), iota((C, 512), 1)
    lane = j % 128
    owner = (j // 128 + img) % IMAGES
    sel[...] = onehot((lane < OUT_SHARE) & (i == OUT_SHARE * owner + lane))
    i, j = iota((768, 512), 0), iota((768, 512), 1)
    lane = i % 32
    c6[...] = onehot(
        (lane < IN_SHARE)
        & ((i % 128) // 32 == j // 128)
        & (j % 128 == IN_SHARE * (i // 128) + lane)
    )

    acc[...] = jnp.zeros_like(acc)
    pl.semaphore_wait(barrier, greeted + IMAGES + 2)

    def permuted(x, matrix):
        return jnp.dot(x, matrix, preferred_element_type=F32).astype(BF16)

    def spread(src, dst, send, recv, k, ds, center):
        base = 16 if src is dst else 0

        @pl.when(has_right)
        def _():
            pltpu.make_async_remote_copy(
                src_ref=src.at[k, pl.ds(base + POS - 16, 16)],
                dst_ref=dst.at[k, pl.ds(0, 16)],
                send_sem=send.at[2],
                recv_sem=recv.at[k],
                device_id=(s + ds, slab + 1, img),
                device_id_type=MESH,
            ).start()

        @pl.when(has_left)
        def _():
            pltpu.make_async_remote_copy(
                src_ref=src.at[k, pl.ds(base, 16)],
                dst_ref=dst.at[k, pl.ds(DEEP - 16, 16)],
                send_sem=send.at[0],
                recv_sem=recv.at[k],
                device_id=(s + ds, slab - 1, img),
                device_id_type=MESH,
            ).start()

        if center:
            pltpu.make_async_remote_copy(
                src_ref=src.at[k],
                dst_ref=dst.at[k, pl.ds(16, POS)],
                send_sem=send.at[1],
                recv_sem=recv.at[k],
                device_id=(s + ds, slab, img),
                device_id_type=MESH,
            ).start()

    def waited(ref, sem):
        pltpu.make_async_copy(ref, ref, sem).wait()

    inner = has_left & has_right

    def arrive(dst, recv, k, center):
        other = jnp.logical_not(center)
        for case, rows in (
            (center & inner, DEEP),
            (center & jnp.logical_not(inner), DEEP - 16),
            (other & inner, 32),
            (other & jnp.logical_not(inner), 16),
        ):

            @pl.when(case)
            def _():
                waited(dst.at[k, pl.ds(0, rows)], recv.at[k])

    def sent(src, send, center):
        if center:
            waited(src, send.at[1])

        @pl.when(has_right)
        def _():
            waited(src.at[:, pl.ds(0, 16)], send.at[2])

        @pl.when(has_left)
        def _():
            waited(src.at[:, pl.ds(0, 16)], send.at[0])

    loads[0].wait()
    loads[1].wait()

    def share_grad(a, k, chunks):
        gg[a, k, IMAGES - 1] = chunks[:, :128]
        for d in range(1, IMAGES):
            gs[a, k, d - 1] = chunks[:, 128 * d : 128 * (d + 1)]
            pltpu.make_async_remote_copy(
                src_ref=gs.at[a, k, d - 1],
                dst_ref=gg.at[a, k, d - 1],
                send_sem=gg_send.at[a],
                recv_sem=gg_recv.at[a, k],
                device_id=image_of(d),
                device_id_type=MESH,
            ).start()

    @pl.when(s == 0)
    def _():
        def step(k, carry):
            fin[k, 16 : 16 + POS, :] = permuted(swap, sv[k])
            spread(fin, fin, edge_send, fr, k, 0, False)
            return carry

        lax.fori_loop(0, CROPS, step, 0)

    @pl.when(s == SECTIONS - 1)
    def _():
        def step(k, carry):
            center = permuted(swap, cv[k])
            gin[k, 16 : 16 + POS, :] = center
            spread(gin, gin, edge_send, br, k, 0, False)
            share_grad(1, k, permuted(center, sel[...]))
            return carry

        lax.fori_loop(0, CROPS, step, 0)

    waited(w, weight_sem)

    def transpose_weights():
        def step(n, carry):
            part, tap = n // 9, n % 9
            wt[part, 8 - tap] = w[part, tap].T
            return carry

        lax.fori_loop(0, 18, step, 0)

    pl.when(s > 0)(transpose_weights)

    row = iota((WIDE, C), 0)
    inside = jnp.logical_not(
        ((row < 8) & (slab == 0)) | ((row >= WIDE - 8) & (slab == SLABS - 1))
    )

    last = CROPS - 1

    def share_fields(k, wide, active):
        mine = raw.at[k, IMAGES - 1]
        mine[:, 0:256] = wide[:, 0:256].astype(BF16)
        mine[:, 256:512] = active[:, 0:256]
        tails = jnp.concatenate([wide[:, 256:C], active[:, 256:C].astype(F32)], axis=1)
        mine[:, 512:PAIR] = tails.astype(BF16)
        for d in range(1, IMAGES):
            pltpu.make_async_remote_copy(
                src_ref=mine,
                dst_ref=raw.at[k, d - 1],
                send_sem=raw_send,
                recv_sem=raw_recv.at[k],
                device_id=image_of(d),
                device_id_type=MESH,
            ).start()

    def relay_field(k):
        waited(raw.at[k, pl.ds(0, IMAGES - 1)], raw_recv.at[k])
        for a in range(2):
            for n in range(IMAGES):
                both = (
                    jnp.dot(raw[k, n, :, 256 * a : 256 * (a + 1)], pc[...], preferred_element_type=F32)
                    + jnp.dot(raw[k, n, :, 512:PAIR], pct[a], preferred_element_type=F32)
                ).astype(BF16)
                fg[a, k, n] = both[:, :HALF]
                fs[a, k, n] = both[:, HALF:]
            pltpu.make_async_remote_copy(
                src_ref=fs.at[a, k],
                dst_ref=fg.at[a, k, pl.ds(IMAGES, IMAGES)],
                send_sem=fg_send,
                recv_sem=fg_recv.at[a, k],
                device_id=partner,
                device_id_type=MESH,
            ).start()

    def relay_grad(a, k, slots=IMAGES - 1):
        waited(gg.at[a, k, pl.ds(0, slots)], gg_recv.at[a, k])
        pltpu.make_async_remote_copy(
            src_ref=gg.at[a, k, pl.ds(0, IMAGES)],
            dst_ref=gg.at[a, k, pl.ds(IMAGES, IMAGES)],
            send_sem=gr_send,
            recv_sem=gr_recv.at[a, k],
            device_id=partner,
            device_id_type=MESH,
        ).start()

    def forward(k):
        arrive(fin, fr, k, s > 0)
        x = fin[k].astype(F32)
        hidden = conv(x, w, 0, WIDE)
        hid[k] = hidden
        active = jnp.where(inside, hidden * sigmoid(hidden), 0.0).astype(BF16)

        @pl.when(s < SECTIONS - 1)
        def _():
            result = x[16 : 16 + POS] + conv(active.astype(F32), w, 1, POS)
            fout[k] = result.astype(BF16)
            spread(fout, fin, fsend, fr, k, 1, True)

        share_fields(k, x[8 : 8 + WIDE], active)

        @pl.when((s == 0) & (k == last))
        def _():
            transpose_weights()

    def backward(k):
        arrive(gin, br, k, s < SECTIONS - 1)
        g = gin[k].astype(F32)
        center = g[16 : 16 + POS]
        shared = ((s == 0) & (k == last)) | (s == SECTIONS - 1)
        grad_active = conv(g, wt, 1, WIDE)
        hidden = hid[k]
        q = sigmoid(hidden)
        slope = q * (1.0 + hidden * (1.0 - q))
        grad_hidden = jnp.where(inside, grad_active * slope, 0.0).astype(BF16)
        wide = grad_hidden.astype(F32)
        grad_in = (center + conv(wide, wt, 0, POS)).astype(BF16)
        gout[k] = grad_in

        @pl.when(s > 0)
        def _():
            spread(gout, gin, bsend, br, k, -1, True)

        @pl.when((s == 1) & (k == last))
        def _():
            above = permuted(grad_in, sel[...])
            for d in range(IMAGES):
                us[d] = above[:, 128 * d : 128 * (d + 1)]
                pltpu.make_async_remote_copy(
                    src_ref=us.at[d],
                    dst_ref=gg.at[1, k, (d + IMAGES - 1) % IMAGES],
                    send_sem=up_send,
                    recv_sem=gg_recv.at[1, k],
                    device_id=(s - 1, slab, (img + d) % IMAGES),
                    device_id_type=MESH,
                ).start()

        lower = wide[8 : 8 + POS].astype(BF16)
        chunks = permuted(jnp.concatenate([lower, center.astype(BF16)], axis=0), sel[...])
        share_grad(0, k, chunks[:POS])

        @pl.when(jnp.logical_not(shared))
        def _():
            share_grad(1, k, chunks[POS:])

        @pl.when((s <= 1) & (k >= 2))
        def _():
            relay_grad(1, k - 2)
            relay_grad(0, k - 2)

    def unfold(k):
        for a in range(2):
            waited(fg.at[a, k, pl.ds(IMAGES, IMAGES)], fg_recv.at[a, k])

            def source(m, carry):
                shifted = row_shifts(fg[a, k, m].astype(F32))
                for d in range(3):
                    for b in range(3):
                        cc[a, k, 3 * d + b, pl.ds(pl.multiple_of(m * POS, POS), POS), :] = shifted[d][
                            8 * b : 8 * b + POS
                        ].astype(BF16)
                return carry

            lax.fori_loop(0, PEERS, source, 0)

    def contract(a, k):
        waited(gg.at[a, k, pl.ds(IMAGES, IMAGES)], gr_recv.at[a, k])
        grads = gg[a, k].reshape(PEERS * POS, 128).T[:OUT_SHARE]
        for t in range(9):
            acc[a, t] += jnp.dot(grads, cc[a, k, t], preferred_element_type=F32)

    ahead_count = jnp.where(s == 0, CROPS + 1, jnp.where(s == 1, CROPS - 1, 0))

    def unfold_step(n, early):
        late = jnp.logical_not(early)

        @pl.when(late & (n > 1))
        def _():
            def each(a, carry):
                contract(a, n - 2)
                return carry

            lax.fori_loop(0, 2, each, 0)

        todo = early | (n >= ahead_count)

        @pl.when(todo & (n > 0))
        def _():
            unfold(n - 1)

        @pl.when(late & (n > jnp.where(s == 1, 2, 0)))
        def _():
            relay_grad(1, n - 1)
            relay_grad(0, n - 1)

        @pl.when(todo & (n < CROPS))
        def _():
            relay_field(n)

    at_end = s == SECTIONS - 1

    def step(i, carry):
        def vouch(turn):
            for d in (1, CHIPS - 1):
                pl.semaphore_signal(
                    token.at[turn], inc=1, device_id=chip_of(d), device_id_type=MESH
                )

        @pl.when((s >= 2) & (i == 0))
        def _():
            for turn in range(3):
                vouch(turn)
                pl.semaphore_wait(token.at[turn], 2)

        turn = i - CROPS

        @pl.when((s < 2) & (turn > 0) & (turn <= 3))
        def _():
            pl.semaphore_wait(token.at[turn - 1], 2)

        @pl.when((s < 2) & (turn >= 0) & (turn < 3))
        def _():
            vouch(turn)

        back_from = CROPS + ahead_count
        is_forward = jnp.where(at_end, (i < 2 * CROPS) & (i % 2 == 0), i < CROPS)
        is_backward = jnp.where(
            at_end, (i < 2 * CROPS) & (i % 2 == 1), (i >= back_from) & (i < back_from + CROPS)
        )

        @pl.when(is_forward)
        def _():
            forward(jnp.where(at_end, i // 2, i))

        @pl.when(is_backward)
        def _():
            backward(jnp.where(at_end, i // 2, i - back_from))

        @pl.when(jnp.logical_not(is_forward | is_backward))
        def _():
            early = i < back_from
            unfold_step(jnp.where(early, i - CROPS, i - back_from - CROPS), early)

        return carry

    lax.fori_loop(0, 3 * CROPS + 1 + jnp.where(s == 1, ahead_count, 0), step, 0)

    def send_block(block, t, d, dst, recv):
        pltpu.make_async_remote_copy(
            src_ref=pk.at[t, block],
            dst_ref=dst,
            send_sem=z_send,
            recv_sem=recv,
            device_id=chip_of(d),
            device_id_type=MESH,
        ).start()

    def pack(t):
        for p in range(6):
            a, tap = divmod(6 * t + p, 9)
            block = acc[a, tap].astype(BF16)
            for half in range(2):
                pkl[t, half, :, 128 * p : 128 * (p + 1)] = block[:, 128 * half : 128 * (half + 1)]
        packed = permuted(pkl[t].reshape(2 * OUT_SHARE, 768), c6[...]).reshape(2, OUT_SHARE, 512)
        for half in range(2):
            for q in range(4):
                pk[t, 4 * half + q] = packed[half, :, 128 * q : 128 * (q + 1)]
        send_block((z + 4) % CHIPS, t, 1 if t % 2 == 0 else 7, far.at[t], far_recv.at[t])

    def direct(t):
        held = 3 if t % 2 == 0 else 5
        for slot, d in enumerate(DIRECT):
            if d != held:
                send_block((z + d) % CHIPS, t, d, rz.at[t, slot], z_recv.at[t])

    def merge(t):
        held = 3 if t % 2 == 0 else 5
        waited(far.at[t], far_recv.at[t])
        mine = pk.at[t, (z + held) % CHIPS]
        mine[...] = (mine[...].astype(F32) + far[t].astype(F32)).astype(BF16)
        send_block((z + held) % CHIPS, t, held, rz.at[t, DIRECT.index(held)], z_recv.at[t])

    def tail(i, carry):
        first = s == 0

        @pl.when(first & (i == 2))
        def _():
            relay_grad(1, 2)
            relay_grad(0, 2)
            relay_grad(1, last, IMAGES)

        @pl.when(first & (i == 6))
        def _():
            relay_grad(0, last)

        upper = ((i < 4) & (i % 2 == 0)) | (i == 4) | (i == 5)
        crop = jnp.where(i < 4, i // 2, jnp.where(i % 2 == 0, 2, last))

        @pl.when(first | (i != 6))
        def _():
            contract(jnp.where(upper, 1, 0), crop)

        @pl.when(i == 5)
        def _():
            pack(2)
            direct(2)

        return carry

    lax.fori_loop(jnp.where(s == 0, 0, 5), 2 * CROPS, tail, 0)
    pack(1)
    pack(0)
    direct(1)
    direct(0)
    for k in range(CROPS):
        gi_out[k] = permuted(swap, gout[k])
    merge(2)
    merge(1)
    merge(0)

    for t in (2, 0, 1):
        waited(rz.at[t], z_recv.at[t])
        total = pk[t, z].astype(F32)
        for slot in range(len(DIRECT)):
            total = total + rz[t, slot].astype(F32)
        gk_out[t] = (total * scaling).T

    waited(pk.at[:, pl.ds(0, CHIPS - 1)], z_send)
    waited(raw.at[:, pl.ds(0, IMAGES - 1)], raw_send)
    waited(fs, fg_send)
    waited(gs.at[0], gg_send.at[0])

    @pl.when(s == 0)
    def _():
        waited(gs.at[1, pl.ds(0, last)], gg_send.at[1])

    @pl.when(s > 0)
    def _():
        waited(gs.at[1], gg_send.at[1])

    @pl.when(s == 1)
    def _():
        waited(us, up_send)

    waited(gg.at[:, :, pl.ds(0, IMAGES)], gr_send)

    @pl.when(s == 0)
    def _():
        sent(fin, edge_send, False)

    @pl.when(s == SECTIONS - 1)
    def _():
        sent(gin, edge_send, False)

    @pl.when(s < SECTIONS - 1)
    def _():
        sent(fout, fsend, True)

    @pl.when(s > 0)
    def _():
        sent(gout, bsend, True)


def placed(gk, gi, gk_out, gi_out):
    gi_out[...] = gi[...]
    for n in range(18):
        a, tap = divmod(n, 9)
        t, p = divmod(n, 6)
        gk_out[tap, :, a, :] = gk[t, IN_SHARE * p : IN_SHARE * (p + 1), :]


def shards(strips, kernels, cotangent):
    scaling = 1.0 / math.sqrt(IMAGES * CROPS * ROWS * COLS * SLABS)
    dma = pltpu.SemaphoreType.DMA
    vmem = pl.BlockSpec(memory_space=pltpu.VMEM)
    hbm = pl.BlockSpec(memory_space=pl.ANY)
    gk, gi = pl.pallas_call(
        lambda *refs: kernel(scaling, *refs),
        out_shape=(
            pltpu.VMEM((3, 128, OUT_SHARE), F32),
            pltpu.VMEM((CROPS, POS, C), BF16),
        ),
        in_specs=[hbm, hbm, hbm],
        out_specs=(vmem, vmem),
        scratch_shapes=[
            pltpu.VMEM((2, 9, C, C), BF16),
            pltpu.VMEM((2, 9, C, C), BF16),
            pltpu.VMEM((CROPS, POS, C), BF16),
            pltpu.VMEM((CROPS, POS, C), BF16),
            pltpu.VMEM((CROPS, DEEP, C), BF16),
            pltpu.VMEM((CROPS, DEEP, C), BF16),
            pltpu.VMEM((CROPS, POS, C), BF16),
            pltpu.VMEM((CROPS, POS, C), BF16),
            pltpu.VMEM((CROPS, WIDE, C), F32),
            pltpu.VMEM((CROPS, IMAGES, WIDE, PAIR), BF16),
            pltpu.VMEM((2, CROPS, IMAGES, WIDE, HALF), BF16),
            pltpu.VMEM((2, CROPS, PEERS, WIDE, HALF), BF16),
            pltpu.VMEM((2, CROPS, IMAGES - 1, POS, 128), BF16),
            pltpu.VMEM((IMAGES, POS, 128), BF16),
            pltpu.VMEM((2, CROPS, PEERS, POS, 128), BF16),
            pltpu.VMEM((2, CROPS, 9, PEERS * POS, HALF), BF16),
            pltpu.VMEM((2, 9, OUT_SHARE, HALF), F32),
            pltpu.VMEM((3, 2, OUT_SHARE, 768), BF16),
            pltpu.VMEM((3, CHIPS, OUT_SHARE, 128), BF16),
            pltpu.VMEM((3, len(DIRECT), OUT_SHARE, 128), BF16),
            pltpu.VMEM((3, OUT_SHARE, 128), BF16),
            pltpu.VMEM((256, 2 * HALF), BF16),
            pltpu.VMEM((2, 128, 2 * HALF), BF16),
            pltpu.VMEM((C, 512), BF16),
            pltpu.VMEM((768, 512), BF16),
            dma((2,)),
            dma,
            dma((CROPS,)),
            dma((3,)),
            dma((CROPS,)),
            dma((3,)),
            dma((3,)),
            dma((CROPS,)),
            dma,
            dma((2, CROPS)),
            dma,
            dma((2, CROPS)),
            dma((2,)),
            dma,
            dma((2, CROPS)),
            dma,
            dma((3,)),
            dma((3,)),
            dma,
            pltpu.SemaphoreType.REGULAR((3,)),
        ],
        compiler_params=pltpu.CompilerParams(
            collective_id=0, has_side_effects=True, vmem_limit_bytes=60 * 1024 * 1024
        ),
        name="residual_step",
    )(
        strips.reshape(CROPS, POS, C),
        kernels.reshape(2, 9, C, C),
        cotangent.reshape(CROPS, POS, C),
    )
    gk, gi = pl.pallas_call(
        placed,
        out_shape=(
            jax.ShapeDtypeStruct((9, IN_SHARE, 2, OUT_SHARE), F32),
            jax.ShapeDtypeStruct((CROPS, POS, C), BF16),
        ),
        in_specs=[vmem, vmem],
        out_specs=(vmem, vmem),
        name="outputs",
    )(
        pltpu.with_memory_space_constraint(gk, pltpu.VMEM),
        pltpu.with_memory_space_constraint(gi, pltpu.VMEM),
    )
    return jnp.transpose(gk, (2, 0, 1, 3))[None], gi.reshape(1, 1, CROPS, ROWS, COLS, C)


def solution(mesh):
    return jax.shard_map(
        shards,
        mesh=mesh,
        in_specs=(
            P("img", None, None, "slab", None),
            P("section", None, None, None, None),
            P("img", None, None, "slab", None),
        ),
        out_specs=(
            P("section", None, None, "slab", "img"),
            P("section", "img", None, None, "slab", None),
        ),
        check_vma=False,
    )
```
